32 devices in a mesh: rep: 4 (over x, core), grp: 8 (over z, y).
Axes of the slice: x: 2, y: 2, z: 4, core: 2. Of those that a mesh axis runs over, the one named last changes fastest.
Arguments:
- tokens: float32 [8192, 1088], P(('rep', 'grp')), may hold values from -6 to 6
- document_lengths: int32 [32, 8], P(('rep', 'grp')), may hold values from 0 to 256, as said below
- cotangent: float32 [8192, 1088], P(('rep', 'grp')), may hold values from -6 to 6
- first_gain: bfloat16 [1088], P('grp'), may hold values from 0.25 to 1.75
- first_shift: bfloat16 [1088], P('grp'), may hold values from -3 to 3
- attention_in: bfloat16 [1088, 3264], P(None, 'grp'), may hold values from -2 to 2
- query_bias: bfloat16 [1088], P('grp'), may hold values from -3 to 3
- value_bias: bfloat16 [1088], P('grp'), may hold values from -3 to 3
- attention_out: bfloat16 [1088, 1088], P(None, 'grp'), may hold values from -0.75 to 0.75
- output_bias: bfloat16 [1088], P('grp'), may hold values from -3 to 3
- second_gain: bfloat16 [1088], P('grp'), may hold values from 0.25 to 1.75
- second_shift: bfloat16 [1088], P('grp'), may hold values from -3 to 3
- expand_weight: bfloat16 [1088, 4352], P(None, 'grp'), may hold values from -0.1875 to 0.1875
- expand_bias: bfloat16 [4352], P('grp'), may hold values from -3 to 3
- contract_weight: bfloat16 [4352, 1088], P(None, 'grp'), may hold values from -0.09375 to 0.09375
- contract_bias: bfloat16 [1088], P('grp'), may hold values from -3 to 3
Outputs:
- block_output: float32 [8192, 1088], P(('rep', 'grp'))
- tokens_gradient: float32 [8192, 1088], P(('rep', 'grp'))
- first_gain_gradient: float32 [1088], P('grp')
- first_shift_gradient: float32 [1088], P('grp')
- attention_in_gradient: float32 [1088, 3264], P(None, 'grp')
- query_bias_gradient: float32 [1088], P('grp')
- value_bias_gradient: float32 [1088], P('grp')
- attention_out_gradient: float32 [1088, 1088], P(None, 'grp')
- output_bias_gradient: float32 [1088], P('grp')
- second_gain_gradient: float32 [1088], P('grp')
- second_shift_gradient: float32 [1088], P('grp')
- expand_weight_gradient: float32 [1088, 4352], P(None, 'grp')
- expand_bias_gradient: float32 [4352], P('grp')
- contract_weight_gradient: float32 [4352, 1088], P(None, 'grp')
- contract_bias_gradient: float32 [1088], P('grp')
The draws below stay inside these ranges and needn't reach their ends.
Inputs may be any that keep to these rules, and one draw needn't show every extreme that they name: `document_lengths`: row r lists, in slot order, the lengths of up to 8 documents packed from the first of device r's 256 slots; a row sums to at least 64 and at most 256, some lengths are zero, and in every draw one row is a single document filling all 256 slots.
All inputs are finite; a program needn't handle non-finite values.
Results may differ from the reference program's by a relative error of at most 0.012.
Values may be sent and summed in bfloat16 or wider, within the bound.
A program may use at most 320 MiB of HBM per device.

```python
import jax
import jax.numpy as jnp
from jax import lax

D = 1088
H = 17
HD = 64
FF = 4352
TOK_DEV = 256
DOCS_DEV = 8
SHARDS = 32
TOKENS = 8192


def draw_document_lengths(key, part):
    count_key, full_key, cut_key = jax.random.split(key, 3)
    counts = jax.random.randint(count_key, (SHARDS,), TOK_DEV // 4, TOK_DEV + 1, dtype=jnp.int32)
    chosen = jax.random.randint(full_key, (), 0, SHARDS, dtype=jnp.int32)
    filled = jnp.arange(SHARDS, dtype=jnp.int32) == chosen
    counts = jnp.where(filled, TOK_DEV, counts).astype(jnp.int32)
    cuts = jax.random.randint(cut_key, (SHARDS, DOCS_DEV - 1), 0, counts[:, None] + 1, dtype=jnp.int32)
    cuts = jnp.sort(cuts, axis=1)
    cuts = jnp.where(filled[:, None], counts[:, None], cuts)
    zeros = jnp.zeros((SHARDS, 1), jnp.int32)
    bounds = jnp.concatenate([zeros, cuts, counts[:, None]], axis=1)
    return (bounds[:, 1:] - bounds[:, :-1]).astype(jnp.int32)


def draw_attention_in(key, part):
    base = jnp.clip(jax.random.normal(key, (D, 3 * D), jnp.float32), -4.0, 4.0) * D ** (-0.5)
    return base.astype(jnp.bfloat16)


def raised(drawn, rng, source, target, shards_of, factor):
    def block_of(dim):
        return (jnp.arange(drawn.shape[dim]) // (drawn.shape[dim] // shards_of)).reshape((-1,) + (1,) * (drawn.ndim - 1 - dim))

    first = jax.random.permutation(rng, shards_of)[block_of(target)]
    other_side = (block_of(target) + shards_of // 2) % shards_of
    return jnp.where((block_of(source) == first) | (block_of(source) == other_side), factor * drawn, drawn)


def shard_levels(rng, dims, cuts, low, high):
    level, own = 1.0, jax.random.fold_in(rng, 6)
    for position, blocks in cuts:
        steps = jnp.exp(jax.random.uniform(jax.random.fold_in(own, position), (blocks,), jnp.float32, low / len(cuts), high / len(cuts)))
        level = level * jnp.repeat(steps, dims[position] // blocks).reshape([-1 if axis == position else 1 for axis in range(len(dims))])
    return level


def bell_draw(key, extent, width, most, cuts=(), kind=jnp.bfloat16):
    loudness = shard_levels(key, extent, cuts, -0.22, 0.18) if cuts else 1.0
    drawn = jax.random.normal(key, extent, jnp.float32) * width * loudness
    return jnp.minimum(jnp.maximum(drawn, -most), most).astype(kind)


def heavy_noise(stream_key, shape, spread, reach, shards, heavy, held_as=jnp.bfloat16):
    values = spread * jax.random.normal(stream_key, shape, jnp.float32)
    if shards:
        values = values * shard_levels(stream_key, shape, shards, -0.22, 0.18)
    return jnp.clip(raised(values, jax.random.fold_in(stream_key, 3), *heavy), -reach, reach).astype(held_as)


def setup_inputs(seed: int = 0) -> dict:
    key_of = jax.random.split(jax.random.key(seed), 17)
    return {
        "tokens": bell_draw(key_of[0], (TOKENS, D), 1.0, 6.0, ((0, 32),), jnp.float32),
        "document_lengths": draw_document_lengths(jax.random.fold_in(key_of[16], 71), 0),
        "cotangent": heavy_noise(key_of[2], (TOKENS, D), 1.0, 6.0, ((0, 32),), (0, 1, 32, 2.75), jnp.float32),
        "first_gain": jnp.clip(1.0 + 0.15 * jax.random.normal(key_of[3], (D,), jnp.float32), 0.25, 1.75).astype(jnp.bfloat16),
        "first_shift": bell_draw(key_of[4], (D,), 0.5, 3.0, ((0, 8),)),
        "attention_in": draw_attention_in(jax.random.fold_in(key_of[16], 71), 0),
        "query_bias": bell_draw(key_of[6], (D,), 0.5, 3.0, ((0, 8),)),
        "value_bias": bell_draw(key_of[7], (D,), 0.5, 3.0, ((0, 8),)),
        "attention_out": bell_draw(key_of[8], (D, D), (D // 16) ** -0.5, 0.75, ((1, 8),)),
        "output_bias": bell_draw(key_of[9], (D,), 0.5, 3.0, ((0, 8),)),
        "second_gain": jnp.clip(1.0 + 0.15 * jax.random.normal(key_of[10], (D,), jnp.float32), 0.25, 1.75).astype(jnp.bfloat16),
        "second_shift": bell_draw(key_of[11], (D,), 0.5, 3.0, ((0, 8),)),
        "expand_weight": bell_draw(key_of[12], (D, FF), D ** -0.5, 0.1875, ((1, 8),)),
        "expand_bias": bell_draw(key_of[13], (FF,), 0.5, 3.0, ((0, 8),)),
        "contract_weight": bell_draw(key_of[14], (FF, D), FF ** -0.5, 0.09375, ((1, 8),)),
        "contract_bias": bell_draw(key_of[15], (D,), 0.5, 3.0, ((0, 8),)),
    }


EPSILON = 1e-05
MASKED = -1e+30

def matmul(left, right):
    return jnp.dot(left.astype(jnp.float32), right.astype(jnp.float32), precision=lax.Precision.HIGHEST)

def product(form, left, right):
    return jnp.einsum(form, left.astype(jnp.float32), right.astype(jnp.float32), precision=lax.Precision.HIGHEST)

def layer_norm(values, gain, shift):
    center = values - lax.optimization_barrier(jnp.mean(values, axis=-1, keepdims=True))
    inverse = lax.rsqrt(lax.optimization_barrier(jnp.mean(center * center, axis=-1, keepdims=True)) + EPSILON)
    normed = center * inverse
    return (normed, inverse, normed * gain.astype(jnp.float32) + shift.astype(jnp.float32))

def norm_back(upstream, normed, inverse, gain):
    scaled = upstream * gain.astype(jnp.float32)
    return inverse * (scaled - lax.optimization_barrier(jnp.mean(scaled, axis=-1, keepdims=True)) - normed * lax.optimization_barrier(jnp.mean(scaled * normed, axis=-1, keepdims=True)))

def document_layout(lengths, count):
    ends = jnp.cumsum(lengths).astype(jnp.int32)
    slots = jnp.arange(count, dtype=jnp.int32)
    number = lax.optimization_barrier(jnp.sum((slots[:, None] >= ends[None, :]).astype(jnp.int32), axis=1)).astype(jnp.int32)
    valid = slots < ends[-1]
    labels = jnp.where(valid, number, lengths.shape[0] + slots).astype(jnp.int32)
    return (valid, labels)

def block_scores(query, keyset, labels, lower, upper):
    positions = jnp.arange(upper, dtype=jnp.int32)
    allowed = (positions[None, :] <= positions[lower:upper, None]) & (labels[None, :upper] == labels[lower:upper, None])
    raw = product('qhd,khd->hqk', query[lower:upper], keyset[:upper]) * HD ** (-0.5)
    return jnp.where(allowed[None, :, :], raw, MASKED)

def attend_forward(query, keyset, valueset, labels):
    count = query.shape[0]
    span = min(count, 512)
    outputs = []
    totals = []
    for index in range(count // span):
        lower = index * span
        upper = lower + span
        scores = block_scores(query, keyset, labels, lower, upper)
        peak = lax.optimization_barrier(jnp.max(scores, axis=-1, keepdims=True))
        logsum = peak + jnp.log(lax.optimization_barrier(jnp.sum(jnp.exp(scores - peak), axis=-1, keepdims=True)))
        weights = jnp.exp(scores - logsum).astype(jnp.bfloat16)
        outputs.append(product('hqk,khd->qhd', weights, valueset[:upper]))
        totals.append(logsum[:, :, 0])
    return (jnp.concatenate(outputs, axis=0), jnp.concatenate(totals, axis=1))

def attend_backward(query, keyset, valueset, labels, logsum, upstream, attended):
    count = query.shape[0]
    span = min(count, 512)
    delta = lax.optimization_barrier(jnp.sum(upstream.astype(jnp.float32) * attended.astype(jnp.float32), axis=-1)).T
    query_parts = []
    key_grad = jnp.zeros(keyset.shape, jnp.float32)
    value_grad = jnp.zeros(valueset.shape, jnp.float32)
    for index in range(count // span):
        lower = index * span
        upper = lower + span
        scores = block_scores(query, keyset, labels, lower, upper)
        probability = jnp.exp(scores - logsum[:, lower:upper, None])
        weights = probability.astype(jnp.bfloat16)
        flow = product('qhd,khd->hqk', upstream[lower:upper], valueset[:upper])
        slope = (probability * (flow - delta[:, lower:upper, None]) * HD ** (-0.5)).astype(jnp.bfloat16)
        query_parts.append(product('hqk,khd->qhd', slope, keyset[:upper]))
        key_grad = key_grad.at[:upper].add(product('hqk,qhd->khd', slope, query[lower:upper]))
        value_grad = value_grad.at[:upper].add(product('hqk,qhd->khd', weights, upstream[lower:upper]))
    return (jnp.concatenate(query_parts, axis=0), key_grad, value_grad)

def device_pass(params, tokens, lengths, cotangent):
    first_gain, first_shift, attention_in, query_bias, value_bias, attention_out, output_bias, second_gain, second_shift, expand_weight, expand_bias, contract_weight, contract_bias = params
    count = tokens.shape[0]
    valid, labels = document_layout(lengths, count)
    normed_one, inverse_one, hidden_one = layer_norm(tokens, first_gain, first_shift)
    hidden_one = hidden_one.astype(jnp.bfloat16)
    bias_all = jnp.concatenate([query_bias.astype(jnp.float32), jnp.zeros((D,), jnp.float32), value_bias.astype(jnp.float32)])
    projected = (matmul(hidden_one, attention_in) + bias_all).astype(jnp.bfloat16)
    heads = projected.reshape(count, 3, H, HD)
    query = heads[:, 0]
    keyset = heads[:, 1]
    valueset = heads[:, 2]
    mixed, logsum = attend_forward(query, keyset, valueset, labels)
    attended = mixed.astype(jnp.bfloat16)
    flat_attended = attended.reshape(count, D)
    residual = tokens + matmul(flat_attended, attention_out) + output_bias.astype(jnp.float32)
    normed_two, inverse_two, hidden_two = layer_norm(residual, second_gain, second_shift)
    hidden_two = hidden_two.astype(jnp.bfloat16)
    before = matmul(hidden_two, expand_weight) + expand_bias.astype(jnp.float32)
    activated = jax.nn.gelu(before).astype(jnp.bfloat16)
    output = residual + matmul(activated, contract_weight) + contract_bias.astype(jnp.float32)
    live = valid[:, None]
    block_output = jnp.where(live, output, 0.0)
    start = jnp.where(live, cotangent, 0.0)
    start_low = start.astype(jnp.bfloat16)
    _, gelu_back = jax.vjp(jax.nn.gelu, before)
    back_before = gelu_back(matmul(start_low, contract_weight.T))[0]
    back_before_low = back_before.astype(jnp.bfloat16)
    back_hidden_two = matmul(back_before_low, expand_weight.T)
    back_residual = start + norm_back(back_hidden_two, normed_two, inverse_two, second_gain)
    back_residual_low = back_residual.astype(jnp.bfloat16)
    back_attended = matmul(back_residual_low, attention_out.T).astype(jnp.bfloat16).reshape(count, H, HD)
    back_query, back_key, back_value = attend_backward(query, keyset, valueset, labels, logsum, back_attended, attended)
    back_query = back_query.reshape(count, D)
    back_value = back_value.reshape(count, D)
    back_projected = jnp.concatenate([back_query, back_key.reshape(count, D), back_value], axis=1)
    back_projected_low = back_projected.astype(jnp.bfloat16)
    back_hidden_one = matmul(back_projected_low, attention_in.T)
    tokens_gradient = back_residual + norm_back(back_hidden_one, normed_one, inverse_one, first_gain)
    gradients = (lax.optimization_barrier(jnp.sum(back_hidden_one * normed_one, axis=0)), lax.optimization_barrier(jnp.sum(back_hidden_one, axis=0)), matmul(hidden_one.T, back_projected_low), lax.optimization_barrier(jnp.sum(back_query, axis=0)), lax.optimization_barrier(jnp.sum(back_value, axis=0)), matmul(flat_attended.T, back_residual_low), lax.optimization_barrier(jnp.sum(back_residual, axis=0)), lax.optimization_barrier(jnp.sum(back_hidden_two * normed_two, axis=0)), lax.optimization_barrier(jnp.sum(back_hidden_two, axis=0)), matmul(hidden_two.T, back_before_low), lax.optimization_barrier(jnp.sum(back_before, axis=0)), matmul(activated.T, start_low), lax.optimization_barrier(jnp.sum(start, axis=0)))
    return (block_output, tokens_gradient, gradients)

def reference(tokens, document_lengths, cotangent, first_gain, first_shift, attention_in, query_bias, value_bias, attention_out, output_bias, second_gain, second_shift, expand_weight, expand_bias, contract_weight, contract_bias):
    params = (first_gain, first_shift, attention_in, query_bias, value_bias, attention_out, output_bias, second_gain, second_shift, expand_weight, expand_bias, contract_weight, contract_bias)

    def advance(carry, inputs):
        piece, lengths, upstream = inputs
        shard_output, shard_gradient, terms = device_pass(params, piece, lengths, upstream)
        return (tuple((left + right for left, right in zip(carry, terms))), (shard_output, shard_gradient))
    zeros_start = tuple((jnp.zeros(weight.shape, jnp.float32) for weight in params))
    totals, (outputs, gradients) = lax.scan(advance, zeros_start, (tokens.reshape(SHARDS, TOK_DEV, D), document_lengths, cotangent.reshape(SHARDS, TOK_DEV, D)))
    return (outputs.reshape(TOKENS, D), gradients.reshape(TOKENS, D), totals[0], totals[1], totals[2], totals[3], totals[4], totals[5], totals[6], totals[7], totals[8], totals[9], totals[10], totals[11], totals[12])
```

```python
import functools

import jax
import jax.numpy as jnp
from jax import lax
from jax.experimental import pallas as pl
from jax.experimental.pallas import tpu as pltpu
from jax.sharding import PartitionSpec as P

HD = 64
EPSILON = 1e-05
MASKED = -1e30
YSIZE = 2
MESH_ID = pl.DeviceIdType.MESH
VMEM_LIMIT = 67043328


def layer_norm(values, gain, shift):
    center = values - jnp.mean(values, axis=-1, keepdims=True)
    inverse = lax.rsqrt(jnp.mean(center * center, axis=-1, keepdims=True) + EPSILON)
    normed = center * inverse
    return (normed, inverse, normed * gain.astype(jnp.float32) + shift.astype(jnp.float32))


def norm_back(upstream, normed, inverse, gain):
    scaled = upstream * gain.astype(jnp.float32)
    return inverse * (
        scaled
        - jnp.mean(scaled, axis=-1, keepdims=True)
        - normed * jnp.mean(scaled * normed, axis=-1, keepdims=True)
    )


def product(form, left, right):
    return jnp.einsum(form, left, right, preferred_element_type=jnp.float32)


def document_layout(lengths, count):
    ends = jnp.cumsum(lengths)
    slots = jnp.arange(count, dtype=jnp.int32)
    number = jnp.sum((slots[:, None] >= ends[None, :]).astype(jnp.int32), axis=1)
    valid = slots < ends[-1]
    labels = jnp.where(valid, number, lengths.shape[0] + slots)
    return (valid, labels)


class Place:
    def __init__(self, rep_count, grp_count):
        self.R, self.G = rep_count, grp_count
        self.Y = YSIZE
        self.Z = grp_count // YSIZE
        self.r = lax.axis_index("rep")
        self.g = lax.axis_index("grp")
        self.c = self.r % 2
        self.m = self.r // 2
        self.xi = self.m % 2
        self.z = self.g // YSIZE
        self.y = self.g % YSIZE
        self.partner = (self.r + 1 - 2 * self.c, self.g)
        self.xnbr = (self.r + 2 - 4 * self.xi, self.g)
        self.ynbr = (self.r, self.g + 1 - 2 * self.y)
        self.up = (self.r, self.g + YSIZE)
        self.down = (self.r, self.g - YSIZE)

    def flip_rep(self, bit):
        on = (self.r // (1 << bit)) % 2
        return (self.r + (1 << bit) - (2 << bit) * on, self.g)

    def flip_grp(self, bit):
        on = (self.g // (1 << bit)) % 2
        return (self.r, self.g + (1 << bit) - (2 << bit) * on)


def greet(here, others):
    barrier = pltpu.get_barrier_semaphore()

    def hello(target):
        pl.semaphore_signal(barrier, inc=1, device_id=target, device_id_type=MESH_ID)

    for target in [here.partner, here.xnbr, here.ynbr] + others:
        hello(target)

    @pl.when(here.z < here.Z - 1)
    def _():
        hello(here.up)

    @pl.when(here.z > 0)
    def _():
        hello(here.down)

    inner = jnp.where((here.z > 0) & (here.z < here.Z - 1), 1, 0)
    pl.semaphore_wait(barrier, 4 + len(others) + inner)


def remote(src, dst, send, recv, target):
    return pltpu.make_async_remote_copy(
        src_ref=src, dst_ref=dst, send_sem=send, recv_sem=recv, device_id=target, device_id_type=MESH_ID
    )


def bits_of(count):
    return count.bit_length() - 1


def gather_kernel(
    R,
    G,
    share,
    ahead,
    own_ref,
    small_ref,
    all_ref,
    small_all,
    bounce,
    local_sem,
    small_send,
    small_recv,
    send_own,
    send_fwd,
    send_y,
    send_x,
    send_cp,
    send_cx,
    recv_p,
    recv_x,
    recv_cp,
    recv_cx,
):
    here = Place(R, G)
    N, n = own_ref.shape[0], own_ref.shape[1]
    Z = here.Z
    y, z, c, xi = here.y, here.z, here.c, here.xi
    width = n - share
    start = pl.multiple_of(xi * share, 8)
    give = pl.multiple_of(xi * width, 8)
    take = pl.multiple_of((1 - xi) * width, 8)
    grp_bits = bits_of(G)
    extra = [here.flip_grp(b) for b in range(2, grp_bits)]
    greet(here, extra)

    pull = pltpu.make_async_copy(own_ref, bounce, local_sem.at[0])
    pull.start()

    def plane(k, g):
        return all_ref.at[g, k, pl.ds(start, width), :]

    def gift(k, g):
        return all_ref.at[g, k, pl.ds(give, share), :]

    def due(k, g):
        return all_ref.at[g, k, pl.ds(take, share), :]

    def own_part(k):
        return own_ref.at[k, pl.ds(start, width), :]

    def shard(zz, yy):
        return zz * YSIZE + yy

    def own_copy(k, way):
        target = (here.up, here.down, here.ynbr)[way]
        return remote(own_part(k), plane(k, here.g), send_own.at[k, way], recv_p.at[k, z], target)

    def passing(k, zz):
        step = jnp.where(zz < z, YSIZE, -YSIZE)
        ref = plane(k, shard(zz, y))
        return remote(ref, ref, send_fwd.at[k, zz], recv_p.at[k, zz], (here.r, here.g + step))

    def over_y(k, zz):
        ref = plane(k, shard(zz, y))
        return remote(ref, ref, send_y.at[k, zz], recv_p.at[k, zz], here.ynbr)

    def over_x(k, zz):
        ref = gift(k, shard(zz, c))
        return remote(ref, ref, send_x.at[k, zz], recv_x.at[k, zz], here.xnbr)

    def plane_to_partner(k, zz):
        ref = plane(k, shard(zz, c))
        return remote(ref, ref, send_cp.at[k, zz], recv_cp.at[k, zz], here.partner)

    def rest_to_partner(k, zz):
        ref = due(k, shard(zz, c))
        return remote(ref, ref, send_cx.at[k, zz], recv_cx.at[k, zz], here.partner)

    def from_partner_plane(k, zz):
        ref = plane(k, shard(zz, 1 - c))
        return remote(ref, ref, send_cp.at[k, zz], recv_cp.at[k, zz], here.partner)

    def from_partner_rest(k, zz):
        ref = due(k, shard(zz, 1 - c))
        return remote(ref, ref, send_cx.at[k, zz], recv_cx.at[k, zz], here.partner)

    def x_arrival(k, zz):
        ref = due(k, shard(zz, c))
        return remote(ref, ref, send_x.at[k, zz], recv_x.at[k, zz], here.xnbr)

    def nth(i):
        table = [sorted([q for q in range(Z) if q != p], key=lambda q: abs(q - p)) for p in range(Z)]
        pick = table[0][i]
        for p in range(1, Z):
            pick = jnp.where(z == p, table[p][i], pick)
        return pick

    def goes_on(zz):
        return ((zz < z) & (z < Z - 1)) | ((zz > z) & (z > 0))

    source = y == c

    def small_copy(bit):
        size = 1 << bit
        base = (here.g // size) * size
        ref = small_all.at[pl.ds(base, size)]
        return remote(ref, ref, small_send.at[bit], small_recv.at[bit], here.flip_grp(bit))

    def small_arrival(bit):
        size = 1 << bit
        base = (here.g // size) * size
        base = base + size - 2 * size * ((here.g // size) % 2)
        ref = small_all.at[pl.ds(base, size)]
        return remote(ref, ref, small_send.at[bit], small_recv.at[bit], here.flip_grp(bit))

    def body(t, carry):
        @pl.when((t < N) & source)
        def _():
            @pl.when(z < Z - 1)
            def _():
                own_copy(t, 0).start()

            @pl.when(z > 0)
            def _():
                own_copy(t, 1).start()

            own_copy(t, 2).start()

        k = t - ahead

        @pl.when((k >= 0) & (k < N) & source)
        def _():
            def arrival(i, carry):
                zz = nth_dynamic(i)
                passing(k, zz).wait_recv()

                @pl.when(goes_on(zz))
                def _():
                    passing(k, zz).start()

                over_y(k, zz).start()
                over_x(k, zz).start()
                plane_to_partner(k, zz).start()
                return carry

            lax.fori_loop(0, Z - 1, arrival, 0)

        @pl.when((k >= 0) & (k < N) & (y != c))
        def _():
            def arrival(i, carry):
                zz = jnp.where(i == 0, z, nth_dynamic(i - 1))
                ref = plane(k, shard(zz, c))
                remote(ref, ref, send_y.at[k, zz], recv_p.at[k, zz], here.ynbr).wait_recv()
                over_x(k, zz).start()
                plane_to_partner(k, zz).start()
                return carry

            lax.fori_loop(0, Z, arrival, 0)

        q = t - ahead - 1

        @pl.when((q >= 0) & (q < N))
        def _():
            def arrival(zz, carry):
                @pl.when((y != c) | (zz != z))
                def _():
                    x_arrival(q, zz).wait_recv()
                    rest_to_partner(q, zz).start()

                return carry

            lax.fori_loop(0, Z, arrival, 0)

        return carry

    def nth_dynamic(i):
        pick = nth(0)
        for j in range(1, Z - 1):
            pick = jnp.where(i == j, nth(j), pick)
        return pick

    seed = pltpu.make_async_copy(small_ref, small_all.at[here.g], local_sem.at[1])
    seed.start()
    seed.wait()
    for bit in range(grp_bits):
        small_copy(bit).start()
        if bit == 0:
            lax.fori_loop(0, ahead, body, 0)
        small_arrival(bit).wait_recv()
    pull.wait()
    push = pltpu.make_async_copy(bounce, all_ref.at[here.g], local_sem.at[0])
    push.start()
    lax.fori_loop(ahead, N + ahead + 1, body, 0)
    push.wait()

    def settle(k, carry):
        @pl.when(source)
        def _():
            @pl.when(z < Z - 1)
            def _():
                own_copy(k, 0).wait_send()

            @pl.when(z > 0)
            def _():
                own_copy(k, 1).wait_send()

            own_copy(k, 2).wait_send()

        def each(zz, carry):
            @pl.when((y != c) | (zz != z))
            def _():
                over_x(k, zz).wait_send()
                plane_to_partner(k, zz).wait_send()
                rest_to_partner(k, zz).wait_send()

            @pl.when(source & (zz != z))
            def _():
                over_y(k, zz).wait_send()

                @pl.when(goes_on(zz))
                def _():
                    passing(k, zz).wait_send()

            @pl.when((y == c) | (zz != z))
            def _():
                from_partner_plane(k, zz).wait_recv()
                from_partner_rest(k, zz).wait_recv()

            return carry

        lax.fori_loop(0, Z, each, 0)
        return carry

    lax.fori_loop(0, N, settle, 0)
    for bit in range(grp_bits):
        small_copy(bit).wait_send()


def gather_all(own, small, R, G):
    N, n, K = own.shape
    Z = G // YSIZE
    bits = bits_of(G)
    share = (6 * n // 17) // 8 * 8
    dma = pltpu.SemaphoreType.DMA
    return pl.pallas_call(
        functools.partial(gather_kernel, R, G, share, 2),
        out_shape=(
            jax.ShapeDtypeStruct((G, N, n, K), jnp.bfloat16),
            jax.ShapeDtypeStruct((G,) + small.shape, jnp.bfloat16),
        ),
        in_specs=[pl.BlockSpec(memory_space=pl.ANY)] * 2,
        out_specs=(pl.BlockSpec(memory_space=pl.ANY),) * 2,
        scratch_shapes=[
            pltpu.VMEM((N, n, K), jnp.bfloat16),
            dma((2,)),
            dma((bits,)),
            dma((bits,)),
            dma((N, 3)),
        ]
        + [dma((N, Z))] * 9,
        compiler_params=pltpu.CompilerParams(collective_id=0, has_side_effects=True, vmem_limit_bytes=VMEM_LIMIT),
        name="gather_all",
    )(own, small)


def reduce_kernel(
    R,
    G,
    share,
    con_count,
    exp_count,
    dy_ref,
    x_ref,
    vec_ref,
    out_ref,
    vec_out,
    pair_buf,
    dyo,
    dyp,
    xo,
    xp,
    plane,
    xs,
    xb,
    yb,
    zb,
    fx,
    fin,
    pair_tmp,
    vec_buf,
    vec_got,
    dy_local,
    x_local,
    dy_send,
    dy_recv,
    x_send,
    x_recv,
    xs_send,
    xs_recv,
    y_send,
    y_recv,
    z_send,
    z_recv,
    f_send,
    f_recv,
    o_local,
    o_send,
    o_recv,
    pair_send,
    pair_recv,
    pair_local,
    vec_send,
    vec_recv,
):
    here = Place(R, G)
    Z = here.Z
    y, z, c, xi = here.y, here.z, here.c, here.xi
    N, n = out_ref.shape[0], out_ref.shape[1]
    D_N, X_N = dy_ref.shape[0], x_ref.shape[0]
    width = n - share
    rep_bits, grp_bits = bits_of(R), bits_of(G)
    rounds = rep_bits + grp_bits
    extra = [here.flip_grp(b) for b in range(2, grp_bits)] + [here.flip_rep(b) for b in range(2, rep_bits)]
    greet(here, extra)
    sink = y == c

    def dy_local_copy(i):
        return pltpu.make_async_copy(dy_ref.at[i, :, c], dyo.at[i], dy_local.at[i])

    def x_local_copy(i):
        return pltpu.make_async_copy(x_ref.at[i], xo.at[i], x_local.at[i])

    def dy_swap(i):
        return remote(dy_ref.at[i, :, 1 - c], dyp.at[i], dy_send.at[i], dy_recv.at[i], here.partner)

    def x_swap(i):
        return remote(x_ref.at[i], xp.at[i], x_send.at[i], x_recv.at[i], here.partner)

    order = [("d", 0)] + [("x", i) for i in range(con_count)]
    order += [("d", 1), ("x", con_count)] + [("d", i) for i in range(2, 1 + exp_count)]
    order += [("d", 1 + exp_count), ("x", con_count + 1), ("d", 2 + exp_count), ("x", con_count + 2)]
    order += [("d", i) for i in range(3 + exp_count, D_N)]
    for kind, i in order:
        if kind == "d":
            dy_swap(i).start()
            dy_local_copy(i).start()
        else:
            x_swap(i).start()
            x_local_copy(i).start()

    def dy_of(k):
        return jnp.maximum(k - (con_count - 1), 0)

    def x_of(k):
        first, second = con_count + exp_count, con_count + exp_count + 1
        return jnp.where(
            k < con_count, k, jnp.where(k < first, con_count, jnp.where(k < second, con_count + 1, con_count + 2))
        )

    def x_copy(k, zz):
        return remote(xs.at[k, zz], xb.at[k, zz], xs_send.at[k, zz], xs_recv.at[k, zz], here.xnbr)

    def y_copy(k, zz):
        return remote(plane.at[k, zz], yb.at[k, zz], y_send.at[k, zz], y_recv.at[k, zz], here.ynbr)

    def up_copy(k, zz):
        return remote(plane.at[k, zz], zb.at[k, zz], z_send.at[k, zz], z_recv.at[k, zz], here.up)

    def down_slot(zz, at):
        return jnp.where(zz == at, Z, zz)

    def down_copy(k, zz):
        slot = down_slot(zz, z - 1)
        return remote(plane.at[k, zz], zb.at[k, slot], z_send.at[k, zz], z_recv.at[k, slot], here.down)

    def z_arrival(k, slot, target):
        return remote(plane.at[k, 0], zb.at[k, slot], z_send.at[k, 0], z_recv.at[k, slot], target)

    def f_copy(k):
        return remote(plane.at[k, z], fx.at[k], f_send.at[k], f_recv.at[k], here.xnbr)

    def o_keep(k):
        return pltpu.make_async_copy(fin.at[k % 2], out_ref.at[k], o_local.at[k])

    def o_give(k):
        return remote(fin.at[k % 2], out_ref.at[k], o_send.at[k], o_recv.at[k], here.partner)

    def f32(value):
        return value.astype(jnp.float32)

    def multiply(k):
        di, xj = dy_of(k), x_of(k)

        @pl.when((k == 0) | (k >= con_count))
        def _():
            dy_local_copy(di).wait()
            dy_swap(di).wait_recv()

        @pl.when((k <= con_count) | (k == con_count + exp_count) | (k == con_count + exp_count + 1))
        def _():
            x_local_copy(xj).wait()
            x_swap(xj).wait_recv()

        def each(zz, carry):
            term = jnp.dot(dyo[di, zz], xo[xj], preferred_element_type=jnp.float32)
            term = term + jnp.dot(dyp[di, zz], xp[xj], preferred_element_type=jnp.float32)

            @pl.when(xi == 0)
            def _():
                plane[k, zz] = term[:width].astype(jnp.bfloat16)
                xs[k, zz] = term[width:].astype(jnp.bfloat16)

            @pl.when(xi == 1)
            def _():
                plane[k, zz] = term[share:].astype(jnp.bfloat16)
                xs[k, zz] = term[:share].astype(jnp.bfloat16)

            x_copy(k, zz).start()
            return carry

        lax.fori_loop(0, Z, each, 0)

    def after_x(k):
        def each(zz, carry):
            x_copy(k, zz).wait_recv()
            got = f32(xb[k, zz])

            @pl.when(xi == 0)
            def _():
                plane[k, zz, :share] = (f32(plane[k, zz, :share]) + got).astype(jnp.bfloat16)

            @pl.when(xi == 1)
            def _():
                low = width - share
                plane[k, zz, low:] = (f32(plane[k, zz, low:]) + got).astype(jnp.bfloat16)

            @pl.when(y != c)
            def _():
                y_copy(k, zz).start()

            return carry

        lax.fori_loop(0, Z, each, 0)

    def after_y(k):
        @pl.when(sink)
        def _():
            def each(zz, carry):
                y_copy(k, zz).wait_recv()
                plane[k, zz] = (f32(plane[k, zz]) + f32(yb[k, zz])).astype(jnp.bfloat16)
                return carry

            lax.fori_loop(0, Z, each, 0)

            def line(i, carry):
                high = Z - 1 - i

                @pl.when(high > z)
                def _():
                    @pl.when(z > 0)
                    def _():
                        z_arrival(k, high, here.down).wait_recv()
                        plane[k, high] = (f32(plane[k, high]) + f32(zb[k, high])).astype(jnp.bfloat16)

                    up_copy(k, high).start()

                @pl.when(i < z)
                def _():
                    @pl.when(z < Z - 1)
                    def _():
                        z_arrival(k, i, here.up).wait_recv()
                        plane[k, i] = (f32(plane[k, i]) + f32(zb[k, i])).astype(jnp.bfloat16)

                    down_copy(k, i).start()

                return carry

            lax.fori_loop(0, Z - 1, line, 0)

    def after_z(k):
        @pl.when(sink)
        def _():
            @pl.when(z == 0)
            def _():
                z_arrival(k, Z, here.up).wait_recv()
                plane[k, z] = (f32(plane[k, z]) + f32(zb[k, Z])).astype(jnp.bfloat16)

            @pl.when(z == Z - 1)
            def _():
                z_arrival(k, z, here.down).wait_recv()
                plane[k, z] = (f32(plane[k, z]) + f32(zb[k, z])).astype(jnp.bfloat16)

            @pl.when((z > 0) & (z < Z - 1))
            def _():
                z_arrival(k, z, here.down).wait_recv()
                z_arrival(k, Z, here.up).wait_recv()
                plane[k, z] = (f32(plane[k, z]) + f32(zb[k, z]) + f32(zb[k, Z])).astype(jnp.bfloat16)

            f_copy(k).start()

    def finish(k):
        @pl.when(sink)
        def _():
            f_copy(k).wait_recv()

            @pl.when(k >= 2)
            def _():
                o_keep(k - 2).wait()
                o_give(k - 2).wait_send()

            slot = k % 2

            def assemble(first, second):
                fin[slot, :share] = f32(first[:share])
                fin[slot, share:width] = f32(first[share:]) + f32(second[: width - share])
                fin[slot, width:] = f32(second[width - share :])

            @pl.when(xi == 0)
            def _():
                assemble(plane[k, z], fx[k])

            @pl.when(xi == 1)
            def _():
                assemble(fx[k], plane[k, z])

            for bit in range(2, rep_bits):
                j = bit - 2
                give = remote(fin.at[slot], pair_buf.at[k, j], pair_send, pair_recv.at[k, j], here.flip_rep(bit))
                give.start()
                give.wait()
                bring = pltpu.make_async_copy(pair_buf.at[k, j], pair_tmp, pair_local)
                bring.start()
                bring.wait()
                fin[slot] = fin[slot] + pair_tmp[...]
            o_keep(k).start()
            o_give(k).start()

    def vec_copy(i):
        target_r, target_g = here.flip_rep(0)
        for b in range(1, rep_bits):
            other = here.flip_rep(b)
            target_r = jnp.where(i == b, other[0], target_r)
            target_g = jnp.where(i == b, other[1], target_g)
        for b in range(grp_bits):
            other = here.flip_grp(b)
            target_r = jnp.where(i == rep_bits + b, other[0], target_r)
            target_g = jnp.where(i == rep_bits + b, other[1], target_g)
        return remote(vec_buf.at[i], vec_got.at[i], vec_send.at[i], vec_recv.at[i], (target_r, target_g))

    vec_buf[0] = vec_ref[...]
    vec_copy(0).start()

    def body(t, carry):
        @pl.when(t < N)
        def _():
            multiply(t)

        @pl.when((t >= 1) & (t < N + 1))
        def _():
            after_x(t - 1)

        @pl.when((t >= 2) & (t < N + 2))
        def _():
            after_y(t - 2)

        @pl.when((t >= 3) & (t < N + 3))
        def _():
            after_z(t - 3)

        @pl.when((t >= 4) & (t < N + 4))
        def _():
            finish(t - 4)

        @pl.when(t < rounds)
        def _():
            vec_copy(t).wait_recv()
            vec_buf[t + 1] = vec_buf[t] + vec_got[t]

            @pl.when(t + 1 < rounds)
            def _():
                vec_copy(t + 1).start()

        return carry

    lax.fori_loop(0, N + 4, body, 0)
    vec_out[...] = vec_buf[rounds]

    def settle(k, carry):
        def each(zz, carry):
            x_copy(k, zz).wait_send()

            @pl.when(y != c)
            def _():
                y_copy(k, zz).wait_send()

            @pl.when(sink & (zz > z))
            def _():
                up_copy(k, zz).wait_send()

            @pl.when(sink & (zz < z))
            def _():
                down_copy(k, zz).wait_send()

            return carry

        lax.fori_loop(0, Z, each, 0)

        @pl.when(sink)
        def _():
            f_copy(k).wait_send()

            @pl.when(k >= N - 2)
            def _():
                o_keep(k).wait()
                o_give(k).wait_send()

        @pl.when(y != c)
        def _():
            o_give(k).wait_recv()

        return carry

    lax.fori_loop(0, N, settle, 0)
    for i in range(D_N):
        dy_swap(i).wait_send()
    for i in range(X_N):
        x_swap(i).wait_send()
    for i in range(rounds):
        vec_copy(i).wait_send()


def reduce_all(dy, xs, vec, con_count, exp_count, N, R, G):
    D_N, _, _, n, T = dy.shape
    X_N, _, K = xs.shape
    Z = G // YSIZE
    share = (5 * n // 17) // 8 * 8
    width = n - share
    dma = pltpu.SemaphoreType.DMA
    rounds = bits_of(R) + bits_of(G)
    pairs = max(bits_of(R) - 2, 1)
    deep = bits_of(R) > 2
    bf16, f32 = jnp.bfloat16, jnp.float32
    hbm = pl.BlockSpec(memory_space=pl.ANY)
    vmem = pl.BlockSpec(memory_space=pltpu.VMEM)
    out, vec_sum, _ = pl.pallas_call(
        functools.partial(reduce_kernel, R, G, share, con_count, exp_count),
        out_shape=(
            jax.ShapeDtypeStruct((N, n, K), f32),
            jax.ShapeDtypeStruct(vec.shape, f32),
            jax.ShapeDtypeStruct((N, pairs, n, K) if deep else (1, 1, 8, 128), f32),
        ),
        in_specs=[hbm, hbm, vmem],
        out_specs=(hbm, vmem, hbm),
        scratch_shapes=[
            pltpu.VMEM((D_N, Z, n, T), bf16),
            pltpu.VMEM((D_N, Z, n, T), bf16),
            pltpu.VMEM((X_N, T, K), bf16),
            pltpu.VMEM((X_N, T, K), bf16),
            pltpu.VMEM((N, Z, width, K), bf16),
            pltpu.VMEM((N, Z, share, K), bf16),
            pltpu.VMEM((N, Z, share, K), bf16),
            pltpu.VMEM((N, Z, width, K), bf16),
            pltpu.VMEM((N, Z + 1, width, K), bf16),
            pltpu.VMEM((N, width, K), bf16),
            pltpu.VMEM((2, n, K), f32),
            pltpu.VMEM((n, K) if deep else (8, 128), f32),
            pltpu.VMEM((rounds + 1,) + vec.shape, f32),
            pltpu.VMEM((rounds,) + vec.shape, f32),
            dma((D_N,)),
            dma((X_N,)),
            dma((D_N,)),
            dma((D_N,)),
            dma((X_N,)),
            dma((X_N,)),
            dma((N, Z)),
            dma((N, Z)),
            dma((N, Z)),
            dma((N, Z)),
            dma((N, Z)),
            dma((N, Z + 1)),
            dma((N,)),
            dma((N,)),
            dma((N,)),
            dma((N,)),
            dma((N,)),
            dma,
            dma((N, pairs)),
            dma,
            dma((rounds,)),
            dma((rounds,)),
        ],
        compiler_params=pltpu.CompilerParams(collective_id=1, has_side_effects=True, vmem_limit_bytes=VMEM_LIMIT),
        name="reduce_all",
    )(dy, xs, vec)
    return out, vec_sum


def dot_nt(left, right):
    return lax.dot_general(left, right, (((1,), (1,)), ((), ())), preferred_element_type=jnp.float32)


def per_device(
    tokens,
    document_lengths,
    cotangent,
    first_gain,
    first_shift,
    attention_in,
    query_bias,
    value_bias,
    attention_out,
    output_bias,
    second_gain,
    second_shift,
    expand_weight,
    expand_bias,
    contract_weight,
    contract_bias,
):
    R, G = lax.axis_size("rep"), lax.axis_size("grp")
    T, D = tokens.shape
    H = D // HD
    n = D // G
    FF = contract_weight.shape[0]
    Q = FF // D
    bf16, f32 = jnp.bfloat16, jnp.float32
    valid, labels = document_layout(document_lengths[0], T)

    own = jnp.concatenate(
        [
            attention_in.T.reshape(3, n, D),
            attention_out.T.reshape(1, n, D),
            expand_weight.T.reshape(Q, n, D),
            jnp.swapaxes(contract_weight.reshape(Q, D, n), 1, 2),
        ],
        axis=0,
    )
    N = own.shape[0]
    parts = [
        first_gain,
        first_shift,
        query_bias,
        value_bias,
        output_bias,
        second_gain,
        second_shift,
        contract_bias,
        expand_bias,
    ]
    flat = jnp.concatenate(parts)
    rows = -(-flat.shape[0] // (8 * 128)) * 8
    small = jnp.pad(flat, (0, rows * 128 - flat.shape[0])).reshape(rows, 128)
    gathered, small_all = gather_all(own, small, R, G)
    small_all = small_all.reshape(G, rows * 128)
    full = []
    at = 0
    for part in parts:
        full.append(small_all[:, at : at + part.shape[0]].reshape(-1).astype(f32))
        at += part.shape[0]
    gain_one, shift_one, bias_query, bias_value, bias_output, gain_two, shift_two, bias_contract, bias_expand = full
    in_t = gathered[:, 0:3].reshape(3 * D, D)
    out_t = gathered[:, 3].reshape(D, D)
    exp_t = gathered[:, 4 : 4 + Q].reshape(Q, D, D)
    con_t = jnp.swapaxes(gathered[:, 4 + Q :], 0, 1).reshape(Q, D, D)

    normed_one, inverse_one, hidden_one = layer_norm(tokens, gain_one, shift_one)
    hidden_one = hidden_one.astype(bf16)
    bias_all = jnp.concatenate([bias_query, jnp.zeros((D,), f32), bias_value])
    projected = (dot_nt(hidden_one, in_t) + bias_all).astype(bf16)
    heads = projected.reshape(T, 3, H, HD)
    query, keyset, valueset = heads[:, 0], heads[:, 1], heads[:, 2]
    positions = jnp.arange(T, dtype=jnp.int32)
    allowed = (positions[None, :] <= positions[:, None]) & (labels[None, :] == labels[:, None])
    raw = product("qhd,khd->hqk", query, keyset) * HD ** (-0.5)
    scores = jnp.where(allowed[None], raw, MASKED)
    peak = jnp.max(scores, axis=-1, keepdims=True)
    logsum = peak + jnp.log(jnp.sum(jnp.exp(scores - peak), axis=-1, keepdims=True))
    probability = jnp.exp(scores - logsum)
    weights = probability.astype(bf16)
    attended = product("hqk,khd->qhd", weights, valueset).astype(bf16)
    flat_attended = attended.reshape(T, D)
    residual = tokens + dot_nt(flat_attended, out_t) + bias_output
    normed_two, inverse_two, hidden_two = layer_norm(residual, gain_two, shift_two)
    hidden_two = hidden_two.astype(bf16)
    before = product("tk,qnk->qtn", hidden_two, exp_t) + bias_expand.reshape(Q, 1, D)
    activated = jax.nn.gelu(before).astype(bf16)
    output = residual + product("qtk,qnk->tn", activated, con_t) + bias_contract
    live = valid[:, None]
    block_output = jnp.where(live, output, 0.0)
    start = jnp.where(live, cotangent, 0.0)
    start_low = start.astype(bf16)
    _, gelu_back = jax.vjp(jax.nn.gelu, before)
    back_before = gelu_back(product("tn,qnk->qtk", start_low, con_t))[0]
    back_before_low = back_before.astype(bf16)
    back_hidden_two = product("qtn,qnk->tk", back_before_low, exp_t)
    back_residual = start + norm_back(back_hidden_two, normed_two, inverse_two, gain_two)
    back_residual_low = back_residual.astype(bf16)
    back_attended = product("tn,nk->tk", back_residual_low, out_t).astype(bf16).reshape(T, H, HD)
    delta = jnp.sum(back_attended.astype(f32) * attended.astype(f32), axis=-1).T
    flow = product("qhd,khd->hqk", back_attended, valueset)
    slope = (probability * (flow - delta[:, :, None]) * HD ** (-0.5)).astype(bf16)
    back_query = product("hqk,khd->qhd", slope, keyset).reshape(T, D)
    back_key = product("hqk,qhd->khd", slope, query).reshape(T, D)
    back_value = product("hqk,qhd->khd", weights, back_attended).reshape(T, D)
    back_projected = jnp.concatenate([back_query, back_key, back_value], axis=1)
    back_projected_low = back_projected.astype(bf16)
    back_hidden_one = product("tn,nk->tk", back_projected_low, in_t)
    tokens_gradient = back_residual + norm_back(back_hidden_one, normed_one, inverse_one, gain_one)
    vectors = (
        jnp.sum(back_hidden_one * normed_one, axis=0),
        jnp.sum(back_hidden_one, axis=0),
        jnp.sum(back_query, axis=0),
        jnp.sum(back_value, axis=0),
        jnp.sum(back_residual, axis=0),
        jnp.sum(back_hidden_two * normed_two, axis=0),
        jnp.sum(back_hidden_two, axis=0),
        jnp.sum(start, axis=0),
        jnp.sum(back_before, axis=1).reshape(-1),
    )
    Z = G // YSIZE
    before_t = back_before_low.transpose(0, 2, 1).reshape(G, Q, n, T).transpose(1, 0, 2, 3)
    dy = jnp.concatenate(
        [
            start_low.T.reshape(1, G, n, T),
            before_t,
            back_residual_low.T.reshape(1, G, n, T),
            back_projected_low.T.reshape(G, 3, n, T).transpose(1, 0, 2, 3),
        ],
        axis=0,
    ).reshape(-1, Z, YSIZE, n, T)
    xs = jnp.concatenate([activated, hidden_two[None], flat_attended[None], hidden_one[None]], axis=0)
    flat_vec = jnp.concatenate(vectors)
    vec_rows = -(-flat_vec.shape[0] // (8 * 128)) * 8
    vec = jnp.pad(flat_vec, (0, vec_rows * 128 - flat_vec.shape[0])).reshape(vec_rows, 128)
    grads, vec_sum = reduce_all(dy, xs, vec, Q, Q, N, R, G)
    vec_sum = vec_sum.reshape(-1)
    place = lax.axis_index("grp")
    shares = []
    at = 0
    for vector in vectors:
        size = vector.shape[0]
        shares.append(lax.dynamic_slice_in_dim(vec_sum, at + place * (size // G), size // G))
        at += size
    con_grad = jnp.swapaxes(grads[0:Q], 1, 2).reshape(FF, n)
    exp_grad = grads[Q : 2 * Q].reshape(Q * n, D).T
    out_grad = grads[2 * Q].T
    in_grad = grads[2 * Q + 1 :].reshape(3 * n, D).T
    return (
        block_output,
        tokens_gradient,
        shares[0],
        shares[1],
        in_grad,
        shares[2],
        shares[3],
        out_grad,
        shares[4],
        shares[5],
        shares[6],
        exp_grad,
        shares[8],
        con_grad,
        shares[7],
    )


def solution(mesh):
    rows = P(("rep", "grp"), None)
    split, columns = P("grp"), P(None, "grp")
    return jax.shard_map(
        per_device,
        mesh=mesh,
        in_specs=(
            rows,
            rows,
            rows,
            split,
            split,
            columns,
            split,
            split,
            columns,
            split,
            split,
            split,
            columns,
            split,
            columns,
            split,
        ),
        out_specs=(
            rows,
            rows,
            split,
            split,
            columns,
            split,
            split,
            columns,
            split,
            split,
            split,
            columns,
            split,
            columns,
            split,
        ),
        check_vma=False,
    )
```

```python
import functools
import types

import jax
import jax.numpy as jnp
from jax import lax
from jax.experimental import pallas as pl
from jax.experimental.pallas import tpu as pltpu
from jax.sharding import PartitionSpec as P

HD = 64
EPSILON = 1e-05
MASKED = -1e30
PAD = 8
YSIZE = 2
TEAM = 4
GELU_A = 0.7978845608028654
GELU_B = 0.044715
MESH_ID = pl.DeviceIdType.MESH
VMEM_LIMIT = 67043328
BF16, F32 = jnp.bfloat16, jnp.float32


def bits_of(count):
    return count.bit_length() - 1


def dot_nn(left, right):
    return lax.dot_general(left, right, (((1,), (0,)), ((), ())), preferred_element_type=F32)


def dot_nt(left, right):
    return lax.dot_general(left, right, (((1,), (1,)), ((), ())), preferred_element_type=F32)


def dot_tn(left, right):
    return lax.dot_general(left, right, (((0,), (0,)), ((), ())), preferred_element_type=F32)


def remote(src, dst, send, recv, target):
    return pltpu.make_async_remote_copy(
        src_ref=src, dst_ref=dst, send_sem=send, recv_sem=recv, device_id=target, device_id_type=MESH_ID
    )


def wide(value):
    return value.astype(F32)


def low(value):
    return value.astype(BF16)


class Place:
    def __init__(self, rep_count, grp_count):
        self.R, self.G = rep_count, grp_count
        self.Z = grp_count // YSIZE
        self.r = lax.axis_index("rep")
        self.g = lax.axis_index("grp")
        self.c = self.r % 2
        self.xi = (self.r // 2) % 2
        self.q = self.r % TEAM
        self.z = self.g // YSIZE
        self.y = self.g % YSIZE
        self.partner = (self.r + 1 - 2 * self.c, self.g)
        self.xnbr = (self.r + 2 - 4 * self.xi, self.g)
        self.ynbr = (self.r, self.g + 1 - 2 * self.y)
        self.up = (self.r, self.g + YSIZE)
        self.down = (self.r, self.g - YSIZE)
        self.q_partner = self.q + 1 - 2 * self.c
        self.q_x = self.q + 2 - 4 * self.xi
        self.q_far = self.q_x + 1 - 2 * self.c

    def on_line(self, zz):
        return (self.r, zz * YSIZE + self.y)

    def flip_rep(self, bit):
        on = (self.r // (1 << bit)) % 2
        return (self.r + (1 << bit) - (2 << bit) * on, self.g)

    def flip_grp(self, bit):
        on = (self.g // (1 << bit)) % 2
        return (self.r, self.g + (1 << bit) - (2 << bit) * on)


def greet(here, others):
    barrier = pltpu.get_barrier_semaphore()

    def hello(target):
        pl.semaphore_signal(barrier, inc=1, device_id=target, device_id_type=MESH_ID)

    for target in [here.partner, here.xnbr, here.ynbr] + others:
        hello(target)
    for zz in range(here.Z):

        @pl.when(here.z != zz)
        def _(zz=zz):
            hello(here.on_line(zz))

    pl.semaphore_wait(barrier, 2 + here.Z + len(others))


def loop(count, body):
    def step(i, carry):
        body(i)
        return carry

    lax.fori_loop(0, count, step, 0)


def layer_kernel(R, G, give_in, give_out, names, *refs):
    len_ref, tok_ref, cot_ref, ain_ref, aout_ref, exp_ref, con_ref = refs[:7]
    vector_refs = refs[7:16]
    bo_out, tg_out, grad_out, con_out, vec_out, con_cut, yb_a, zb_a, deep_buf = refs[16:25]
    s = types.SimpleNamespace(**dict(zip(names, refs[25:])))
    here = Place(R, G)
    Z, z, y, c, xi, q, g = here.Z, here.z, here.y, here.c, here.xi, here.q, here.g
    D, T = tok_ref.shape
    n = D // G
    H = D // HD
    Q = TEAM
    FF = con_ref.shape[1]
    n4 = Q * n
    B = 2 * n
    scale = HD ** (-0.5)
    rep_bits, grp_bits = bits_of(R), bits_of(G)
    rounds = rep_bits + grp_bits
    w_io, w_ffn = s.w_io, s.w_ffn
    ioT, xo, xp, projT, resT = s.ioT, s.xo, s.xp, s.projT, s.resT
    h24, st4, brT = s.h24, s.st4, s.brT
    dyp, ps, pS, prb, xrb, accP = s.dyp, s.ps, s.pS, s.prb, s.xrb, s.accP
    lse, maskb, live, vecT = s.lse, s.maskb, s.live, s.vecT
    vec_buf, vec_got = s.vec_buf, s.vec_got
    gk, gs, yb_f, zb_f = s.gk, s.gs, s.yb_f, s.zb_f
    xb, fx, small_all = s.xb, s.fx, s.small_all

    N = 4
    wide_in = n - give_in
    start_in = xi * give_in
    giving = xi * wide_in
    taking = (1 - xi) * wide_in

    def io_row(k, gg):
        return jnp.where(k < 3, 3 * n * gg + n * k, 3 * D + n * gg)

    first_y = (3 * n // 17) // 8 * 8

    def rows(base, offset, size):
        return pl.ds(pl.multiple_of(base + offset, 8), size)

    def plane_w(k, gg):
        return w_io.at[rows(io_row(k, gg), start_in, wide_in), :]

    def gift_w(k, gg):
        return w_io.at[rows(io_row(k, gg), giving, give_in), :]

    def due_w(k, gg):
        return w_io.at[rows(io_row(k, gg), taking, give_in), :]

    def shard(zz, yy):
        return zz * YSIZE + yy

    def farthest(i):
        table = [sorted(range(Z), key=lambda p: -abs(p - at)) for at in range(Z)]
        pick = jnp.int32(0)
        for at in range(Z):
            for j in range(Z):
                pick = jnp.where((z == at) & (i == j), table[at][j], pick)
        return pick

    def goes_on(zz):
        return ((zz < z) & (z < Z - 1)) | ((zz > z) & (z > 0))

    source = y == c
    onward_of = lambda zz: (here.r, g + jnp.where(zz < z, YSIZE, -YSIZE))

    def own_copy(k, way):
        ref = plane_w(k, g)
        return remote(ref, ref, s.a_own.at[k, way], s.a_rp.at[k, z], (here.up, here.down, here.ynbr)[way])

    def passing(k, zz):
        ref = plane_w(k, shard(zz, y))
        return remote(ref, ref, s.a_fwd.at[k, zz], s.a_rp.at[k, zz], onward_of(zz))

    def over_y(k, zz, yy):
        ref = plane_w(k, shard(zz, yy))
        return remote(ref, ref, s.a_y.at[k, zz], s.a_rp.at[k, zz], here.ynbr)

    def over_x(k, zz):
        ref = gift_w(k, shard(zz, c))
        return remote(ref, ref, s.a_x.at[k, zz], s.a_rx.at[k, zz], here.xnbr)

    def x_arrival(k, zz):
        ref = due_w(k, shard(zz, c))
        return remote(ref, ref, s.a_x.at[k, zz], s.a_rx.at[k, zz], here.xnbr)

    def plane_to_partner(k, zz, core):
        ref = plane_w(k, shard(zz, core))
        return remote(ref, ref, s.a_cp.at[k, zz], s.a_rcp.at[k, zz], here.partner)

    def rest_to_partner(k, zz, core):
        ref = due_w(k, shard(zz, core))
        return remote(ref, ref, s.a_cx.at[k, zz], s.a_rcx.at[k, zz], here.partner)

    def ffn_w(mt, gg):
        return w_ffn.at[mt, rows(n * gg, 0, n), :]

    def ffn_own(mt, way):
        ref = ffn_w(mt, g)
        return remote(ref, ref, s.w_own.at[mt, way], s.w_rz.at[mt, z], (here.up, here.down, here.ynbr)[way])

    def ffn_own_y(mt):
        ref = ffn_w(mt, g)
        return remote(ref, ref, s.w_own.at[mt, 2], s.w_ry.at[mt, z], here.ynbr)

    def ffn_pass(mt, zz):
        ref = ffn_w(mt, shard(zz, y))
        return remote(ref, ref, s.w_fwd.at[mt, zz], s.w_rz.at[mt, zz], onward_of(zz))

    def ffn_over_y(mt, zz, yy):
        ref = w_ffn.at[mt, rows(n * shard(zz, yy), 0, n - first_y), :]
        return remote(ref, ref, s.w_y.at[mt, zz], s.w_ry.at[mt, zz], here.ynbr)

    def ffn_own_y_arrival(mt):
        ref = ffn_w(mt, shard(z, 1 - y))
        return remote(ref, ref, s.w_own.at[mt, 2], s.w_ry.at[mt, z], here.ynbr)

    def ffn_edge(mt, zz):
        return w_ffn.at[mt, rows(n * shard(zz, 1 - y), n - first_y, first_y), :]

    def edge_own(mt, way):
        ref = ffn_edge(mt, z)
        return remote(ref, ref, s.u_own.at[mt, way], s.u_rz.at[mt, z], (here.up, here.down)[way])

    def edge_pass(mt, zz):
        ref = ffn_edge(mt, zz)
        return remote(ref, ref, s.u_fwd.at[mt, zz], s.u_rz.at[mt, zz], onward_of(zz))

    def start_own(k):
        @pl.when(source)
        def _():
            @pl.when(z < Z - 1)
            def _():
                own_copy(k, 0).start()

            @pl.when(z > 0)
            def _():
                own_copy(k, 1).start()

            own_copy(k, 2).start()

    def start_ffn(mt):
        @pl.when(z < Z - 1)
        def _():
            ffn_own(mt, 0).start()

        @pl.when(z > 0)
        def _():
            ffn_own(mt, 1).start()

    def start_ffn_y(mt):
        ffn_own_y(mt).start()

    def both_sides(distance, act):
        def side(i):
            zz = z + jnp.where(i == 0, -distance, distance)

            @pl.when((zz >= 0) & (zz < Z) & ((i == 0) | (distance > 0)))
            def _():
                act(zz)

        loop(2, side)

    def gather_wave(d, part):
        def plane_step(j):
            k = 3 * part + j

            @pl.when((k < N) & source & (d > 0))
            def _():
                def arrived(zz):
                    passing(k, zz).wait_recv()

                    @pl.when(goes_on(zz))
                    def _():
                        passing(k, zz).start()

                    over_y(k, zz, y).start()
                    over_x(k, zz).start()
                    plane_to_partner(k, zz, c).start()

                both_sides(d, arrived)

            @pl.when((k < N) & (y != c))
            def _():
                def arrived(zz):
                    over_y(k, zz, c).wait_recv()
                    over_x(k, zz).start()
                    plane_to_partner(k, zz, c).start()

                both_sides(d, arrived)

        def x_step(j):
            k = 3 * part + j

            @pl.when((k < N) & ((d > 1) | ((d > 0) & (y != c))))
            def _():
                def arrived(zz):
                    x_arrival(k, zz).wait_recv()
                    rest_to_partner(k, zz, c).start()

                both_sides(d - 1, arrived)

        loop(3, plane_step)
        loop(3, x_step)

    def partner_arrivals(k):
        def each(zz):
            @pl.when((y == c) | (zz != z))
            def _():
                plane_to_partner(k, zz, 1 - c).wait_recv()
                rest_to_partner(k, zz, 1 - c).wait_recv()

        loop(Z, each)

    def ffn_wave(mt, d):
        def arrived(zz):
            ffn_pass(mt, zz).wait_recv()

            @pl.when(goes_on(zz))
            def _():
                ffn_pass(mt, zz).start()

            ffn_over_y(mt, zz, y).start()

        both_sides(d, arrived)

    def ffn_edges(mt, d):
        @pl.when(d == 0)
        def _():
            ffn_own_y_arrival(mt).wait_recv()

            @pl.when(z < Z - 1)
            def _():
                edge_own(mt, 0).start()

            @pl.when(z > 0)
            def _():
                edge_own(mt, 1).start()

        @pl.when(d > 0)
        def _():
            def arrived(zz):
                edge_pass(mt, zz).wait_recv()

                @pl.when(goes_on(zz))
                def _():
                    edge_pass(mt, zz).start()

            both_sides(d, arrived)

    def ffn_y_arrivals(mt):
        def each(zz):
            @pl.when(zz != z)
            def _():
                ffn_over_y(mt, zz, 1 - y).wait_recv()

        loop(Z, each)

    def share_copy(e, buf, kind):
        slot = (q, q, here.q_x)[kind]
        target = (here.partner, here.xnbr, here.partner)[kind]
        ref = buf.at[slot]
        return remote(ref, ref, s.e_send.at[e, kind], s.e_recv.at[e, kind], target)

    def share_arrival(e, buf, kind):
        slot = (here.q_partner, here.q_x, here.q_far)[kind]
        target = (here.partner, here.xnbr, here.partner)[kind]
        ref = buf.at[slot]
        return remote(ref, ref, s.e_send.at[e, kind], s.e_recv.at[e, kind], target)

    def swap_copy(i):
        return remote(xo.at[i], xp.at[i], s.p_send.at[i], s.p_recv.at[i], here.partner)

    def part_to_partner(e, j):
        return remote(ps.at[j], prb.at[e, j], s.r_send.at[e, j], s.r_recv.at[e, j], here.partner)

    def part_to_x(e):
        return remote(pS, xrb.at[e], s.r_send.at[e, 2], s.r_recv.at[e, 2], here.xnbr)

    def small_copy(bit, mine):
        size = 1 << bit
        base = (g // size) * size
        if not mine:
            base = base + size - 2 * size * ((g // size) % 2)
        ref = small_all.at[rows(n * base, 0, n * size), :]
        return remote(ref, ref, s.s_send.at[bit], s.s_recv.at[bit], here.flip_grp(bit))

    def fy_copy(mt, zz):
        return remote(gs.at[mt, zz], yb_f.at[mt, zz], s.fy_send.at[mt, zz], s.fy_recv.at[mt, zz], here.ynbr)

    def fz_copy(mt, zz):
        return remote(
            gk.at[mt, zz], zb_f.at[mt, z], s.fz_send.at[mt, zz], s.fz_recv.at[mt, z], here.on_line(zz)
        )

    def fz_arrival(mt, zz):
        return remote(
            gk.at[mt, zz], zb_f.at[mt, zz], s.fz_send.at[mt, zz], s.fz_recv.at[mt, zz], here.on_line(zz)
        )

    def piece(mt, which):
        return N + Q * mt + which

    def final_copy(mt, kind):
        target = (here.partner, here.xnbr, here.partner)[kind]
        slot = (q, q, here.q_x)[kind]
        src = grad_out.at[piece(mt, slot)] if kind == 2 else gk.at[mt, z]
        dst = grad_out.at[piece(mt, slot)]
        return remote(src, dst, s.fo_send.at[mt, kind], s.fo_recv.at[mt, kind], target)

    def final_arrival(mt, kind):
        target = (here.partner, here.xnbr, here.partner)[kind]
        slot = (here.q_partner, here.q_x, here.q_far)[kind]
        ref = grad_out.at[piece(mt, slot)]
        return remote(ref, ref, s.fo_send.at[mt, kind], s.fo_recv.at[mt, kind], target)

    def final_keep(mt):
        return pltpu.make_async_copy(gk.at[mt, z], grad_out.at[piece(mt, q)], s.fo_keep.at[mt])

    def deepen(ref, k):
        for bit in range(2, rep_bits):
            j = bit - 2
            give = remote(ref, deep_buf.at[k, j], s.d_send, s.d_recv.at[k, j], here.flip_rep(bit))
            give.start()
            give.wait()
            bring = pltpu.make_async_copy(deep_buf.at[k, j], s.d_tmp, s.d_local)
            bring.start()
            bring.wait()
            ref[...] = low(wide(ref[...]) + wide(s.d_tmp[...]))

    def ffn_grads(mt, left, right):
        def block(b):
            at = pl.ds(pl.multiple_of(b * B, 16), B)
            total = dot_nt(left[0, at, :], right[0])
            for t in range(1, Q):
                total = total + dot_nt(left[t, at, :], right[t])

            @pl.when(y == 0)
            def _():
                gk[mt, b] = low(total[:n])
                gs[mt, b] = low(total[n:])

            @pl.when(y == 1)
            def _():
                gk[mt, b] = low(total[n:])
                gs[mt, b] = low(total[:n])

            fy_copy(mt, b).start()

        loop(Z, lambda i: block(farthest(i)))

    def ffn_reduce_y(mt, i):
        zz = farthest(i)
        fy_copy(mt, zz).wait_recv()
        gk[mt, zz] = low(wide(gk[mt, zz]) + wide(yb_f[mt, zz]))

        @pl.when(zz != z)
        def _():
            fz_copy(mt, zz).start()

    def ffn_reduce_own(mt):
        total = wide(gk[mt, z])
        for i in range(Z - 1):
            zz = farthest(i)
            fz_arrival(mt, zz).wait_recv()
            total = total + wide(zb_f[mt, zz])
        gk[mt, z] = low(total)
        deepen(gk.at[mt, z], piece(mt, 0))
        final_keep(mt).start()
        final_copy(mt, 0).start()
        final_copy(mt, 1).start()

    def ffn_reduce_far(mt):
        final_arrival(mt, 1).wait_recv()
        final_copy(mt, 2).start()

    def column(j, at=None):
        block = small_all[: D] if at is None else small_all[at, :]
        return wide(block)[:, j : j + 1]

    def statistics(values):
        center = values - jnp.mean(values, axis=0, keepdims=True)
        inverse = lax.rsqrt(jnp.mean(center * center, axis=0, keepdims=True) + EPSILON)
        return center * inverse, inverse

    def norm_back(upstream, normed, inverse, gain):
        scaled = upstream * gain
        return inverse * (
            scaled
            - jnp.mean(scaled, axis=0, keepdims=True)
            - normed * jnp.mean(scaled * normed, axis=0, keepdims=True)
        )

    def total_of(values):
        return jnp.sum(values, axis=1, keepdims=True)

    extra = [here.flip_rep(b) for b in range(2, rep_bits)]

    def schedule(steps):
        def body(at):
            for act in dict.fromkeys(step[0] for step in steps):
                slots = [(i, step[1:]) for i, step in enumerate(steps) if step[0] is act]
                hit = at == slots[0][0]
                for i, _ in slots[1:]:
                    hit = hit | (at == i)

                @pl.when(hit)
                def _(act=act, slots=slots):
                    picked = []
                    for j in range(len(slots[0][1])):
                        values = [args[j] for _, args in slots]
                        pick = jnp.int32(values[0])
                        if len(set(values)) > 1:
                            for (i, _), value in zip(slots[1:], values[1:]):
                                pick = jnp.where(at == i, value, pick)
                        picked.append(pick)
                    act(*picked)

        loop(len(steps), body)

    local = s.l_sem

    def pull_io(ref, i):
        return pltpu.make_async_copy(ref, ioT, local.at[i])

    def opening(raw_con, turned, cut, piece_con, raw_cot, small_rows, small_own):
        put_in = pltpu.make_async_copy(ain_ref, w_io.at[rows(3 * n * g, 0, 3 * n), :], local.at[0])
        put_out = pltpu.make_async_copy(aout_ref, w_io.at[rows(3 * D + n * g, 0, n), :], local.at[1])
        put_exp = pltpu.make_async_copy(
            exp_ref.at[rows(n * q, 0, n), :], w_ffn.at[0, rows(n * g, 0, n), :], local.at[2]
        )
        pull_con = pltpu.make_async_copy(con_ref, raw_con, local.at[3])
        pull_cot = pltpu.make_async_copy(cot_ref, raw_cot, local.at[4])
        pull_tok = pull_io(tok_ref, 5)
        put_in.start()
        put_out.start()
        pull_tok.start()
        put_exp.start()
        pull_cot.start()
        pull_con.start()
        small_rows[...] = jnp.zeros_like(small_rows)
        for j, ref in enumerate(vector_refs[:8]):
            small_rows[j : j + 1, :] = wide(ref[...]).reshape(1, n)
        expand_bias = wide(vector_refs[8][...]).reshape(1, Q * n)
        for j in range(Q):
            small_rows[8 + j : 9 + j, :] = expand_bias[:, j * n : (j + 1) * n]
        small_own[...] = low(small_rows[...].T)
        put_small = pltpu.make_async_copy(small_own, small_all.at[rows(n * g, 0, n), :], s.k_sem.at[0])
        put_small.start()
        greet(here, extra)
        put_in.wait()
        put_small.wait()
        small_copy(0, True).start()
        put_out.wait()
        put_exp.wait()
        ends = []
        end = 0
        for i in range(len_ref.shape[1]):
            end = end + len_ref[0, i]
            ends.append(end)

        def labels(position):
            number = jnp.zeros(position.shape, jnp.int32)
            for end in ends:
                number = number + jnp.where(position >= end, 1, 0)
            return jnp.where(position < ends[-1], number, len(ends) + position)

        def small_rounds(bit):
            for b in range(grp_bits):

                @pl.when(bit == b)
                def _(b=b):
                    small_copy(b, False).wait_recv()
                    if b + 1 < grp_bits:
                        small_copy(b + 1, True).start()

        def layout():
            query_slot = lax.broadcasted_iota(jnp.int32, (1, T), 1)
            key_slot = lax.broadcasted_iota(jnp.int32, (T, 1), 0)
            query_label, key_label = labels(query_slot), labels(key_slot)
            allowed = (key_slot <= query_slot) & (key_label == query_label)
            maskb[...] = jnp.where(allowed, 0.0, MASKED)
            live[...] = jnp.where(query_slot < ends[-1], 1.0, 0.0)

        def first_norm():
            pull_tok.wait()
            normed, _ = statistics(ioT[...])
            xo[1] = low(normed * column(0) + column(1))
            swap_copy(1).start()

        def upstream():
            pull_cot.wait()
            start = jnp.where(live[...] > 0.5, raw_cot[...], 0.0)
            st4[q] = low(start)
            vecT[...] = jnp.zeros_like(vecT)
            vecT[:, 7:8] = total_of(start)

        def share_start():
            share_copy(0, st4, 0).start()
            share_copy(0, st4, 1).start()

        def pass_start():
            share_arrival(0, st4, 1).wait_recv()
            share_copy(0, st4, 2).start()

        def con_block(gg):
            return pltpu.make_async_copy(
                turned.at[rows(Q * n * gg, n * q, n), :], cut.at[rows(n * gg, 0, n), :], s.k_sem.at[gg]
            )

        def cut_contract():
            pull_con.wait()
            turned[:FF] = raw_con[...].T
            loop(G, lambda gg: con_block(gg).start())
            loop(G, lambda gg: con_block(gg).wait())
            piece_con[...] = cut[:D].T
            put = pltpu.make_async_copy(piece_con, w_ffn.at[1, rows(n * g, 0, n), :], local.at[3])
            put.start()
            put.wait()

        def project():
            def block(b):
                at = pl.ds(pl.multiple_of(b * B, 16), B)
                projT[at, :] = low(dot_nn(w_io[at, :], xo[1]))

            def add_bias(first, j):
                def each(b):
                    at = pl.ds(pl.multiple_of(b * B, 16), B)
                    to = pl.ds(pl.multiple_of(first + b * B, 16), B)
                    projT[to, :] = low(dot_nn(w_io[to, :], xo[1]) + column(j, at))

                loop(D // B, each)

            add_bias(0, 2)
            loop(D // B, lambda b: block(b + D // B))
            add_bias(2 * D, 3)

        def head_forward(h):
            at = pl.multiple_of(h * HD, HD)
            query = projT[pl.ds(at, HD), :]
            key = projT[pl.ds(pl.multiple_of(D + at, HD), HD), :]
            value = projT[pl.ds(pl.multiple_of(2 * D + at, HD), HD), :]
            scores = dot_nn(low(wide(key).T), query) * scale + maskb[...]
            peak = jnp.max(scores, axis=0, keepdims=True)
            logsum = peak + jnp.log(jnp.sum(jnp.exp(scores - peak), axis=0, keepdims=True))
            lse[h] = logsum
            weights = low(jnp.exp(scores - logsum))
            xo[0, pl.ds(at, HD), :] = low(dot_nn(value, weights))

        steps = [(start_own, k) for k in range(3)] + [(small_rounds, 0), (layout,)]
        steps += [(gather_wave, 0, 0), (start_own, 3), (gather_wave, 1, 0), (small_rounds, 1), (cut_contract,)]
        steps += [(gather_wave, 2, 0), (start_ffn, 0)] + [(small_rounds, b) for b in range(2, grp_bits)]
        steps += [(first_norm,)] + [(gather_wave, i, 0) for i in range(3, Z)] + [(gather_wave, 0, 1), (gather_wave, 1, 1)]
        steps += [(start_ffn_y, 0), (gather_wave, Z, 0), (upstream,), (gather_wave, 2, 1)]
        steps += [(partner_arrivals, k) for k in range(3)] + [(ffn_wave, 0, 1), (gather_wave, 3, 1)]
        steps += [(project,), (ffn_edges, 0, 0), (gather_wave, 4, 1), (share_start,)]
        served = {
            2: [(ffn_wave, 0, 2)],
            5: [(ffn_edges, 0, 1)],
            8: [(start_ffn, 1)],
            10: [(ffn_edges, 0, 2)],
            13: [(ffn_wave, 0, 3), (start_ffn_y, 1)],
            15: [(ffn_edges, 0, 3)],
            16: [(pass_start,)],
        }
        for h in range(H):
            steps += [(head_forward, h)] + served.get(h, [])
        schedule(steps)

    pl.run_scoped(
        opening,
        pltpu.VMEM((n, FF), BF16),
        pltpu.VMEM((FF + PAD, n), BF16),
        pltpu.VMEM((D + PAD, n), BF16),
        pltpu.VMEM((n, D), BF16),
        pltpu.VMEM((D, T), F32),
        pltpu.VMEM((128, n), F32),
        pltpu.VMEM((n, 128), BF16),
    )
    swap_copy(0).start()
    partner_arrivals(3)

    def attention_out(b):
        at = pl.ds(pl.multiple_of(b * B, 16), B)
        to = pl.ds(pl.multiple_of(3 * D + b * B, 16), B)
        resT[at, :] = ioT[at, :] + dot_nn(w_io[to, :], xo[0]) + column(4, at)

    loop(D // B, attention_out)
    pull_io(cot_ref, 5).start()
    normed, _ = statistics(resT[...])
    h24[q] = low(normed * column(5) + column(6))
    share_copy(1, h24, 0).start()
    share_copy(1, h24, 1).start()

    def dy_rows(k, zz, core):
        gg = shard(zz, core)
        row = jnp.where(k == 0, 3 * D + n * gg, 3 * n * gg + n * (k - 1))
        return rows(row, 0, n)

    def dy_swap(k, zz):
        return remote(
            projT.at[dy_rows(k, zz, 1 - c), :],
            dyp.at[k, zz],
            s.dy_send.at[k, zz],
            s.dy_recv.at[k, zz],
            here.partner,
        )

    def middle(gp4, act4, bb4):
        def expand(t):
            def block(b):
                at = pl.ds(pl.multiple_of(b * B, 16), B)
                part = wide(small_all[at, :])
                bias = part[:, 8:9]
                for j in range(1, Q):
                    bias = jnp.where(q == j, part[:, 8 + j : 9 + j], bias)
                u = dot_nn(w_ffn[0, at, :], h24[t]) + bias
                th = jnp.tanh(GELU_A * (u + GELU_B * (u * u * u)))
                act4[t, at, :] = low(0.5 * u * (1.0 + th))
                gp4[t, at, :] = 0.5 * (1.0 + th) + (0.5 * GELU_A) * u * (1.0 - th * th) * (
                    1.0 + (3.0 * GELU_B) * (u * u)
                )

            loop(D // B, block)

        def expand_step(i):
            @pl.when(i == 1)
            def _():
                share_arrival(1, h24, 0).wait_recv()

            @pl.when(i == 2)
            def _():
                share_arrival(1, h24, 1).wait_recv()
                share_copy(1, h24, 2).start()

            @pl.when(i == 3)
            def _():
                share_arrival(1, h24, 2).wait_recv()

            expand(member(i))

        def gradients():
            share_arrival(0, st4, 0).wait_recv()
            share_arrival(0, st4, 2).wait_recv()
            ffn_grads(1, st4, act4)

        def member(i):
            first = jnp.where(i == 1, here.q_partner, q)
            return jnp.where(i == 2, here.q_x, jnp.where(i == 3, here.q_far, first))

        def back_step(i):
            t = member(Q - 1 - i)

            def block(b):
                at = pl.ds(pl.multiple_of(b * B, 16), B)
                value = accP[at, :] * gp4[t, at, :]
                bb4[t, at, :] = low(value)
                vecT[at, 12:13] = vecT[at, 12:13] + total_of(value)

            accP[...] = dot_tn(w_ffn[1, :D], st4[t])
            loop(D // B, block)
            accP[...] = dot_tn(w_ffn[0, :D], bb4[t])

            @pl.when(i == 0)
            def _():
                ps[1] = low(accP[...])
                part_to_partner(0, 1).start()

            @pl.when(i == 1)
            def _():
                part_to_partner(0, 1).wait_recv()
                pS[...] = low(accP[...] + wide(prb[0, 1]))
                part_to_x(0).start()

            @pl.when(i == 2)
            def _():
                ps[0] = low(accP[...])
                part_to_partner(0, 0).start()

        def expand_gradients():
            ffn_grads(0, bb4, h24)
            for j in range(2):
                part_to_partner(0, j).wait_send()

        def out_step(i):
            t = member(Q - 1 - i)
            brT[...] = dot_nn(w_ffn[1, :D], act4[t])

            @pl.when(i == 0)
            def _():
                ps[1] = low(brT[...])
                part_to_partner(1, 1).start()

            @pl.when(i == 1)
            def _():
                gp4[1] = brT[...]

            @pl.when(i == 2)
            def _():
                ps[0] = low(brT[...])
                part_to_partner(1, 0).start()

            @pl.when(i == 3)
            def _():
                gp4[0] = brT[...]

        steps = [(ffn_wave, 1, 1), (ffn_y_arrivals, 0), (expand_step, 0), (ffn_wave, 1, 2), (expand_step, 1)]
        steps += [(ffn_edges, 1, 0), (ffn_wave, 1, 3), (expand_step, 2), (ffn_edges, 1, 1), (expand_step, 3)]
        steps += [(ffn_edges, 1, 2), (gradients,), (ffn_edges, 1, 3), (ffn_y_arrivals, 1)]
        steps += [(back_step, 0), (back_step, 1), (ffn_reduce_y, 1, 0), (back_step, 2), (ffn_reduce_y, 1, 1)]
        steps += [(back_step, 3), (expand_gradients,), (ffn_reduce_y, 1, 2)] + [(out_step, i) for i in range(Q)]
        steps += [(ffn_reduce_y, 1, 3)]
        schedule(steps)
        part_to_partner(0, 0).wait_recv()
        part_to_x(0).wait_recv()
        back_hidden = accP[...] + wide(prb[0, 0]) + wide(xrb[0])
        normed, inverse = statistics(resT[...])
        vecT[:, 5:6] = total_of(back_hidden * normed)
        vecT[:, 6:7] = total_of(back_hidden)
        pull_io(cot_ref, 5).wait()
        start = jnp.where(live[...] > 0.5, ioT[...], 0.0)
        brT[...] = start + norm_back(back_hidden, normed, inverse, column(5))
        projT[pl.ds(3 * D, D), :] = low(brT[...])
        loop(Z, lambda zz: dy_swap(0, zz).start())
        pull_io(tok_ref, 5).start()
        part_to_x(0).wait_send()
        part_to_partner(1, 1).wait_recv()
        pS[...] = low(gp4[1] + wide(prb[1, 1]))
        part_to_x(1).start()
        resT[...] = resT[...] + gp4[0] + column(7)
        vecT[:, 4:5] = total_of(brT[...])

    pl.run_scoped(
        middle, pltpu.VMEM((Q, D, T), F32), pltpu.VMEM((Q, D, T), BF16), pltpu.VMEM((Q, D, T), BF16)
    )
    batt = xrb.at[0]
    batt[...] = low(dot_tn(w_io[pl.ds(3 * D, D), :], projT[pl.ds(3 * D, D), :]))

    def head_backward(h):
        at = pl.multiple_of(h * HD, HD)
        at_q = pl.ds(at, HD)
        at_k = pl.ds(pl.multiple_of(D + at, HD), HD)
        at_v = pl.ds(pl.multiple_of(2 * D + at, HD), HD)
        query, key, value, up = projT[at_q, :], projT[at_k, :], projT[at_v, :], batt[at_q, :]
        scores = dot_nn(low(wide(key).T), query) * scale + maskb[...]
        probability = jnp.exp(scores - lse[h])
        weights = low(probability)
        delta = jnp.sum(wide(up) * wide(xo[0, at_q, :]), axis=0, keepdims=True)
        flow = dot_nn(low(wide(value).T), up)
        slope = low(probability * (flow - delta) * scale)
        back_query = dot_nn(key, slope)
        back_value = dot_nt(up, weights)
        vecT[at_q, 2:3] = total_of(back_query)
        vecT[at_q, 3:4] = total_of(back_value)
        projT[at_k, :] = low(dot_nt(query, slope))
        projT[at_q, :] = low(back_query)
        projT[at_v, :] = low(back_value)

    wide_out = n - give_out

    def closing(plane, xs, stage, fin, con_in, con_turn, con_tall, con_flat, vec_own):
        def x_copy(k, zz):
            return remote(xs.at[k, zz], xb.at[k, zz], s.gx_send.at[k, zz], s.gx_recv.at[k, zz], here.xnbr)

        def y_copy(k, zz):
            return remote(plane.at[k, zz], yb_a.at[k, zz], s.gy_send.at[k, zz], s.gy_recv.at[k, zz], here.ynbr)

        def z_copy(k, zz):
            return remote(
                plane.at[k, zz], zb_a.at[k, z], s.gz_send.at[k, zz], s.gz_recv.at[k, z], here.on_line(zz)
            )

        def z_arrival(k, zz):
            return remote(
                plane.at[k, zz], zb_a.at[k, zz], s.gz_send.at[k, zz], s.gz_recv.at[k, zz], here.on_line(zz)
            )

        def f_copy(k):
            return remote(plane.at[k, z], fx.at[k], s.gf_send.at[k], s.gf_recv.at[k], here.xnbr)

        def o_keep(k):
            return pltpu.make_async_copy(fin.at[k % 2], grad_out.at[k], s.go_keep.at[k])

        def o_give(k):
            return remote(fin.at[k % 2], grad_out.at[k], s.go_send.at[k], s.go_recv.at[k], here.partner)

        def bring(src, slot):
            copy = pltpu.make_async_copy(src, stage.at[slot], s.st_sem.at[slot])
            copy.start()
            return copy

        def multiply(k):
            j = jnp.where(k == 0, 0, 1)

            @pl.when(k == 0)
            def _():
                swap_copy(0).wait_recv()
                swap_copy(1).wait_recv()


            def each(i):
                zz = farthest(i)
                dy_swap(k, zz).wait_recv()
                term = dot_nt(projT[dy_rows(k, zz, c), :], xo[j]) + dot_nt(dyp[k, zz], xp[j])

                @pl.when(xi == 0)
                def _():
                    plane[k, zz] = low(term[:wide_out])
                    xs[k, zz] = low(term[wide_out:])

                @pl.when(xi == 1)
                def _():
                    plane[k, zz] = low(term[give_out:])
                    xs[k, zz] = low(term[:give_out])

                x_copy(k, zz).start()

            loop(Z, each)

        def after_x(k):
            def each(i):
                zz = farthest(i)
                x_copy(k, zz).wait_recv()
                got = wide(xb[k, zz])

                @pl.when(xi == 0)
                def _():
                    plane[k, zz, :give_out] = low(wide(plane[k, zz, :give_out]) + got)

                @pl.when(xi == 1)
                def _():
                    edge = wide_out - give_out
                    plane[k, zz, edge:] = low(wide(plane[k, zz, edge:]) + got)

                @pl.when(y != c)
                def _():
                    y_copy(k, zz).start()

            loop(Z, each)

        def after_y(k):
            @pl.when(source)
            def _():
                def fetch(i):
                    zz = farthest(i)
                    y_copy(k, zz).wait_recv()
                    bring(yb_a.at[k, zz], i)

                def add(i):
                    zz = farthest(i)
                    pltpu.make_async_copy(yb_a.at[k, zz], stage.at[i], s.st_sem.at[i]).wait()
                    plane[k, zz] = low(wide(plane[k, zz]) + wide(stage[i]))

                    @pl.when(i < Z - 1)
                    def _():
                        z_copy(k, zz).start()

                def step(i):
                    @pl.when(i < Z)
                    def _():
                        fetch(i)

                    @pl.when(i > 0)
                    def _():
                        add(i - 1)

                loop(Z + 1, step)

        def after_z(k):
            @pl.when(source)
            def _():
                def fetch(i):
                    zz = farthest(i)
                    z_arrival(k, zz).wait_recv()
                    bring(zb_a.at[k, zz], i)

                def arrived(i):
                    zz = farthest(i)
                    pltpu.make_async_copy(zb_a.at[k, zz], stage.at[i], s.st_sem.at[i]).wait()

                loop(Z - 1, fetch)
                loop(Z - 1, arrived)
                total = wide(plane[k, z])
                for i in range(Z - 1):
                    total = total + wide(stage[i])
                plane[k, z] = low(total)
                f_copy(k).start()

        def finish(k):
            @pl.when(source)
            def _():
                f_copy(k).wait_recv()

                @pl.when(k >= 2)
                def _():
                    o_keep(k - 2).wait()
                    o_give(k - 2).wait_send()

                slot = k % 2

                def assemble(first, second):
                    fin[slot, :give_out] = first[:give_out]
                    fin[slot, give_out:wide_out] = low(
                        wide(first[give_out:]) + wide(second[: wide_out - give_out])
                    )
                    fin[slot, wide_out:] = second[wide_out - give_out :]

                @pl.when(xi == 0)
                def _():
                    assemble(plane[k, z], fx[k])

                @pl.when(xi == 1)
                def _():
                    assemble(fx[k], plane[k, z])

                deepen(fin.at[slot], k)
                o_keep(k).start()
                o_give(k).start()

        def vec_copy(i):
            target_r, target_g = here.flip_rep(0)
            for b in range(1, rep_bits):
                other = here.flip_rep(b)
                target_r = jnp.where(i == b, other[0], target_r)
                target_g = jnp.where(i == b, other[1], target_g)
            for b in range(grp_bits):
                other = here.flip_grp(b)
                target_r = jnp.where(i == rep_bits + b, other[0], target_r)
                target_g = jnp.where(i == rep_bits + b, other[1], target_g)
            return remote(
                vec_buf.at[i], vec_got.at[i], s.v_send.at[i], s.v_recv.at[i], (target_r, target_g)
            )

        def swap_all():
            for k in range(1, N):
                loop(Z, lambda zz, k=k: dy_swap(k, zz).start())

        def last_norm():
            back_hidden = dot_tn(w_io[pl.ds(0, 3 * D), :], projT[: 3 * D])
            pull_io(tok_ref, 5).wait()
            normed, inverse = statistics(ioT[...])
            vecT[:, 0:1] = total_of(back_hidden * normed)
            vecT[:, 1:2] = total_of(back_hidden)
            accP[...] = brT[...] + norm_back(back_hidden, normed, inverse, column(0))
            tg_copy.start()
            spread = vecT[:, 12:13]
            for j in range(Q):
                vecT[:, 8 + j : 9 + j] = jnp.where(q == j, spread, 0.0)
            vec_buf[0] = vecT[...].T[:16]
            vec_copy(0).start()

        tg_copy = pltpu.make_async_copy(accP, tg_out, local.at[1])
        bo_copy = pltpu.make_async_copy(resT, bo_out, local.at[0])
        push_vec = pltpu.make_async_copy(vec_own, vec_out, local.at[2])

        def block_done():
            part_to_partner(1, 0).wait_recv()
            part_to_x(1).wait_recv()
            output = resT[...] + wide(prb[1, 0]) + wide(xrb[1])
            resT[...] = jnp.where(live[...] > 0.5, output, 0.0)
            bo_copy.start()

        def vec_round(t):
            vec_copy(t).wait_recv()
            vec_buf[t + 1] = vec_buf[t] + vec_got[t]

            @pl.when(t + 1 < rounds)
            def _():
                vec_copy(t + 1).start()

            @pl.when(t + 1 == rounds)
            def _():
                vecT[:, :16] = vec_buf[rounds].T
                vec_own[...] = vecT[pl.ds(pl.multiple_of(n * g, 8), n), :].T[:16]
                push_vec.start()

        def bring_piece(j):
            return pltpu.make_async_copy(grad_out.at[piece(1, j)], con_in.at[j % 2], s.k_sem.at[2 * G + j % 2])

        def put_block(j, gg):
            return pltpu.make_async_copy(
                con_turn.at[j % 2, rows(n * gg, 0, n), :],
                con_cut.at[rows(Q * n * gg, n * j, n), :],
                s.k_sem.at[G * (j % 2) + gg],
            )

        def con_finals():
            final_keep(1).wait()
            final_arrival(1, 0).wait_recv()
            final_arrival(1, 2).wait_recv()
            bring_piece(0).start()
            bring_piece(1).start()

        def con_piece(j):
            bring_piece(j).wait()

            @pl.when(j >= 2)
            def _():
                loop(G, lambda gg: put_block(j - 2, gg).wait())

            con_turn[j % 2, :D] = con_in[j % 2].T

            @pl.when(j + 2 < Q)
            def _():
                bring_piece(j + 2).start()

            loop(G, lambda gg: put_block(j, gg).start())

        half_size = FF // 2

        def bring_side(half):
            return pltpu.make_async_copy(
                con_cut.at[rows(half_size * half, 0, half_size), :], con_tall, s.k_sem.at[2 * G + 2]
            )

        def put_side(half):
            to = pl.ds(pl.multiple_of(half_size * half, 128), half_size)
            return pltpu.make_async_copy(con_flat, con_out.at[:, to], s.k_sem.at[2 * G + 3])

        def con_side(i):
            @pl.when(i == 0)
            def _():
                loop(G, lambda gg: put_block(Q - 2, gg).wait())
                loop(G, lambda gg: put_block(Q - 1, gg).wait())
                bring_side(0).start()

            @pl.when(i > 0)
            def _():
                half = i - 1
                bring_side(half).wait()

                @pl.when(half == 1)
                def _():
                    put_side(0).wait()

                con_flat[...] = con_tall[...].T
                put_side(half).start()

                @pl.when(half == 0)
                def _():
                    bring_side(1).start()

        served = {11: [(ffn_reduce_y, 0, 0)]}
        steps = [(multiply, 0)]
        for h in range(H):
            steps += [(head_backward, h)] + served.get(h, [])
        steps += [(swap_all,), (multiply, 1), (ffn_reduce_y, 0, 1), (after_x, 0), (multiply, 2), (multiply, 3)]
        steps += [(after_x, 1), (ffn_reduce_y, 0, 2), (last_norm,), (ffn_reduce_y, 0, 3), (after_x, 2), (after_y, 0)]
        steps += [(ffn_reduce_own, 1), (vec_round, 0), (after_x, 3), (after_z, 0), (vec_round, 1)]
        steps += [(after_y, 1), (finish, 0), (vec_round, 2), (block_done,), (ffn_reduce_far, 1), (ffn_reduce_own, 0)]
        steps += [(after_y, 2), (after_z, 1), (vec_round, 3), (con_finals,), (finish, 1), (con_piece, 0)]
        steps += [(after_y, 3), (con_piece, 1), (after_z, 2), (con_piece, 2), (con_piece, 3)]
        steps += [(after_z, 3), (vec_round, 4), (con_side, 0), (finish, 2)]
        steps += [(con_side, 1), (con_side, 2), (ffn_reduce_far, 0), (finish, 3)]
        steps += [(vec_round, t) for t in range(5, rounds)]
        schedule(steps)

        def settle(k):
            @pl.when(source)
            def _():
                @pl.when(z < Z - 1)
                def _():
                    own_copy(k, 0).wait_send()

                @pl.when(z > 0)
                def _():
                    own_copy(k, 1).wait_send()

                own_copy(k, 2).wait_send()

            def each(zz):
                @pl.when((y != c) | (zz != z))
                def _():
                    over_x(k, zz).wait_send()
                    plane_to_partner(k, zz, c).wait_send()
                    rest_to_partner(k, zz, c).wait_send()

                @pl.when(source & (zz != z))
                def _():
                    over_y(k, zz, y).wait_send()

                    @pl.when(goes_on(zz))
                    def _():
                        passing(k, zz).wait_send()

                x_copy(k, zz).wait_send()
                dy_swap(k, zz).wait_send()

                @pl.when(y != c)
                def _():
                    y_copy(k, zz).wait_send()

                @pl.when(source & (zz != z))
                def _():
                    z_copy(k, zz).wait_send()

            loop(Z, each)

            @pl.when(source)
            def _():
                f_copy(k).wait_send()

                @pl.when(k >= N - 2)
                def _():
                    o_keep(k).wait()
                    o_give(k).wait_send()

            @pl.when(y != c)
            def _():
                o_give(k).wait_recv()

        loop(N, settle)

        def settle_ffn(mt):
            @pl.when(z < Z - 1)
            def _():
                ffn_own(mt, 0).wait_send()
                edge_own(mt, 0).wait_send()

            @pl.when(z > 0)
            def _():
                ffn_own(mt, 1).wait_send()
                edge_own(mt, 1).wait_send()


            ffn_own_y(mt).wait_send()

            def each(zz):
                fy_copy(mt, zz).wait_send()

                @pl.when(zz != z)
                def _():
                    ffn_over_y(mt, zz, y).wait_send()

                    @pl.when(goes_on(zz))
                    def _():
                        ffn_pass(mt, zz).wait_send()
                        edge_pass(mt, zz).wait_send()

                @pl.when(zz != z)
                def _():
                    fz_copy(mt, zz).wait_send()

            loop(Z, each)

        for mt in range(2):
            settle_ffn(mt)
            for kind in range(3):
                final_copy(mt, kind).wait_send()
        final_keep(0).wait()
        put_side(1).wait()
        final_arrival(0, 0).wait_recv()
        final_arrival(0, 2).wait_recv()
        for e, buf in ((0, st4), (1, h24)):
            for kind in range(3):
                share_copy(e, buf, kind).wait_send()
        for i in range(2):
            swap_copy(i).wait_send()
        for j in range(2):
            part_to_partner(1, j).wait_send()
        part_to_x(1).wait_send()
        for bit in range(grp_bits):
            small_copy(bit, True).wait_send()
        loop(rounds, lambda i: vec_copy(i).wait_send())
        bo_copy.wait()
        tg_copy.wait()
        push_vec.wait()

    pl.run_scoped(
        closing,
        pltpu.VMEM((N, Z, wide_out, D), BF16),
        pltpu.VMEM((N, Z, give_out, D), BF16),
        pltpu.VMEM((Z, wide_out, D), BF16),
        pltpu.VMEM((2, n, D), BF16),
        pltpu.VMEM((2, n, D), BF16),
        pltpu.VMEM((2, D + PAD, n), BF16),
        pltpu.VMEM((FF // 2, n), BF16),
        pltpu.VMEM((n, FF // 2), BF16),
        pltpu.VMEM((16, n), F32),
    )


def run_layer(lengths, tokens, cotangent, a_in, a_out, w_exp, w_con, vectors, R, G):
    D, T = tokens.shape
    FF = w_con.shape[1]
    n = D // G
    H = D // HD
    Z = G // YSIZE
    Q = TEAM
    N = 4
    give_in = (6 * n // 17) // 8 * 8
    give_out = (5 * n // 17) // 8 * 8
    wide_out = n - give_out
    rounds = bits_of(R) + bits_of(G)
    deep = bits_of(R) - 2
    dma = pltpu.SemaphoreType.DMA
    v = pltpu.VMEM
    scratch = dict(
        w_io=v((4 * D + PAD, D), BF16),
        w_ffn=v((2, D + PAD, D), BF16),
        small_all=v((D + PAD, 128), BF16),
        ioT=v((D, T), F32),
        xo=v((2, D, T), BF16),
        xp=v((2, D, T), BF16),
        projT=v((4 * D + PAD, T), BF16),
        resT=v((D, T), F32),
        h24=v((Q, D, T), BF16),
        st4=v((Q, D, T), BF16),
        brT=v((D, T), F32),
        dyp=v((N, Z, n, T), BF16),
        ps=v((2, D, T), BF16),
        pS=v((D, T), BF16),
        prb=v((2, 2, D, T), BF16),
        xrb=v((2, D, T), BF16),
        accP=v((D, T), F32),
        lse=v((H, 1, T), F32),
        maskb=v((T, T), F32),
        live=v((1, T), F32),
        vecT=v((D, 128), F32),
        vec_buf=v((rounds + 1, 16, D), F32),
        vec_got=v((rounds, 16, D), F32),
        gk=v((2, Z, n, D), BF16),
        gs=v((2, Z, n, D), BF16),
        yb_f=v((2, Z, n, D), BF16),
        zb_f=v((2, Z, n, D), BF16),
        xb=v((N, Z, give_out, D), BF16),
        fx=v((N, wide_out, D), BF16),
        d_tmp=v((n, D) if deep > 0 else (8, 128), BF16),
        l_sem=dma((6,)),
        k_sem=dma((2 * G + 4,)),
        a_own=dma((N, 3)),
        w_own=dma((2, 3)),
        e_send=dma((2, 3)),
        e_recv=dma((2, 3)),
        p_send=dma((2,)),
        p_recv=dma((2,)),
        r_send=dma((2, 3)),
        r_recv=dma((2, 3)),
        s_send=dma((bits_of(G),)),
        s_recv=dma((bits_of(G),)),
        v_send=dma((rounds,)),
        v_recv=dma((rounds,)),
        fo_send=dma((2, 3)),
        fo_recv=dma((2, 3)),
        fo_keep=dma((2,)),
        fz_recv=dma((2, Z)),
        gz_recv=dma((N, Z)),
        gf_send=dma((N,)),
        gf_recv=dma((N,)),
        go_keep=dma((N,)),
        go_send=dma((N,)),
        go_recv=dma((N,)),
        st_sem=dma((Z,)),
        d_send=dma,
        d_local=dma,
        d_recv=dma((N + 2 * Q, max(deep, 1))),
        u_own=dma((2, 2)),
        u_rz=dma((2, Z)),
        u_fwd=dma((2, Z)),
        w_rz=dma((2, Z)),
        w_ry=dma((2, Z)),
        w_fwd=dma((2, Z)),
        w_y=dma((2, Z)),
        fy_send=dma((2, Z)),
        fy_recv=dma((2, Z)),
        fz_send=dma((2, Z)),
        a_rp=dma((N, Z)),
        a_rx=dma((N, Z)),
        a_rcp=dma((N, Z)),
        a_rcx=dma((N, Z)),
        a_fwd=dma((N, Z)),
        a_y=dma((N, Z)),
        a_x=dma((N, Z)),
        a_cp=dma((N, Z)),
        a_cx=dma((N, Z)),
        gx_send=dma((N, Z)),
        gx_recv=dma((N, Z)),
        gy_send=dma((N, Z)),
        gy_recv=dma((N, Z)),
        gz_send=dma((N, Z)),
        dy_send=dma((N, Z)),
        dy_recv=dma((N, Z)),
    )
    hbm = pl.BlockSpec(memory_space=pl.ANY)
    outs = pl.pallas_call(
        functools.partial(layer_kernel, R, G, give_in, give_out, tuple(scratch)),
        out_shape=(
            jax.ShapeDtypeStruct((D, T), F32),
            jax.ShapeDtypeStruct((D, T), F32),
            jax.ShapeDtypeStruct((N + 2 * Q, n, D), BF16),
            jax.ShapeDtypeStruct((n, FF), BF16),
            jax.ShapeDtypeStruct((16, n), F32),
            jax.ShapeDtypeStruct((FF, n), BF16),
            jax.ShapeDtypeStruct((N, Z, wide_out, D), BF16),
            jax.ShapeDtypeStruct((N, Z, wide_out, D), BF16),
            jax.ShapeDtypeStruct((N + 2 * Q, deep, n, D) if deep > 0 else (1, 1, 8, 128), BF16),
        ),
        in_specs=[pl.BlockSpec(memory_space=pltpu.SMEM)] + [hbm] * 6 + [pl.BlockSpec(memory_space=pltpu.VMEM)] * 9,
        out_specs=(hbm,) * 9,
        scratch_shapes=list(scratch.values()),
        compiler_params=pltpu.CompilerParams(collective_id=0, has_side_effects=True, vmem_limit_bytes=VMEM_LIMIT),
        name="layer",
    )(lengths, tokens, cotangent, a_in, a_out, w_exp, w_con, *vectors)
    return outs[:5]


def per_device(
    tokens,
    document_lengths,
    cotangent,
    first_gain,
    first_shift,
    attention_in,
    query_bias,
    value_bias,
    attention_out,
    output_bias,
    second_gain,
    second_shift,
    expand_weight,
    expand_bias,
    contract_weight,
    contract_bias,
):
    R, G = lax.axis_size("rep"), lax.axis_size("grp")
    T, D = tokens.shape
    n = D // G
    Q = TEAM
    vectors = [
        first_gain,
        first_shift,
        query_bias,
        value_bias,
        output_bias,
        second_gain,
        second_shift,
        contract_bias,
        expand_bias,
    ]
    block_t, tokens_t, grads, con_grad, share = run_layer(
        document_lengths,
        tokens.T,
        cotangent.T,
        attention_in.T,
        attention_out.T,
        expand_weight.T,
        contract_weight.T,
        vectors,
        R,
        G,
    )
    out_grad = grads[0].T.astype(F32)
    in_grad = grads[1:4].reshape(3 * n, D).T.astype(F32)
    exp_grad = grads[4 : 4 + Q].reshape(Q * n, D).T.astype(F32)
    con_grad = con_grad.T.astype(F32)
    return (
        block_t.T,
        tokens_t.T,
        share[0],
        share[1],
        in_grad,
        share[2],
        share[3],
        out_grad,
        share[4],
        share[5],
        share[6],
        exp_grad,
        share[8 : 8 + Q].reshape(Q * n),
        con_grad,
        share[7],
    )


def solution(mesh):
    rows = P(("rep", "grp"), None)
    split, columns = P("grp"), P(None, "grp")
    return jax.shard_map(
        per_device,
        mesh=mesh,
        in_specs=(
            rows,
            rows,
            rows,
            split,
            split,
            columns,
            split,
            split,
            columns,
            split,
            split,
            split,
            columns,
            split,
            columns,
            split,
        ),
        out_specs=(
            rows,
            rows,
            split,
            split,
            columns,
            split,
            split,
            columns,
            split,
            split,
            split,
            columns,
            split,
            columns,
            split,
        ),
        check_vma=False,
    )
```

```python
import functools
import types

import jax
import jax.numpy as jnp
from jax import lax
from jax.experimental import pallas as pl
from jax.experimental.pallas import tpu as pltpu
from jax.sharding import PartitionSpec as P

HD = 64
EPSILON = 1e-05
MASKED = -1e30
PAD = 8
YSIZE = 2
TEAM = 4
GELU_A = 0.7978845608028654
GELU_B = 0.044715
MESH_ID = pl.DeviceIdType.MESH
VMEM_LIMIT = 67043328
BF16, F32 = jnp.bfloat16, jnp.float32


def bits_of(count):
    return count.bit_length() - 1


def dot_nn(left, right):
    return lax.dot_general(left, right, (((1,), (0,)), ((), ())), preferred_element_type=F32)


def dot_nt(left, right):
    return lax.dot_general(left, right, (((1,), (1,)), ((), ())), preferred_element_type=F32)


def dot_tn(left, right):
    return lax.dot_general(left, right, (((0,), (0,)), ((), ())), preferred_element_type=F32)


def remote(src, dst, send, recv, target):
    return pltpu.make_async_remote_copy(
        src_ref=src, dst_ref=dst, send_sem=send, recv_sem=recv, device_id=target, device_id_type=MESH_ID
    )


def wide(value):
    return value.astype(F32)


def low(value):
    return value.astype(BF16)


class Place:
    def __init__(self, rep_count, grp_count):
        self.R, self.G = rep_count, grp_count
        self.Z = grp_count // YSIZE
        self.r = lax.axis_index("rep")
        self.g = lax.axis_index("grp")
        self.c = self.r % 2
        self.xi = (self.r // 2) % 2
        self.q = self.r % TEAM
        self.z = self.g // YSIZE
        self.y = self.g % YSIZE
        self.partner = (self.r + 1 - 2 * self.c, self.g)
        self.xnbr = (self.r + 2 - 4 * self.xi, self.g)
        self.ynbr = (self.r, self.g + 1 - 2 * self.y)
        self.up = (self.r, self.g + YSIZE)
        self.down = (self.r, self.g - YSIZE)
        self.q_partner = self.q + 1 - 2 * self.c
        self.q_x = self.q + 2 - 4 * self.xi
        self.q_far = self.q_x + 1 - 2 * self.c

    def on_line(self, zz):
        return (self.r, zz * YSIZE + self.y)

    def flip_rep(self, bit):
        on = (self.r // (1 << bit)) % 2
        return (self.r + (1 << bit) - (2 << bit) * on, self.g)

    def flip_grp(self, bit):
        on = (self.g // (1 << bit)) % 2
        return (self.r, self.g + (1 << bit) - (2 << bit) * on)


def greet(here, others):
    barrier = pltpu.get_barrier_semaphore()

    def hello(target):
        pl.semaphore_signal(barrier, inc=1, device_id=target, device_id_type=MESH_ID)

    for target in [here.partner, here.xnbr, here.ynbr] + others:
        hello(target)
    for zz in range(here.Z):

        @pl.when(here.z != zz)
        def _(zz=zz):
            hello(here.on_line(zz))

    pl.semaphore_wait(barrier, 2 + here.Z + len(others))


def loop(count, body):
    def step(i, carry):
        body(i)
        return carry

    lax.fori_loop(0, count, step, 0)


def layer_kernel(R, G, give_in, give_out, names, *refs):
    len_ref, tok_ref, cot_ref, ain_ref, aout_ref, exp_ref, con_ref = refs[:7]
    vector_refs = refs[7:16]
    bo_out, tg_out, in_out, out_out, exp_out, con_out, vec_out, con_raw, con_cut, yb_a, zb_a, deep_buf = refs[16:28]
    s = types.SimpleNamespace(**dict(zip(names, refs[28:])))
    ffn_out = (exp_out, con_raw)
    here = Place(R, G)
    Z, z, y, c, xi, q, g = here.Z, here.z, here.y, here.c, here.xi, here.q, here.g
    D, T = tok_ref.shape
    n = D // G
    H = D // HD
    Q = TEAM
    FF = con_ref.shape[1]
    n4 = Q * n
    B = 2 * n
    scale = HD ** (-0.5)
    rep_bits, grp_bits = bits_of(R), bits_of(G)
    rounds = rep_bits + grp_bits
    w_io, w_ffn = s.w_io, s.w_ffn
    ioT, xo, xp, projT, resT = s.ioT, s.xo, s.xp, s.projT, s.resT
    h24, st4, brT = s.h24, s.st4, s.brT
    dyp, ps, pS, prb, xrb, accP = s.dyp, s.ps, s.pS, s.prb, s.xrb, s.accP
    lse, maskb, live, vecT = s.lse, s.maskb, s.live, s.vecT
    vec_buf, vec_got = s.vec_buf, s.vec_got
    gk, gs, yb_f, zb_f = s.gk, s.gs, s.yb_f, s.zb_f
    xb, fx, small_all = s.xb, s.fx, s.small_all

    N = 4
    wide_in = n - give_in
    start_in = xi * give_in
    giving = xi * wide_in
    taking = (1 - xi) * wide_in

    def io_row(k, gg):
        return jnp.where(k < 3, 3 * n * gg + n * k, 3 * D + n * gg)

    first_y = (3 * n // 17) // 8 * 8

    def rows(base, offset, size):
        return pl.ds(pl.multiple_of(base + offset, 8), size)

    def plane_w(k, gg):
        return w_io.at[rows(io_row(k, gg), start_in, wide_in), :]

    def gift_w(k, gg):
        return w_io.at[rows(io_row(k, gg), giving, give_in), :]

    def due_w(k, gg):
        return w_io.at[rows(io_row(k, gg), taking, give_in), :]

    def shard(zz, yy):
        return zz * YSIZE + yy

    def farthest(i):
        table = [sorted(range(Z), key=lambda p: -abs(p - at)) for at in range(Z)]
        pick = jnp.int32(0)
        for at in range(Z):
            for j in range(Z):
                pick = jnp.where((z == at) & (i == j), table[at][j], pick)
        return pick

    assert Z == 4
    at_end = (z == 0) | (z == Z - 1)
    mate = z + 1 - 2 * (z % 2)

    def is_far(zz):
        return (zz != z) & (zz != mate)

    def line_target(zz):
        return here.on_line(jnp.where((zz == mate) | at_end, mate, zz))

    def line_slot(zz):
        return jnp.where(zz == mate, z, zz)

    def goes_on(zz):
        return ((zz < z) & (z < Z - 1)) | ((zz > z) & (z > 0))

    source = y == c
    onward_of = lambda zz: (here.r, g + jnp.where(zz < z, YSIZE, -YSIZE))

    def own_copy(k, way):
        ref = plane_w(k, g)
        return remote(ref, ref, s.a_own.at[k, way], s.a_rp.at[k, z], (here.up, here.down, here.ynbr)[way])

    def passing(k, zz):
        ref = plane_w(k, shard(zz, y))
        return remote(ref, ref, s.a_fwd.at[k, zz], s.a_rp.at[k, zz], onward_of(zz))

    def over_y(k, zz, yy):
        ref = plane_w(k, shard(zz, yy))
        return remote(ref, ref, s.a_y.at[k, zz], s.a_rp.at[k, zz], here.ynbr)

    def over_x(k, zz):
        ref = gift_w(k, shard(zz, c))
        return remote(ref, ref, s.a_x.at[k, zz], s.a_rx.at[k, zz], here.xnbr)

    def x_arrival(k, zz):
        ref = due_w(k, shard(zz, c))
        return remote(ref, ref, s.a_x.at[k, zz], s.a_rx.at[k, zz], here.xnbr)

    def plane_to_partner(k, zz, core):
        ref = plane_w(k, shard(zz, core))
        return remote(ref, ref, s.a_cp.at[k, zz], s.a_rcp.at[k, zz], here.partner)

    def rest_to_partner(k, zz, core):
        ref = due_w(k, shard(zz, core))
        return remote(ref, ref, s.a_cx.at[k, zz], s.a_rcx.at[k, zz], here.partner)

    def ffn_w(mt, gg):
        return w_ffn.at[mt, rows(n * gg, 0, n), :]

    def ffn_own(mt, way):
        ref = ffn_w(mt, g)
        return remote(ref, ref, s.w_own.at[mt, way], s.w_rz.at[mt, z], (here.up, here.down, here.ynbr)[way])

    def ffn_own_y(mt):
        ref = ffn_w(mt, g)
        return remote(ref, ref, s.w_own.at[mt, 2], s.w_ry.at[mt, z], here.ynbr)

    def ffn_pass(mt, zz):
        ref = ffn_w(mt, shard(zz, y))
        return remote(ref, ref, s.w_fwd.at[mt, zz], s.w_rz.at[mt, zz], onward_of(zz))

    def ffn_over_y(mt, zz, yy):
        ref = w_ffn.at[mt, rows(n * shard(zz, yy), 0, n - first_y), :]
        return remote(ref, ref, s.w_y.at[mt, zz], s.w_ry.at[mt, zz], here.ynbr)

    def ffn_own_y_arrival(mt):
        ref = ffn_w(mt, shard(z, 1 - y))
        return remote(ref, ref, s.w_own.at[mt, 2], s.w_ry.at[mt, z], here.ynbr)

    def ffn_edge(mt, zz):
        return w_ffn.at[mt, rows(n * shard(zz, 1 - y), n - first_y, first_y), :]

    def edge_own(mt, way):
        ref = ffn_edge(mt, z)
        return remote(ref, ref, s.u_own.at[mt, way], s.u_rz.at[mt, z], (here.up, here.down)[way])

    def edge_pass(mt, zz):
        ref = ffn_edge(mt, zz)
        return remote(ref, ref, s.u_fwd.at[mt, zz], s.u_rz.at[mt, zz], onward_of(zz))

    def start_own(k):
        @pl.when(source)
        def _():
            @pl.when(z < Z - 1)
            def _():
                own_copy(k, 0).start()

            @pl.when(z > 0)
            def _():
                own_copy(k, 1).start()

            own_copy(k, 2).start()

    def start_ffn(mt):
        @pl.when(z < Z - 1)
        def _():
            ffn_own(mt, 0).start()

        @pl.when(z > 0)
        def _():
            ffn_own(mt, 1).start()

    def start_ffn_y(mt):
        ffn_own_y(mt).start()

    def both_sides(distance, act):
        def side(i):
            zz = z + jnp.where(i == 0, -distance, distance)

            @pl.when((zz >= 0) & (zz < Z) & ((i == 0) | (distance > 0)))
            def _():
                act(zz)

        loop(2, side)

    def gather_wave(d, part):
        def plane_step(j):
            k = 3 * part + j

            @pl.when((k < N) & source & (d > 0))
            def _():
                def arrived(zz):
                    passing(k, zz).wait_recv()

                    @pl.when(goes_on(zz))
                    def _():
                        passing(k, zz).start()

                    over_y(k, zz, y).start()
                    over_x(k, zz).start()
                    plane_to_partner(k, zz, c).start()

                both_sides(d, arrived)

            @pl.when((k < N) & (y != c))
            def _():
                def arrived(zz):
                    over_y(k, zz, c).wait_recv()
                    over_x(k, zz).start()
                    plane_to_partner(k, zz, c).start()

                both_sides(d, arrived)

        def x_step(j):
            k = 3 * part + j

            @pl.when((k < N) & ((d > 1) | ((d > 0) & (y != c))))
            def _():
                def arrived(zz):
                    x_arrival(k, zz).wait_recv()
                    rest_to_partner(k, zz, c).start()

                both_sides(d - 1, arrived)

        loop(3, plane_step)
        loop(3, x_step)

    def partner_arrivals(k):
        def each(zz):
            @pl.when((y == c) | (zz != z))
            def _():
                plane_to_partner(k, zz, 1 - c).wait_recv()
                rest_to_partner(k, zz, 1 - c).wait_recv()

        loop(Z, each)

    def ffn_wave(mt, d):
        def arrived(zz):
            ffn_pass(mt, zz).wait_recv()

            @pl.when(goes_on(zz))
            def _():
                ffn_pass(mt, zz).start()

            ffn_over_y(mt, zz, y).start()

        both_sides(d, arrived)

    def ffn_edges(mt, d):
        @pl.when(d == 0)
        def _():
            ffn_own_y_arrival(mt).wait_recv()

            @pl.when(z < Z - 1)
            def _():
                edge_own(mt, 0).start()

            @pl.when(z > 0)
            def _():
                edge_own(mt, 1).start()

        @pl.when(d > 0)
        def _():
            def arrived(zz):
                edge_pass(mt, zz).wait_recv()

                @pl.when(goes_on(zz))
                def _():
                    edge_pass(mt, zz).start()

            both_sides(d, arrived)

    def ffn_y_arrivals(mt):
        def each(zz):
            @pl.when(zz != z)
            def _():
                ffn_over_y(mt, zz, 1 - y).wait_recv()

        loop(Z, each)

    def share_copy(e, buf, kind):
        slot = (q, q, here.q_x)[kind]
        target = (here.partner, here.xnbr, here.partner)[kind]
        ref = buf.at[slot]
        return remote(ref, ref, s.e_send.at[e, kind], s.e_recv.at[e, kind], target)

    def share_arrival(e, buf, kind):
        slot = (here.q_partner, here.q_x, here.q_far)[kind]
        target = (here.partner, here.xnbr, here.partner)[kind]
        ref = buf.at[slot]
        return remote(ref, ref, s.e_send.at[e, kind], s.e_recv.at[e, kind], target)

    def swap_copy(i):
        return remote(xo.at[i], xp.at[i], s.p_send.at[i], s.p_recv.at[i], here.partner)

    def part_to_partner(e, j):
        return remote(ps.at[j], prb.at[e, j], s.r_send.at[e, j], s.r_recv.at[e, j], here.partner)

    def part_to_x(e):
        return remote(pS, xrb.at[e], s.r_send.at[e, 2], s.r_recv.at[e, 2], here.xnbr)

    def small_copy(bit, mine):
        size = 1 << bit
        base = (g // size) * size
        if not mine:
            base = base + size - 2 * size * ((g // size) % 2)
        ref = small_all.at[rows(n * base, 0, n * size), :]
        return remote(ref, ref, s.s_send.at[bit], s.s_recv.at[bit], here.flip_grp(bit))

    def fy_copy(mt, zz):
        return remote(gs.at[mt, zz], yb_f.at[mt, zz], s.fy_send.at[mt, zz], s.fy_recv.at[mt, zz], here.ynbr)

    def fz_copy(mt, zz):
        slot = line_slot(zz)
        return remote(gk.at[mt, zz], zb_f.at[mt, slot], s.fz_send.at[mt, zz], s.fz_recv.at[mt, slot], line_target(zz))

    def fz_arrival(mt, slot):
        return remote(gk.at[mt, slot], zb_f.at[mt, slot], s.fz_send.at[mt, slot], s.fz_recv.at[mt, slot], line_target(mate))

    def piece(mt, which):
        return N + Q * mt + which

    def final_copy(mt, kind):
        target = (here.partner, here.xnbr, here.partner)[kind]
        slot = (q, q, here.q_x)[kind]
        src = ffn_out[mt].at[slot] if kind == 2 else gk.at[mt, z]
        dst = ffn_out[mt].at[slot]
        return remote(src, dst, s.fo_send.at[mt, kind], s.fo_recv.at[mt, kind], target)

    def final_arrival(mt, kind):
        target = (here.partner, here.xnbr, here.partner)[kind]
        slot = (here.q_partner, here.q_x, here.q_far)[kind]
        ref = ffn_out[mt].at[slot]
        return remote(ref, ref, s.fo_send.at[mt, kind], s.fo_recv.at[mt, kind], target)

    def final_keep(mt):
        return pltpu.make_async_copy(gk.at[mt, z], ffn_out[mt].at[q], s.fo_keep.at[mt])

    def deepen(ref, k):
        for bit in range(2, rep_bits):
            j = bit - 2
            give = remote(ref, deep_buf.at[k, j], s.d_send, s.d_recv.at[k, j], here.flip_rep(bit))
            give.start()
            give.wait()
            bring = pltpu.make_async_copy(deep_buf.at[k, j], s.d_tmp, s.d_local)
            bring.start()
            bring.wait()
            ref[...] = low(wide(ref[...]) + wide(s.d_tmp[...]))

    def ffn_grads(mt, left, right):
        def block(b):
            at = pl.ds(pl.multiple_of(b * B, 16), B)
            total = dot_nt(left[0, at, :], right[0])
            for t in range(1, Q):
                total = total + dot_nt(left[t, at, :], right[t])

            @pl.when(y == 0)
            def _():
                gk[mt, b] = low(total[:n])
                gs[mt, b] = low(total[n:])

            @pl.when(y == 1)
            def _():
                gk[mt, b] = low(total[n:])
                gs[mt, b] = low(total[:n])

            fy_copy(mt, b).start()

        loop(Z, lambda i: block(farthest(i)))

    def ffn_reduce_y(mt, i):
        zz = farthest(i)
        fy_copy(mt, zz).wait_recv()
        gk[mt, zz] = low(wide(gk[mt, zz]) + wide(yb_f[mt, zz]))

        @pl.when((zz == mate) | (at_end & (zz != z)))
        def _():
            fz_copy(mt, zz).start()

    def ffn_relay(mt):
        def each(i):
            zz = farthest(i)

            @pl.when(is_far(zz) & jnp.logical_not(at_end))
            def _():
                fz_arrival(mt, zz).wait_recv()
                gk[mt, zz] = low(wide(gk[mt, zz]) + wide(zb_f[mt, zz]))
                fz_copy(mt, zz).start()

        loop(Z, each)

    def ffn_reduce_own(mt):
        fz_arrival(mt, mate).wait_recv()
        fz_arrival(mt, z).wait_recv()
        total = wide(gk[mt, z]) + wide(zb_f[mt, mate]) + wide(zb_f[mt, z])
        gk[mt, z] = low(total)
        deepen(gk.at[mt, z], piece(mt, 0))
        for m in range(2):

            @pl.when(mt == m)
            def _(m=m):
                final_keep(m).start()
                final_copy(m, 0).start()
                final_copy(m, 1).start()

    def ffn_reduce_far(mt):
        for m in range(2):

            @pl.when(mt == m)
            def _(m=m):
                final_arrival(m, 1).wait_recv()
                final_copy(m, 2).start()

    def column(j, at=None):
        block = small_all[: D] if at is None else small_all[at, :]
        return wide(block)[:, j : j + 1]

    def statistics(values):
        center = values - jnp.mean(values, axis=0, keepdims=True)
        inverse = lax.rsqrt(jnp.mean(center * center, axis=0, keepdims=True) + EPSILON)
        return center * inverse, inverse

    def norm_back(upstream, normed, inverse, gain):
        scaled = upstream * gain
        return inverse * (
            scaled
            - jnp.mean(scaled, axis=0, keepdims=True)
            - normed * jnp.mean(scaled * normed, axis=0, keepdims=True)
        )

    def total_of(values):
        return jnp.sum(values, axis=1, keepdims=True)

    extra = [here.flip_rep(b) for b in range(2, rep_bits)]

    def schedule(steps):
        def body(at):
            for act in dict.fromkeys(step[0] for step in steps):
                slots = [(i, step[1:]) for i, step in enumerate(steps) if step[0] is act]
                hit = at == slots[0][0]
                for i, _ in slots[1:]:
                    hit = hit | (at == i)

                @pl.when(hit)
                def _(act=act, slots=slots):
                    picked = []
                    for j in range(len(slots[0][1])):
                        values = [args[j] for _, args in slots]
                        pick = jnp.int32(values[0])
                        if len(set(values)) > 1:
                            for (i, _), value in zip(slots[1:], values[1:]):
                                pick = jnp.where(at == i, value, pick)
                        picked.append(pick)
                    act(*picked)

        loop(len(steps), body)

    def ranges(head, served):
        def run(first, last):
            def each(h, carry):
                head(h)
                return carry

            lax.fori_loop(first, last, each, 0)

        steps, first = [], 0
        for h in sorted(served):
            steps += [(run, first, h + 1)] + served[h]
            first = h + 1
        if first < H:
            steps += [(run, first, H)]
        return steps

    local = s.l_sem

    def pull_io(ref, i):
        return pltpu.make_async_copy(ref, ioT, local.at[i])

    def opening(raw_con, turned, cut, piece_con, raw_cot, small_rows, small_own):
        put_in = pltpu.make_async_copy(ain_ref, w_io.at[rows(3 * n * g, 0, 3 * n), :], local.at[0])
        put_out = pltpu.make_async_copy(aout_ref, w_io.at[rows(3 * D + n * g, 0, n), :], local.at[1])
        put_exp = pltpu.make_async_copy(
            exp_ref.at[rows(n * q, 0, n), :], w_ffn.at[0, rows(n * g, 0, n), :], local.at[2]
        )
        pull_con = pltpu.make_async_copy(con_ref, raw_con, local.at[3])
        pull_cot = pltpu.make_async_copy(cot_ref, raw_cot, local.at[4])
        pull_tok = pull_io(tok_ref, 5)
        put_in.start()
        put_out.start()
        pull_tok.start()
        put_exp.start()
        pull_cot.start()
        pull_con.start()
        small_rows[...] = jnp.zeros_like(small_rows)
        for j, ref in enumerate(vector_refs[:8]):
            small_rows[j : j + 1, :] = wide(ref[...]).reshape(1, n)
        expand_bias = wide(vector_refs[8][...]).reshape(1, Q * n)
        for j in range(Q):
            small_rows[8 + j : 9 + j, :] = expand_bias[:, j * n : (j + 1) * n]
        small_own[...] = low(small_rows[...].T)
        put_small = pltpu.make_async_copy(small_own, small_all.at[rows(n * g, 0, n), :], s.k_sem.at[0])
        put_small.start()
        greet(here, extra)
        put_in.wait()
        put_small.wait()
        small_copy(0, True).start()
        put_out.wait()
        put_exp.wait()
        ends = []
        end = 0
        for i in range(len_ref.shape[1]):
            end = end + len_ref[0, i]
            ends.append(end)

        def labels(position):
            number = jnp.zeros(position.shape, jnp.int32)
            for end in ends:
                number = number + jnp.where(position >= end, 1, 0)
            return jnp.where(position < ends[-1], number, len(ends) + position)

        def small_rounds(bit):
            for b in range(grp_bits):

                @pl.when(bit == b)
                def _(b=b):
                    small_copy(b, False).wait_recv()
                    if b + 1 < grp_bits:
                        small_copy(b + 1, True).start()

        def layout():
            query_slot = lax.broadcasted_iota(jnp.int32, (1, T), 1)
            key_slot = lax.broadcasted_iota(jnp.int32, (T, 1), 0)
            query_label, key_label = labels(query_slot), labels(key_slot)
            allowed = (key_slot <= query_slot) & (key_label == query_label)
            maskb[...] = jnp.where(allowed, 0.0, MASKED)
            live[...] = jnp.where(query_slot < ends[-1], 1.0, 0.0)

        def first_norm():
            pull_tok.wait()
            normed, _ = statistics(ioT[...])
            xo[1] = low(normed * column(0) + column(1))
            swap_copy(1).start()

        def upstream():
            pull_cot.wait()
            start = jnp.where(live[...] > 0.5, raw_cot[...], 0.0)
            st4[q] = low(start)
            vecT[...] = jnp.zeros_like(vecT)
            vecT[:, 7:8] = total_of(start)

        def share_start():
            share_copy(0, st4, 0).start()
            share_copy(0, st4, 1).start()

        def pass_start():
            share_arrival(0, st4, 1).wait_recv()
            share_copy(0, st4, 2).start()

        def con_block(gg):
            return pltpu.make_async_copy(
                turned.at[rows(Q * n * gg, n * q, n), :], cut.at[rows(n * gg, 0, n), :], s.k_sem.at[gg]
            )

        def cut_contract():
            pull_con.wait()
            turned[:FF] = raw_con[...].T
            loop(G, lambda gg: con_block(gg).start())
            loop(G, lambda gg: con_block(gg).wait())
            piece_con[...] = cut[:D].T
            put = pltpu.make_async_copy(piece_con, w_ffn.at[1, rows(n * g, 0, n), :], local.at[3])
            put.start()
            put.wait()

        def project():
            def block(b):
                at = pl.ds(pl.multiple_of(b * B, 16), B)
                projT[at, :] = low(dot_nn(w_io[at, :], xo[1]))

            def add_bias(first, j):
                def each(b):
                    at = pl.ds(pl.multiple_of(b * B, 16), B)
                    to = pl.ds(pl.multiple_of(first + b * B, 16), B)
                    projT[to, :] = low(dot_nn(w_io[to, :], xo[1]) + column(j, at))

                loop(D // B, each)

            add_bias(0, 2)
            loop(D // B, lambda b: block(b + D // B))
            add_bias(2 * D, 3)

        def head_forward(h):
            at = pl.multiple_of(h * HD, HD)
            query = projT[pl.ds(at, HD), :]
            key = projT[pl.ds(pl.multiple_of(D + at, HD), HD), :]
            value = projT[pl.ds(pl.multiple_of(2 * D + at, HD), HD), :]
            scores = dot_nn(low(wide(key).T), query) * scale + maskb[...]
            peak = jnp.max(scores, axis=0, keepdims=True)
            logsum = peak + jnp.log(jnp.sum(jnp.exp(scores - peak), axis=0, keepdims=True))
            lse[h] = logsum
            weights = low(jnp.exp(scores - logsum))
            xo[0, pl.ds(at, HD), :] = low(dot_nn(value, weights))

        steps = [(start_own, k) for k in range(3)] + [(small_rounds, 0), (layout,)]
        steps += [(gather_wave, 0, 0), (start_own, 3), (gather_wave, 1, 0), (small_rounds, 1), (cut_contract,)]
        steps += [(gather_wave, 2, 0), (start_ffn, 0)] + [(small_rounds, b) for b in range(2, grp_bits)]
        steps += [(first_norm,)] + [(gather_wave, i, 0) for i in range(3, Z)] + [(gather_wave, 0, 1), (gather_wave, 1, 1)]
        steps += [(start_ffn_y, 0), (gather_wave, Z, 0), (upstream,), (gather_wave, 2, 1)]
        steps += [(partner_arrivals, k) for k in range(3)] + [(ffn_wave, 0, 1), (gather_wave, 3, 1)]
        steps += [(project,), (ffn_edges, 0, 0), (gather_wave, 4, 1), (share_start,)]
        served = {
            2: [(ffn_wave, 0, 2)],
            6: [(ffn_edges, 0, 1), (start_ffn, 1)],
            11: [(ffn_wave, 0, 3), (start_ffn_y, 1)],
            14: [(ffn_edges, 0, 2)],
            16: [(pass_start,)],
        }
        steps += ranges(head_forward, served)
        schedule(steps)

    pl.run_scoped(
        opening,
        pltpu.VMEM((n, FF), BF16),
        pltpu.VMEM((FF + PAD, n), BF16),
        pltpu.VMEM((D + PAD, n), BF16),
        pltpu.VMEM((n, D), BF16),
        pltpu.VMEM((D, T), F32),
        pltpu.VMEM((128, n), F32),
        pltpu.VMEM((n, 128), BF16),
    )
    swap_copy(0).start()
    partner_arrivals(3)

    def attention_out(b):
        at = pl.ds(pl.multiple_of(b * B, 16), B)
        to = pl.ds(pl.multiple_of(3 * D + b * B, 16), B)
        resT[at, :] = ioT[at, :] + dot_nn(w_io[to, :], xo[0]) + column(4, at)

    loop(D // B, attention_out)
    pull_io(cot_ref, 5).start()
    normed, _ = statistics(resT[...])
    h24[q] = low(normed * column(5) + column(6))
    share_copy(1, h24, 0).start()
    share_copy(1, h24, 1).start()

    def dy_rows(k, zz, core):
        gg = shard(zz, core)
        row = jnp.where(k == 0, 3 * D + n * gg, 3 * n * gg + n * (k - 1))
        return rows(row, 0, n)

    def dy_swap(k, zz):
        return remote(
            projT.at[dy_rows(k, zz, 1 - c), :],
            dyp.at[k, zz],
            s.dy_send.at[k, zz],
            s.dy_recv.at[k, zz],
            here.partner,
        )

    def middle(gp4, act4, bb4):
        def expand(t):
            def block(b):
                at = pl.ds(pl.multiple_of(b * B, 16), B)
                part = wide(small_all[at, :])
                bias = part[:, 8:9]
                for j in range(1, Q):
                    bias = jnp.where(q == j, part[:, 8 + j : 9 + j], bias)
                u = dot_nn(w_ffn[0, at, :], h24[t]) + bias
                th = jnp.tanh(GELU_A * (u + GELU_B * (u * u * u)))
                act4[t, at, :] = low(0.5 * u * (1.0 + th))
                gp4[t, at, :] = 0.5 * (1.0 + th) + (0.5 * GELU_A) * u * (1.0 - th * th) * (
                    1.0 + (3.0 * GELU_B) * (u * u)
                )

            loop(D // B, block)

        def expand_step(i):
            @pl.when(i == 1)
            def _():
                share_arrival(1, h24, 0).wait_recv()

            @pl.when(i == 2)
            def _():
                share_arrival(1, h24, 1).wait_recv()
                share_copy(1, h24, 2).start()

            @pl.when(i == 3)
            def _():
                share_arrival(1, h24, 2).wait_recv()

            expand(member(i))

        def gradients():
            share_arrival(0, st4, 0).wait_recv()
            share_arrival(0, st4, 2).wait_recv()
            ffn_grads(1, st4, act4)

        def member(i):
            first = jnp.where(i == 1, here.q_partner, q)
            return jnp.where(i == 2, here.q_x, jnp.where(i == 3, here.q_far, first))

        def back_step(i):
            t = member(Q - 1 - i)

            def block(b):
                at = pl.ds(pl.multiple_of(b * B, 16), B)
                value = accP[at, :] * gp4[t, at, :]
                bb4[t, at, :] = low(value)
                vecT[at, 12:13] = vecT[at, 12:13] + total_of(value)

            accP[...] = dot_tn(w_ffn[1, :D], st4[t])
            loop(D // B, block)
            accP[...] = dot_tn(w_ffn[0, :D], bb4[t])

            @pl.when(i == 0)
            def _():
                ps[1] = low(accP[...])
                part_to_partner(0, 1).start()

            @pl.when(i == 1)
            def _():
                part_to_partner(0, 1).wait_recv()
                pS[...] = low(accP[...] + wide(prb[0, 1]))
                part_to_x(0).start()

            @pl.when(i == 2)
            def _():
                ps[0] = low(accP[...])
                part_to_partner(0, 0).start()

        def expand_gradients():
            ffn_grads(0, bb4, h24)
            for j in range(2):
                part_to_partner(0, j).wait_send()

        def out_step(i):
            t = member(Q - 1 - i)
            brT[...] = dot_nn(w_ffn[1, :D], act4[t])

            @pl.when(i == 0)
            def _():
                ps[1] = low(brT[...])
                part_to_partner(1, 1).start()

            @pl.when(i == 1)
            def _():
                gp4[1] = brT[...]

            @pl.when(i == 2)
            def _():
                ps[0] = low(brT[...])
                part_to_partner(1, 0).start()

            @pl.when(i == 3)
            def _():
                gp4[0] = brT[...]

        steps = [(ffn_edges, 0, 3), (ffn_wave, 1, 1), (ffn_y_arrivals, 0), (expand_step, 0), (ffn_wave, 1, 2), (expand_step, 1)]
        steps += [(ffn_edges, 1, 0), (ffn_wave, 1, 3), (expand_step, 2), (ffn_edges, 1, 1), (expand_step, 3)]
        steps += [(ffn_edges, 1, 2), (gradients,), (ffn_edges, 1, 3), (ffn_y_arrivals, 1)]
        steps += [(back_step, 0), (back_step, 1), (ffn_reduce_y, 1, 0), (back_step, 2), (ffn_reduce_y, 1, 1)]
        steps += [(back_step, 3), (expand_gradients,), (ffn_reduce_y, 1, 2)] + [(out_step, i) for i in range(Q)]
        steps += [(ffn_reduce_y, 1, 3)]
        schedule(steps)
        part_to_partner(0, 0).wait_recv()
        part_to_x(0).wait_recv()
        back_hidden = accP[...] + wide(prb[0, 0]) + wide(xrb[0])
        normed, inverse = statistics(resT[...])
        vecT[:, 5:6] = total_of(back_hidden * normed)
        vecT[:, 6:7] = total_of(back_hidden)
        pull_io(cot_ref, 5).wait()
        start = jnp.where(live[...] > 0.5, ioT[...], 0.0)
        brT[...] = start + norm_back(back_hidden, normed, inverse, column(5))
        projT[pl.ds(3 * D, D), :] = low(brT[...])
        loop(Z, lambda zz: dy_swap(0, zz).start())
        pull_io(tok_ref, 5).start()
        part_to_x(0).wait_send()
        part_to_partner(1, 1).wait_recv()
        pS[...] = low(gp4[1] + wide(prb[1, 1]))
        part_to_x(1).start()
        resT[...] = resT[...] + gp4[0] + column(7)
        vecT[:, 4:5] = total_of(brT[...])

    pl.run_scoped(
        middle, pltpu.VMEM((Q, D, T), F32), pltpu.VMEM((Q, D, T), BF16), pltpu.VMEM((Q, D, T), BF16)
    )
    batt = xrb.at[0]
    batt[...] = low(dot_tn(w_io[pl.ds(3 * D, D), :], projT[pl.ds(3 * D, D), :]))

    def head_backward(h):
        at = pl.multiple_of(h * HD, HD)
        at_q = pl.ds(at, HD)
        at_k = pl.ds(pl.multiple_of(D + at, HD), HD)
        at_v = pl.ds(pl.multiple_of(2 * D + at, HD), HD)
        query, key, value, up = projT[at_q, :], projT[at_k, :], projT[at_v, :], batt[at_q, :]
        scores = dot_nn(low(wide(key).T), query) * scale + maskb[...]
        probability = jnp.exp(scores - lse[h])
        weights = low(probability)
        delta = jnp.sum(wide(up) * wide(xo[0, at_q, :]), axis=0, keepdims=True)
        flow = dot_nn(low(wide(value).T), up)
        slope = low(probability * (flow - delta) * scale)
        back_query = dot_nn(key, slope)
        back_value = dot_nt(up, weights)
        vecT[at_q, 2:3] = total_of(back_query)
        vecT[at_q, 3:4] = total_of(back_value)
        projT[at_k, :] = low(dot_nt(query, slope))
        projT[at_q, :] = low(back_query)
        projT[at_v, :] = low(back_value)

    wide_out = n - give_out

    def closing(plane, xs, stage, fin, con_in, con_turn, con_tall, con_flat, vec_own):
        def x_copy(k, zz):
            return remote(xs.at[k, zz], xb.at[k, zz], s.gx_send.at[k, zz], s.gx_recv.at[k, zz], here.xnbr)

        def y_copy(k, zz):
            return remote(plane.at[k, zz], yb_a.at[k, zz], s.gy_send.at[k, zz], s.gy_recv.at[k, zz], here.ynbr)

        def z_copy(k, zz):
            slot = line_slot(zz)
            return remote(
                plane.at[k, zz], zb_a.at[k, slot], s.gz_send.at[k, zz], s.gz_recv.at[k, slot], line_target(zz)
            )

        def z_arrival(k, slot):
            return remote(
                plane.at[k, slot], zb_a.at[k, slot], s.gz_send.at[k, slot], s.gz_recv.at[k, slot], line_target(mate)
            )

        def f_copy(k):
            return remote(plane.at[k, z], fx.at[k], s.gf_send.at[k], s.gf_recv.at[k], here.xnbr)

        def o_keep(k, dst):
            return pltpu.make_async_copy(fin.at[k % 2], dst, s.go_keep.at[k])

        def o_give(k, dst):
            return remote(fin.at[k % 2], dst, s.go_send.at[k], s.go_recv.at[k], here.partner)

        any_out = in_out.at[0]

        def bring(src, slot):
            copy = pltpu.make_async_copy(src, stage.at[slot], s.st_sem.at[slot])
            copy.start()
            return copy

        def multiply(k):
            j = jnp.where(k == 0, 0, 1)

            @pl.when(k == 0)
            def _():
                swap_copy(0).wait_recv()
                swap_copy(1).wait_recv()


            def each(i):
                zz = farthest(i)
                dy_swap(k, zz).wait_recv()
                term = dot_nt(projT[dy_rows(k, zz, c), :], xo[j]) + dot_nt(dyp[k, zz], xp[j])

                @pl.when(xi == 0)
                def _():
                    plane[k, zz] = low(term[:wide_out])
                    xs[k, zz] = low(term[wide_out:])

                @pl.when(xi == 1)
                def _():
                    plane[k, zz] = low(term[give_out:])
                    xs[k, zz] = low(term[:give_out])

                x_copy(k, zz).start()

            loop(Z, each)

        def after_x(k):
            def each(i):
                zz = farthest(i)
                x_copy(k, zz).wait_recv()
                got = wide(xb[k, zz])

                @pl.when(xi == 0)
                def _():
                    plane[k, zz, :give_out] = low(wide(plane[k, zz, :give_out]) + got)

                @pl.when(xi == 1)
                def _():
                    edge = wide_out - give_out
                    plane[k, zz, edge:] = low(wide(plane[k, zz, edge:]) + got)

                @pl.when(y != c)
                def _():
                    y_copy(k, zz).start()

            loop(Z, each)

        def after_y(k):
            @pl.when(source)
            def _():
                def fetch(i):
                    zz = farthest(i)
                    y_copy(k, zz).wait_recv()
                    bring(yb_a.at[k, zz], i)

                def add(i):
                    zz = farthest(i)
                    pltpu.make_async_copy(yb_a.at[k, zz], stage.at[i], s.st_sem.at[i]).wait()
                    plane[k, zz] = low(wide(plane[k, zz]) + wide(stage[i]))

                    @pl.when((zz == mate) | (at_end & (zz != z)))
                    def _():
                        z_copy(k, zz).start()

                def step(i):
                    @pl.when(i < Z)
                    def _():
                        fetch(i)

                    @pl.when(i > 0)
                    def _():
                        add(i - 1)

                loop(Z + 1, step)

        def relay(k):
            def each(i):
                zz = farthest(i)

                @pl.when(source & is_far(zz) & jnp.logical_not(at_end))
                def _():
                    z_arrival(k, zz).wait_recv()
                    bring(zb_a.at[k, zz], i).wait()
                    plane[k, zz] = low(wide(plane[k, zz]) + wide(stage[i]))
                    z_copy(k, zz).start()

            loop(Z, each)

        def after_z(k):
            @pl.when(source)
            def _():
                z_arrival(k, mate).wait_recv()
                near = bring(zb_a.at[k, mate], 0)
                z_arrival(k, z).wait_recv()
                far = bring(zb_a.at[k, z], 1)
                near.wait()
                far.wait()
                plane[k, z] = low(wide(plane[k, z]) + wide(stage[0]) + wide(stage[1]))
                f_copy(k).start()

        def finish(k):
            @pl.when(source)
            def _():
                f_copy(k).wait_recv()

                @pl.when(k >= 2)
                def _():
                    o_keep(k - 2, any_out).wait()
                    o_give(k - 2, any_out).wait_send()

                slot = k % 2

                def assemble(first, second):
                    fin[slot, :give_out] = first[:give_out]
                    fin[slot, give_out:wide_out] = low(
                        wide(first[give_out:]) + wide(second[: wide_out - give_out])
                    )
                    fin[slot, wide_out:] = second[wide_out - give_out :]

                @pl.when(xi == 0)
                def _():
                    assemble(plane[k, z], fx[k])

                @pl.when(xi == 1)
                def _():
                    assemble(fx[k], plane[k, z])

                deepen(fin.at[slot], k)
                @pl.when(k == 0)
                def _():
                    o_keep(k, out_out).start()
                    o_give(k, out_out).start()

                @pl.when(k > 0)
                def _():
                    o_keep(k, in_out.at[k - 1]).start()
                    o_give(k, in_out.at[k - 1]).start()


        def vec_copy(i):
            target_r, target_g = here.flip_rep(0)
            for b in range(1, rep_bits):
                other = here.flip_rep(b)
                target_r = jnp.where(i == b, other[0], target_r)
                target_g = jnp.where(i == b, other[1], target_g)
            for b in range(grp_bits):
                other = here.flip_grp(b)
                target_r = jnp.where(i == rep_bits + b, other[0], target_r)
                target_g = jnp.where(i == rep_bits + b, other[1], target_g)
            return remote(
                vec_buf.at[i], vec_got.at[i], s.v_send.at[i], s.v_recv.at[i], (target_r, target_g)
            )

        def swap_all():
            for k in range(1, N):
                loop(Z, lambda zz, k=k: dy_swap(k, zz).start())

        def last_norm():
            back_hidden = dot_tn(w_io[pl.ds(0, 3 * D), :], projT[: 3 * D])
            pull_io(tok_ref, 5).wait()
            normed, inverse = statistics(ioT[...])
            vecT[:, 0:1] = total_of(back_hidden * normed)
            vecT[:, 1:2] = total_of(back_hidden)
            accP[...] = brT[...] + norm_back(back_hidden, normed, inverse, column(0))
            tg_copy.start()
            spread = vecT[:, 12:13]
            for j in range(Q):
                vecT[:, 8 + j : 9 + j] = jnp.where(q == j, spread, 0.0)
            vec_buf[0] = vecT[...].T[:16]
            vec_copy(0).start()

        tg_copy = pltpu.make_async_copy(accP, tg_out, local.at[1])
        bo_copy = pltpu.make_async_copy(resT, bo_out, local.at[0])
        push_vec = pltpu.make_async_copy(vec_own, vec_out, local.at[2])

        def block_done():
            part_to_partner(1, 0).wait_recv()
            part_to_x(1).wait_recv()
            output = resT[...] + wide(prb[1, 0]) + wide(xrb[1])
            resT[...] = jnp.where(live[...] > 0.5, output, 0.0)
            bo_copy.start()

        def vec_round(t):
            vec_copy(t).wait_recv()
            vec_buf[t + 1] = vec_buf[t] + vec_got[t]

            @pl.when(t + 1 < rounds)
            def _():
                vec_copy(t + 1).start()

            @pl.when(t + 1 == rounds)
            def _():
                vecT[:, :16] = vec_buf[rounds].T
                vec_own[...] = vecT[pl.ds(pl.multiple_of(n * g, 8), n), :].T[:16]
                push_vec.start()

        def bring_piece(j):
            return pltpu.make_async_copy(con_raw.at[j], con_in.at[j % 2], s.k_sem.at[2 * G + j % 2])

        def put_block(j, gg):
            return pltpu.make_async_copy(
                con_turn.at[j % 2, rows(n * gg, 0, n), :],
                con_cut.at[rows(Q * n * gg, n * j, n), :],
                s.k_sem.at[G * (j % 2) + gg],
            )

        def con_finals():
            final_keep(1).wait()
            final_arrival(1, 0).wait_recv()
            final_arrival(1, 2).wait_recv()
            bring_piece(0).start()
            bring_piece(1).start()

        def con_piece(j):
            bring_piece(j).wait()

            @pl.when(j >= 2)
            def _():
                loop(G, lambda gg: put_block(j - 2, gg).wait())

            con_turn[j % 2, :D] = con_in[j % 2].T

            @pl.when(j + 2 < Q)
            def _():
                bring_piece(j + 2).start()

            loop(G, lambda gg: put_block(j, gg).start())

        half_size = FF // 2

        def bring_side(half):
            return pltpu.make_async_copy(
                con_cut.at[rows(half_size * half, 0, half_size), :], con_tall, s.k_sem.at[2 * G + 2]
            )

        def put_side(half):
            to = pl.ds(pl.multiple_of(half_size * half, 128), half_size)
            return pltpu.make_async_copy(con_flat, con_out.at[:, to], s.k_sem.at[2 * G + 3])

        def con_side(i):
            @pl.when(i == 0)
            def _():
                loop(G, lambda gg: put_block(Q - 2, gg).wait())
                loop(G, lambda gg: put_block(Q - 1, gg).wait())
                bring_side(0).start()

            @pl.when(i > 0)
            def _():
                half = i - 1
                bring_side(half).wait()

                @pl.when(half == 1)
                def _():
                    put_side(0).wait()

                con_flat[...] = con_tall[...].T
                put_side(half).start()

                @pl.when(half == 0)
                def _():
                    bring_side(1).start()

        served = {7: [(ffn_relay, 1)], 13: [(ffn_reduce_y, 0, 0)]}
        steps = [(multiply, 0)] + ranges(head_backward, served)
        steps += [(swap_all,), (last_norm,), (multiply, 1), (ffn_reduce_y, 0, 1), (vec_round, 0), (after_x, 0)]
        steps += [(multiply, 2), (multiply, 3), (ffn_reduce_y, 0, 2), (ffn_reduce_y, 0, 3), (after_x, 1), (vec_round, 1)]
        steps += [(ffn_reduce_own, 1), (after_x, 2), (after_y, 0), (ffn_relay, 0), (after_x, 3)]
        steps += [(relay, 0), (after_y, 1), (vec_round, 2), (relay, 1), (after_y, 2), (after_z, 0), (block_done,)]
        steps += [(relay, 2), (ffn_reduce_far, 1), (after_y, 3), (after_z, 1), (vec_round, 3), (relay, 3)]
        steps += [(finish, 0), (ffn_reduce_own, 0), (after_z, 2), (con_finals,), (finish, 1), (con_piece, 0)]
        steps += [(con_piece, 1), (con_piece, 2), (con_piece, 3), (after_z, 3), (con_side, 0), (vec_round, 4)]
        steps += [(finish, 2), (con_side, 1), (con_side, 2), (ffn_reduce_far, 0), (finish, 3)]
        steps += [(vec_round, t) for t in range(5, rounds)]
        schedule(steps)

        def settle(k):
            @pl.when(source)
            def _():
                @pl.when(z < Z - 1)
                def _():
                    own_copy(k, 0).wait_send()

                @pl.when(z > 0)
                def _():
                    own_copy(k, 1).wait_send()

                own_copy(k, 2).wait_send()

            def each(zz):
                @pl.when((y != c) | (zz != z))
                def _():
                    over_x(k, zz).wait_send()
                    plane_to_partner(k, zz, c).wait_send()
                    rest_to_partner(k, zz, c).wait_send()

                @pl.when(source & (zz != z))
                def _():
                    over_y(k, zz, y).wait_send()

                    @pl.when(goes_on(zz))
                    def _():
                        passing(k, zz).wait_send()

                x_copy(k, zz).wait_send()
                dy_swap(k, zz).wait_send()

                @pl.when(y != c)
                def _():
                    y_copy(k, zz).wait_send()

                @pl.when(source & (zz != z))
                def _():
                    z_copy(k, zz).wait_send()

            loop(Z, each)

            @pl.when(source)
            def _():
                f_copy(k).wait_send()

                @pl.when(k >= N - 2)
                def _():
                    o_keep(k, any_out).wait()
                    o_give(k, any_out).wait_send()

            @pl.when(y != c)
            def _():
                o_give(k, any_out).wait_recv()

        loop(N, settle)

        def settle_ffn(mt):
            @pl.when(z < Z - 1)
            def _():
                ffn_own(mt, 0).wait_send()
                edge_own(mt, 0).wait_send()

            @pl.when(z > 0)
            def _():
                ffn_own(mt, 1).wait_send()
                edge_own(mt, 1).wait_send()


            ffn_own_y(mt).wait_send()

            def each(zz):
                fy_copy(mt, zz).wait_send()

                @pl.when(zz != z)
                def _():
                    ffn_over_y(mt, zz, y).wait_send()

                    @pl.when(goes_on(zz))
                    def _():
                        ffn_pass(mt, zz).wait_send()
                        edge_pass(mt, zz).wait_send()

                @pl.when(zz != z)
                def _():
                    fz_copy(mt, zz).wait_send()

            loop(Z, each)

        for mt in range(2):
            settle_ffn(mt)
            for kind in range(3):
                final_copy(mt, kind).wait_send()
        final_keep(0).wait()
        put_side(1).wait()
        final_arrival(0, 0).wait_recv()
        final_arrival(0, 2).wait_recv()
        for e, buf in ((0, st4), (1, h24)):
            for kind in range(3):
                share_copy(e, buf, kind).wait_send()
        for i in range(2):
            swap_copy(i).wait_send()
        for j in range(2):
            part_to_partner(1, j).wait_send()
        part_to_x(1).wait_send()
        for bit in range(grp_bits):
            small_copy(bit, True).wait_send()
        loop(rounds, lambda i: vec_copy(i).wait_send())
        bo_copy.wait()
        tg_copy.wait()
        push_vec.wait()

    pl.run_scoped(
        closing,
        pltpu.VMEM((N, Z, wide_out, D), BF16),
        pltpu.VMEM((N, Z, give_out, D), BF16),
        pltpu.VMEM((Z, wide_out, D), BF16),
        pltpu.VMEM((2, n, D), BF16),
        pltpu.VMEM((2, n, D), BF16),
        pltpu.VMEM((2, D + PAD, n), BF16),
        pltpu.VMEM((FF // 2, n), BF16),
        pltpu.VMEM((n, FF // 2), BF16),
        pltpu.VMEM((16, n), F32),
    )


def run_layer(lengths, tokens, cotangent, a_in, a_out, w_exp, w_con, vectors, R, G):
    D, T = tokens.shape
    FF = w_con.shape[1]
    n = D // G
    H = D // HD
    Z = G // YSIZE
    Q = TEAM
    N = 4
    give_in = (6 * n // 17) // 8 * 8
    give_out = (6 * n // 17) // 8 * 8
    wide_out = n - give_out
    rounds = bits_of(R) + bits_of(G)
    deep = bits_of(R) - 2
    dma = pltpu.SemaphoreType.DMA
    v = pltpu.VMEM
    scratch = dict(
        w_io=v((4 * D + PAD, D), BF16),
        w_ffn=v((2, D + PAD, D), BF16),
        small_all=v((D + PAD, 128), BF16),
        ioT=v((D, T), F32),
        xo=v((2, D, T), BF16),
        xp=v((2, D, T), BF16),
        projT=v((4 * D + PAD, T), BF16),
        resT=v((D, T), F32),
        h24=v((Q, D, T), BF16),
        st4=v((Q, D, T), BF16),
        brT=v((D, T), F32),
        dyp=v((N, Z, n, T), BF16),
        ps=v((2, D, T), BF16),
        pS=v((D, T), BF16),
        prb=v((2, 2, D, T), BF16),
        xrb=v((2, D, T), BF16),
        accP=v((D, T), F32),
        lse=v((H, 1, T), F32),
        maskb=v((T, T), F32),
        live=v((1, T), F32),
        vecT=v((D, 128), F32),
        vec_buf=v((rounds + 1, 16, D), F32),
        vec_got=v((rounds, 16, D), F32),
        gk=v((2, Z, n, D), BF16),
        gs=v((2, Z, n, D), BF16),
        yb_f=v((2, Z, n, D), BF16),
        zb_f=v((2, Z, n, D), BF16),
        xb=v((N, Z, give_out, D), BF16),
        fx=v((N, wide_out, D), BF16),
        d_tmp=v((n, D) if deep > 0 else (8, 128), BF16),
        l_sem=dma((6,)),
        k_sem=dma((2 * G + 4,)),
        a_own=dma((N, 3)),
        w_own=dma((2, 3)),
        e_send=dma((2, 3)),
        e_recv=dma((2, 3)),
        p_send=dma((2,)),
        p_recv=dma((2,)),
        r_send=dma((2, 3)),
        r_recv=dma((2, 3)),
        s_send=dma((bits_of(G),)),
        s_recv=dma((bits_of(G),)),
        v_send=dma((rounds,)),
        v_recv=dma((rounds,)),
        fo_send=dma((2, 3)),
        fo_recv=dma((2, 3)),
        fo_keep=dma((2,)),
        fz_recv=dma((2, Z)),
        gz_recv=dma((N, Z)),
        gf_send=dma((N,)),
        gf_recv=dma((N,)),
        go_keep=dma((N,)),
        go_send=dma((N,)),
        go_recv=dma((N,)),
        st_sem=dma((Z,)),
        d_send=dma,
        d_local=dma,
        d_recv=dma((N + 2 * Q, max(deep, 1))),
        u_own=dma((2, 2)),
        u_rz=dma((2, Z)),
        u_fwd=dma((2, Z)),
        w_rz=dma((2, Z)),
        w_ry=dma((2, Z)),
        w_fwd=dma((2, Z)),
        w_y=dma((2, Z)),
        fy_send=dma((2, Z)),
        fy_recv=dma((2, Z)),
        fz_send=dma((2, Z)),
        a_rp=dma((N, Z)),
        a_rx=dma((N, Z)),
        a_rcp=dma((N, Z)),
        a_rcx=dma((N, Z)),
        a_fwd=dma((N, Z)),
        a_y=dma((N, Z)),
        a_x=dma((N, Z)),
        a_cp=dma((N, Z)),
        a_cx=dma((N, Z)),
        gx_send=dma((N, Z)),
        gx_recv=dma((N, Z)),
        gy_send=dma((N, Z)),
        gy_recv=dma((N, Z)),
        gz_send=dma((N, Z)),
        dy_send=dma((N, Z)),
        dy_recv=dma((N, Z)),
    )
    hbm = pl.BlockSpec(memory_space=pl.ANY)
    outs = pl.pallas_call(
        functools.partial(layer_kernel, R, G, give_in, give_out, tuple(scratch)),
        out_shape=(
            jax.ShapeDtypeStruct((D, T), F32),
            jax.ShapeDtypeStruct((D, T), F32),
            jax.ShapeDtypeStruct((3, n, D), BF16),
            jax.ShapeDtypeStruct((n, D), BF16),
            jax.ShapeDtypeStruct((Q, n, D), BF16),
            jax.ShapeDtypeStruct((n, FF), BF16),
            jax.ShapeDtypeStruct((16, n), F32),
            jax.ShapeDtypeStruct((Q, n, D), BF16),
            jax.ShapeDtypeStruct((FF, n), BF16),
            jax.ShapeDtypeStruct((N, Z, wide_out, D), BF16),
            jax.ShapeDtypeStruct((N, Z, wide_out, D), BF16),
            jax.ShapeDtypeStruct((N + 2 * Q, deep, n, D) if deep > 0 else (1, 1, 8, 128), BF16),
        ),
        in_specs=[pl.BlockSpec(memory_space=pltpu.SMEM)] + [hbm] * 6 + [pl.BlockSpec(memory_space=pltpu.VMEM)] * 9,
        out_specs=(hbm,) * 12,
        scratch_shapes=list(scratch.values()),
        compiler_params=pltpu.CompilerParams(collective_id=0, has_side_effects=True, vmem_limit_bytes=VMEM_LIMIT),
        name="layer",
    )(lengths, tokens, cotangent, a_in, a_out, w_exp, w_con, *vectors)
    return outs[:7]


def per_device(
    tokens,
    document_lengths,
    cotangent,
    first_gain,
    first_shift,
    attention_in,
    query_bias,
    value_bias,
    attention_out,
    output_bias,
    second_gain,
    second_shift,
    expand_weight,
    expand_bias,
    contract_weight,
    contract_bias,
):
    R, G = lax.axis_size("rep"), lax.axis_size("grp")
    T, D = tokens.shape
    n = D // G
    Q = TEAM
    vectors = [
        first_gain,
        first_shift,
        query_bias,
        value_bias,
        output_bias,
        second_gain,
        second_shift,
        contract_bias,
        expand_bias,
    ]
    block_t, tokens_t, in_grad, out_grad, exp_grad, con_grad, share = run_layer(
        document_lengths,
        tokens.T,
        cotangent.T,
        attention_in.T,
        attention_out.T,
        expand_weight.T,
        contract_weight.T,
        vectors,
        R,
        G,
    )
    out_grad = out_grad.T.astype(F32)
    in_grad = in_grad.reshape(3 * n, D).T.astype(F32)
    exp_grad = exp_grad.reshape(Q * n, D).T.astype(F32)
    con_grad = con_grad.T.astype(F32)
    return (
        block_t.T,
        tokens_t.T,
        share[0],
        share[1],
        in_grad,
        share[2],
        share[3],
        out_grad,
        share[4],
        share[5],
        share[6],
        exp_grad,
        share[8 : 8 + Q].reshape(Q * n),
        con_grad,
        share[7],
    )


def solution(mesh):
    rows = P(("rep", "grp"), None)
    split, columns = P("grp"), P(None, "grp")
    return jax.shard_map(
        per_device,
        mesh=mesh,
        in_specs=(
            rows,
            rows,
            rows,
            split,
            split,
            columns,
            split,
            split,
            columns,
            split,
            split,
            split,
            columns,
            split,
            columns,
            split,
        ),
        out_specs=(
            rows,
            rows,
            split,
            split,
            columns,
            split,
            split,
            columns,
            split,
            split,
            split,
            columns,
            split,
            columns,
            split,
        ),
        check_vma=False,
    )
```

```python
import functools
import types

import jax
import jax.numpy as jnp
from jax import lax
from jax.experimental import pallas as pl
from jax.experimental.pallas import tpu as pltpu
from jax.sharding import PartitionSpec as P

HD = 64
EPSILON = 1e-05
MASKED = -1e30
PAD = 8
YSIZE = 2
TEAM = 4
GELU_A = 0.7978845608028654
GELU_B = 0.044715
MESH_ID = pl.DeviceIdType.MESH
VMEM_LIMIT = 67043328
BF16, F32 = jnp.bfloat16, jnp.float32


def bits_of(count):
    return count.bit_length() - 1


def dot_nn(left, right):
    return lax.dot_general(left, right, (((1,), (0,)), ((), ())), preferred_element_type=F32)


def dot_nt(left, right):
    return lax.dot_general(left, right, (((1,), (1,)), ((), ())), preferred_element_type=F32)


def dot_tn(left, right):
    return lax.dot_general(left, right, (((0,), (0,)), ((), ())), preferred_element_type=F32)


def remote(src, dst, send, recv, target):
    return pltpu.make_async_remote_copy(
        src_ref=src, dst_ref=dst, send_sem=send, recv_sem=recv, device_id=target, device_id_type=MESH_ID
    )


def wide(value):
    return value.astype(F32)


def low(value):
    return value.astype(BF16)


class Place:
    def __init__(self, rep_count, grp_count):
        self.R, self.G = rep_count, grp_count
        self.Z = grp_count // YSIZE
        self.r = lax.axis_index("rep")
        self.g = lax.axis_index("grp")
        self.c = self.r % 2
        self.xi = (self.r // 2) % 2
        self.q = self.r % TEAM
        self.z = self.g // YSIZE
        self.y = self.g % YSIZE
        self.partner = (self.r + 1 - 2 * self.c, self.g)
        self.xnbr = (self.r + 2 - 4 * self.xi, self.g)
        self.ynbr = (self.r, self.g + 1 - 2 * self.y)
        self.up = (self.r, self.g + YSIZE)
        self.down = (self.r, self.g - YSIZE)
        self.q_partner = self.q + 1 - 2 * self.c
        self.q_x = self.q + 2 - 4 * self.xi
        self.q_far = self.q_x + 1 - 2 * self.c

    def on_line(self, zz):
        return (self.r, zz * YSIZE + self.y)

    def flip_rep(self, bit):
        on = (self.r // (1 << bit)) % 2
        return (self.r + (1 << bit) - (2 << bit) * on, self.g)

    def flip_grp(self, bit):
        on = (self.g // (1 << bit)) % 2
        return (self.r, self.g + (1 << bit) - (2 << bit) * on)


def greet(here, others):
    barrier = pltpu.get_barrier_semaphore()

    def hello(target):
        pl.semaphore_signal(barrier, inc=1, device_id=target, device_id_type=MESH_ID)

    for target in [here.partner, here.xnbr, here.ynbr] + others:
        hello(target)
    for zz in range(here.Z):

        @pl.when(here.z != zz)
        def _(zz=zz):
            hello(here.on_line(zz))

    pl.semaphore_wait(barrier, 2 + here.Z + len(others))


def loop(count, body):
    def step(i, carry):
        body(i)
        return carry

    lax.fori_loop(0, count, step, 0)


def layer_kernel(R, G, give_in, give_out, names, *refs):
    len_ref, tok_ref, cot_ref, ain_ref, aout_ref, exp_ref, con_ref = refs[:7]
    vector_refs = refs[7:16]
    bo_out, tg_out, in_out, out_out, exp_out, con_out, vec_out, con_raw, con_cut, yb_a, zb_a, deep_buf = refs[16:28]
    s = types.SimpleNamespace(**dict(zip(names, refs[28:])))
    ffn_out = (exp_out, con_raw)
    here = Place(R, G)
    Z, z, y, c, xi, q, g = here.Z, here.z, here.y, here.c, here.xi, here.q, here.g
    D, T = tok_ref.shape
    n = D // G
    H = D // HD
    Q = TEAM
    FF = con_ref.shape[1]
    n4 = Q * n
    B = 2 * n
    scale = HD ** (-0.5)
    rep_bits, grp_bits = bits_of(R), bits_of(G)
    rounds = rep_bits + grp_bits
    w_io, w_ffn = s.w_io, s.w_ffn
    ioT, xo, xp, projT, resT = s.ioT, s.xo, s.xp, s.projT, s.resT
    h24, st4, brT = s.h24, s.st4, s.brT
    dyp, ps, pS, prb, xrb, accP = s.dyp, s.ps, s.pS, s.prb, s.xrb, s.accP
    lse, maskb, live, vecT = s.lse, s.maskb, s.live, s.vecT
    vec_buf, vec_got = s.vec_buf, s.vec_got
    gk, gs, yb_f, zb_f = s.gk, s.gs, s.yb_f, s.zb_f
    xb, fx, small_all = s.xb, s.fx, s.small_all

    N = 4
    wide_in = n - give_in
    start_in = xi * give_in
    giving = xi * wide_in
    taking = (1 - xi) * wide_in

    def io_row(k, gg):
        return jnp.where(k < 3, 3 * n * gg + n * k, 3 * D + n * gg)

    first_y = (3 * n // 17) // 8 * 8

    def rows(base, offset, size):
        return pl.ds(pl.multiple_of(base + offset, 8), size)

    def plane_w(k, gg):
        return w_io.at[rows(io_row(k, gg), start_in, wide_in), :]

    def gift_w(k, gg):
        return w_io.at[rows(io_row(k, gg), giving, give_in), :]

    def due_w(k, gg):
        return w_io.at[rows(io_row(k, gg), taking, give_in), :]

    def shard(zz, yy):
        return zz * YSIZE + yy

    def farthest(i):
        table = [sorted(range(Z), key=lambda p: -abs(p - at)) for at in range(Z)]
        pick = jnp.int32(0)
        for at in range(Z):
            for j in range(Z):
                pick = jnp.where((z == at) & (i == j), table[at][j], pick)
        return pick

    assert Z == 4
    at_end = (z == 0) | (z == Z - 1)
    mate = z + 1 - 2 * (z % 2)

    def is_far(zz):
        return (zz != z) & (zz != mate)

    def line_target(zz):
        return here.on_line(jnp.where((zz == mate) | at_end, mate, zz))

    def line_slot(zz):
        return jnp.where(zz == mate, z, zz)

    def goes_on(zz):
        return ((zz < z) & (z < Z - 1)) | ((zz > z) & (z > 0))

    source = y == c
    onward_of = lambda zz: (here.r, g + jnp.where(zz < z, YSIZE, -YSIZE))

    def own_copy(k, way):
        ref = plane_w(k, g)
        return remote(ref, ref, s.a_own.at[k, way], s.a_rp.at[k, z], (here.up, here.down, here.ynbr)[way])

    def passing(k, zz):
        ref = plane_w(k, shard(zz, y))
        return remote(ref, ref, s.a_fwd.at[k, zz], s.a_rp.at[k, zz], onward_of(zz))

    def over_y(k, zz, yy):
        ref = plane_w(k, shard(zz, yy))
        return remote(ref, ref, s.a_y.at[k, zz], s.a_rp.at[k, zz], here.ynbr)

    def over_x(k, zz):
        ref = gift_w(k, shard(zz, c))
        return remote(ref, ref, s.a_x.at[k, zz], s.a_rx.at[k, zz], here.xnbr)

    def x_arrival(k, zz):
        ref = due_w(k, shard(zz, c))
        return remote(ref, ref, s.a_x.at[k, zz], s.a_rx.at[k, zz], here.xnbr)

    def plane_to_partner(k, zz, core):
        ref = plane_w(k, shard(zz, core))
        return remote(ref, ref, s.a_cp.at[k, zz], s.a_rcp.at[k, zz], here.partner)

    def rest_to_partner(k, zz, core):
        ref = due_w(k, shard(zz, core))
        return remote(ref, ref, s.a_cx.at[k, zz], s.a_rcx.at[k, zz], here.partner)

    def ffn_w(mt, gg):
        return w_ffn.at[mt, rows(n * gg, 0, n), :]

    def ffn_own(mt, way):
        ref = ffn_w(mt, g)
        return remote(ref, ref, s.w_own.at[mt, way], s.w_rz.at[mt, z], (here.up, here.down, here.ynbr)[way])

    def ffn_own_y(mt):
        ref = ffn_w(mt, g)
        return remote(ref, ref, s.w_own.at[mt, 2], s.w_ry.at[mt, z], here.ynbr)

    def ffn_pass(mt, zz):
        ref = ffn_w(mt, shard(zz, y))
        return remote(ref, ref, s.w_fwd.at[mt, zz], s.w_rz.at[mt, zz], onward_of(zz))

    def ffn_over_y(mt, zz, yy):
        ref = w_ffn.at[mt, rows(n * shard(zz, yy), 0, n - first_y), :]
        return remote(ref, ref, s.w_y.at[mt, zz], s.w_ry.at[mt, zz], here.ynbr)

    def ffn_own_y_arrival(mt):
        ref = ffn_w(mt, shard(z, 1 - y))
        return remote(ref, ref, s.w_own.at[mt, 2], s.w_ry.at[mt, z], here.ynbr)

    def ffn_edge(mt, zz):
        return w_ffn.at[mt, rows(n * shard(zz, 1 - y), n - first_y, first_y), :]

    def edge_own(mt, way):
        ref = ffn_edge(mt, z)
        return remote(ref, ref, s.u_own.at[mt, way], s.u_rz.at[mt, z], (here.up, here.down)[way])

    def edge_pass(mt, zz):
        ref = ffn_edge(mt, zz)
        return remote(ref, ref, s.u_fwd.at[mt, zz], s.u_rz.at[mt, zz], onward_of(zz))

    def start_own(k):
        @pl.when(source)
        def _():
            @pl.when(z < Z - 1)
            def _():
                own_copy(k, 0).start()

            @pl.when(z > 0)
            def _():
                own_copy(k, 1).start()

            own_copy(k, 2).start()

    def start_ffn(mt):
        @pl.when(z < Z - 1)
        def _():
            ffn_own(mt, 0).start()

        @pl.when(z > 0)
        def _():
            ffn_own(mt, 1).start()

    def start_ffn_y(mt):
        ffn_own_y(mt).start()

    def both_sides(distance, act):
        def side(i):
            zz = z + jnp.where(i == 0, -distance, distance)

            @pl.when((zz >= 0) & (zz < Z) & ((i == 0) | (distance > 0)))
            def _():
                act(zz)

        loop(2, side)

    def gather_wave(d, part):
        def plane_step(j):
            k = 3 * part + j

            @pl.when((k < N) & source & (d > 0))
            def _():
                def arrived(zz):
                    passing(k, zz).wait_recv()

                    @pl.when(goes_on(zz))
                    def _():
                        passing(k, zz).start()

                    over_y(k, zz, y).start()
                    over_x(k, zz).start()
                    plane_to_partner(k, zz, c).start()

                both_sides(d, arrived)

            @pl.when((k < N) & (y != c))
            def _():
                def arrived(zz):
                    over_y(k, zz, c).wait_recv()
                    over_x(k, zz).start()
                    plane_to_partner(k, zz, c).start()

                both_sides(d, arrived)

        def x_step(j):
            k = 3 * part + j

            @pl.when((k < N) & ((d > 1) | ((d > 0) & (y != c))))
            def _():
                def arrived(zz):
                    x_arrival(k, zz).wait_recv()
                    rest_to_partner(k, zz, c).start()

                both_sides(d - 1, arrived)

        loop(3, plane_step)
        loop(3, x_step)

    def partner_arrivals(k):
        def each(zz):
            @pl.when((y == c) | (zz != z))
            def _():
                plane_to_partner(k, zz, 1 - c).wait_recv()
                rest_to_partner(k, zz, 1 - c).wait_recv()

        loop(Z, each)

    def ffn_wave(mt, d):
        def arrived(zz):
            ffn_pass(mt, zz).wait_recv()

            @pl.when(goes_on(zz))
            def _():
                ffn_pass(mt, zz).start()

            ffn_over_y(mt, zz, y).start()

        both_sides(d, arrived)

    def ffn_edges(mt, d):
        @pl.when(d == 0)
        def _():
            ffn_own_y_arrival(mt).wait_recv()

            @pl.when(z < Z - 1)
            def _():
                edge_own(mt, 0).start()

            @pl.when(z > 0)
            def _():
                edge_own(mt, 1).start()

        @pl.when(d > 0)
        def _():
            def arrived(zz):
                edge_pass(mt, zz).wait_recv()

                @pl.when(goes_on(zz))
                def _():
                    edge_pass(mt, zz).start()

            both_sides(d, arrived)

    def ffn_y_arrivals(mt):
        def each(zz):
            @pl.when(zz != z)
            def _():
                ffn_over_y(mt, zz, 1 - y).wait_recv()

        loop(Z, each)

    def share_copy(e, buf, kind):
        slot = (q, q, here.q_x)[kind]
        target = (here.partner, here.xnbr, here.partner)[kind]
        ref = buf.at[slot]
        return remote(ref, ref, s.e_send.at[e, kind], s.e_recv.at[e, kind], target)

    def share_arrival(e, buf, kind):
        slot = (here.q_partner, here.q_x, here.q_far)[kind]
        target = (here.partner, here.xnbr, here.partner)[kind]
        ref = buf.at[slot]
        return remote(ref, ref, s.e_send.at[e, kind], s.e_recv.at[e, kind], target)

    def swap_copy(i):
        return remote(xo.at[i], xp.at[i], s.p_send.at[i], s.p_recv.at[i], here.partner)

    def part_to_partner(e, j):
        return remote(ps.at[j], prb.at[e, j], s.r_send.at[e, j], s.r_recv.at[e, j], here.partner)

    def part_to_x(e):
        return remote(pS, xrb.at[e], s.r_send.at[e, 2], s.r_recv.at[e, 2], here.xnbr)

    def small_copy(bit, mine):
        size = 1 << bit
        base = (g // size) * size
        if not mine:
            base = base + size - 2 * size * ((g // size) % 2)
        ref = small_all.at[rows(n * base, 0, n * size), :]
        return remote(ref, ref, s.s_send.at[bit], s.s_recv.at[bit], here.flip_grp(bit))

    main = n - first_y
    main_rows, edge_rows = pl.ds(0, main), pl.ds(main, first_y)

    def fy_copy(mt, zz):
        return remote(
            gs.at[mt, zz, main_rows],
            yb_f.at[mt, zz, main_rows],
            s.fy_send.at[mt, zz],
            s.fy_recv.at[mt, zz],
            here.ynbr,
        )

    def edge_y(mt):
        return remote(
            gs.at[mt, z, edge_rows], yb_f.at[mt, z, edge_rows], s.ue_send.at[mt], s.ue_recv.at[mt], here.ynbr
        )

    def edge_copy(mt, zz):
        return remote(
            gs.at[mt, zz, edge_rows], s.zb_e.at[mt, z], s.uz_send.at[mt, zz], s.uz_recv.at[mt, z], here.on_line(zz)
        )

    def edge_arrival(mt, zz):
        return remote(
            gs.at[mt, zz, edge_rows], s.zb_e.at[mt, zz], s.uz_send.at[mt, zz], s.uz_recv.at[mt, zz], here.on_line(zz)
        )

    def edge_over(mt):
        total = wide(gs[mt, z, main:])
        for i in range(Z - 1):
            zz = farthest(i)
            edge_arrival(mt, zz).wait_recv()
            total = total + wide(s.zb_e[mt, zz])
        gs[mt, z, main:] = low(total)
        edge_y(mt).start()

    def fz_copy(mt, zz):
        slot = line_slot(zz)
        return remote(gk.at[mt, zz], zb_f.at[mt, slot], s.fz_send.at[mt, zz], s.fz_recv.at[mt, slot], line_target(zz))

    def fz_arrival(mt, slot):
        return remote(gk.at[mt, slot], zb_f.at[mt, slot], s.fz_send.at[mt, slot], s.fz_recv.at[mt, slot], line_target(mate))

    def piece(mt, which):
        return N + Q * mt + which

    def final_copy(mt, kind):
        target = (here.partner, here.xnbr, here.partner)[kind]
        slot = (q, q, here.q_x)[kind]
        src = ffn_out[mt].at[slot] if kind == 2 else gk.at[mt, z]
        dst = ffn_out[mt].at[slot]
        return remote(src, dst, s.fo_send.at[mt, kind], s.fo_recv.at[mt, kind], target)

    def final_arrival(mt, kind):
        target = (here.partner, here.xnbr, here.partner)[kind]
        slot = (here.q_partner, here.q_x, here.q_far)[kind]
        ref = ffn_out[mt].at[slot]
        return remote(ref, ref, s.fo_send.at[mt, kind], s.fo_recv.at[mt, kind], target)

    def final_keep(mt):
        return pltpu.make_async_copy(gk.at[mt, z], ffn_out[mt].at[q], s.fo_keep.at[mt])

    def deepen(ref, k):
        for bit in range(2, rep_bits):
            j = bit - 2
            give = remote(ref, deep_buf.at[k, j], s.d_send, s.d_recv.at[k, j], here.flip_rep(bit))
            give.start()
            give.wait()
            bring = pltpu.make_async_copy(deep_buf.at[k, j], s.d_tmp, s.d_local)
            bring.start()
            bring.wait()
            ref[...] = low(wide(ref[...]) + wide(s.d_tmp[...]))

    def ffn_grads(mt, left, right):
        def block(b):
            at = pl.ds(pl.multiple_of(b * B, 16), B)
            total = dot_nt(left[0, at, :], right[0])
            for t in range(1, Q):
                total = total + dot_nt(left[t, at, :], right[t])

            @pl.when(y == 0)
            def _():
                gk[mt, b] = low(total[:n])
                gs[mt, b] = low(total[n:])

            @pl.when(y == 1)
            def _():
                gk[mt, b] = low(total[n:])
                gs[mt, b] = low(total[:n])

            fy_copy(mt, b).start()

            @pl.when(b != z)
            def _():
                edge_copy(mt, b).start()

        loop(Z, lambda i: block(farthest(i)))

    def ffn_reduce_y(mt, i):
        zz = farthest(i)
        fy_copy(mt, zz).wait_recv()
        gk[mt, zz, :main] = low(wide(gk[mt, zz, :main]) + wide(yb_f[mt, zz, :main]))

        @pl.when((zz == mate) | (at_end & (zz != z)))
        def _():
            fz_copy(mt, zz).start()

    def ffn_relay(mt):
        def each(i):
            zz = farthest(i)

            @pl.when(is_far(zz) & jnp.logical_not(at_end))
            def _():
                fz_arrival(mt, zz).wait_recv()
                gk[mt, zz] = low(wide(gk[mt, zz]) + wide(zb_f[mt, zz]))
                fz_copy(mt, zz).start()

        loop(Z, each)

    def ffn_reduce_own(mt):
        fz_arrival(mt, mate).wait_recv()
        fz_arrival(mt, z).wait_recv()
        total = wide(gk[mt, z]) + wide(zb_f[mt, mate]) + wide(zb_f[mt, z])
        edge_y(mt).wait_recv()
        gk[mt, z, :main] = low(total[:main])
        gk[mt, z, main:] = low(total[main:] + wide(yb_f[mt, z, main:]))
        deepen(gk.at[mt, z], piece(mt, 0))
        for m in range(2):

            @pl.when(mt == m)
            def _(m=m):
                final_keep(m).start()
                final_copy(m, 0).start()
                final_copy(m, 1).start()

    def ffn_reduce_far(mt):
        for m in range(2):

            @pl.when(mt == m)
            def _(m=m):
                final_arrival(m, 1).wait_recv()
                final_copy(m, 2).start()

    def column(j, at=None):
        block = small_all[: D] if at is None else small_all[at, :]
        return wide(block)[:, j : j + 1]

    def statistics(values):
        center = values - jnp.mean(values, axis=0, keepdims=True)
        inverse = lax.rsqrt(jnp.mean(center * center, axis=0, keepdims=True) + EPSILON)
        return center * inverse, inverse

    def norm_back(upstream, normed, inverse, gain):
        scaled = upstream * gain
        return inverse * (
            scaled
            - jnp.mean(scaled, axis=0, keepdims=True)
            - normed * jnp.mean(scaled * normed, axis=0, keepdims=True)
        )

    def total_of(values):
        return jnp.sum(values, axis=1, keepdims=True)

    extra = [here.flip_rep(b) for b in range(2, rep_bits)]

    def schedule(steps):
        def body(at):
            for act in dict.fromkeys(step[0] for step in steps):
                slots = [(i, step[1:]) for i, step in enumerate(steps) if step[0] is act]
                hit = at == slots[0][0]
                for i, _ in slots[1:]:
                    hit = hit | (at == i)

                @pl.when(hit)
                def _(act=act, slots=slots):
                    picked = []
                    for j in range(len(slots[0][1])):
                        values = [args[j] for _, args in slots]
                        pick = jnp.int32(values[0])
                        if len(set(values)) > 1:
                            for (i, _), value in zip(slots[1:], values[1:]):
                                pick = jnp.where(at == i, value, pick)
                        picked.append(pick)
                    act(*picked)

        loop(len(steps), body)

    def ranges(head, served):
        def run(first, last):
            def each(h, carry):
                head(h)
                return carry

            lax.fori_loop(first, last, each, 0)

        steps, first = [], 0
        for h in sorted(served):
            steps += [(run, first, h + 1)] + served[h]
            first = h + 1
        if first < H:
            steps += [(run, first, H)]
        return steps

    local = s.l_sem

    def pull_io(ref, i):
        return pltpu.make_async_copy(ref, ioT, local.at[i])

    def opening(raw_con, turned, cut, piece_con, raw_cot, small_rows, small_own):
        put_in = pltpu.make_async_copy(ain_ref, w_io.at[rows(3 * n * g, 0, 3 * n), :], local.at[0])
        put_out = pltpu.make_async_copy(aout_ref, w_io.at[rows(3 * D + n * g, 0, n), :], local.at[1])
        put_exp = pltpu.make_async_copy(
            exp_ref.at[rows(n * q, 0, n), :], w_ffn.at[0, rows(n * g, 0, n), :], local.at[2]
        )
        pull_con = pltpu.make_async_copy(con_ref, raw_con, local.at[3])
        pull_cot = pltpu.make_async_copy(cot_ref, raw_cot, local.at[4])
        pull_tok = pull_io(tok_ref, 5)
        put_in.start()
        put_out.start()
        pull_tok.start()
        put_exp.start()
        pull_cot.start()
        pull_con.start()
        small_rows[...] = jnp.zeros_like(small_rows)
        for j, ref in enumerate(vector_refs[:8]):
            small_rows[j : j + 1, :] = wide(ref[...]).reshape(1, n)
        expand_bias = wide(vector_refs[8][...]).reshape(1, Q * n)
        for j in range(Q):
            small_rows[8 + j : 9 + j, :] = expand_bias[:, j * n : (j + 1) * n]
        small_own[...] = low(small_rows[...].T)
        put_small = pltpu.make_async_copy(small_own, small_all.at[rows(n * g, 0, n), :], s.k_sem.at[0])
        put_small.start()
        greet(here, extra)
        put_in.wait()
        put_small.wait()
        small_copy(0, True).start()
        put_out.wait()
        put_exp.wait()
        ends = []
        end = 0
        for i in range(len_ref.shape[1]):
            end = end + len_ref[0, i]
            ends.append(end)

        def labels(position):
            number = jnp.zeros(position.shape, jnp.int32)
            for end in ends:
                number = number + jnp.where(position >= end, 1, 0)
            return jnp.where(position < ends[-1], number, len(ends) + position)

        def small_rounds(bit):
            for b in range(grp_bits):

                @pl.when(bit == b)
                def _(b=b):
                    small_copy(b, False).wait_recv()
                    if b + 1 < grp_bits:
                        small_copy(b + 1, True).start()

        def layout():
            query_slot = lax.broadcasted_iota(jnp.int32, (1, T), 1)
            key_slot = lax.broadcasted_iota(jnp.int32, (T, 1), 0)
            query_label, key_label = labels(query_slot), labels(key_slot)
            allowed = (key_slot <= query_slot) & (key_label == query_label)
            maskb[...] = jnp.where(allowed, 0.0, MASKED)
            live[...] = jnp.where(query_slot < ends[-1], 1.0, 0.0)

        def first_norm():
            pull_tok.wait()
            normed, _ = statistics(ioT[...])
            xo[1] = low(normed * column(0) + column(1))
            swap_copy(1).start()

        def upstream():
            pull_cot.wait()
            start = jnp.where(live[...] > 0.5, raw_cot[...], 0.0)
            st4[q] = low(start)
            vecT[...] = jnp.zeros_like(vecT)
            vecT[:, 7:8] = total_of(start)

        def share_start():
            share_copy(0, st4, 0).start()
            share_copy(0, st4, 1).start()

        def pass_start():
            share_arrival(0, st4, 1).wait_recv()
            share_copy(0, st4, 2).start()

        def con_block(gg):
            return pltpu.make_async_copy(
                turned.at[rows(Q * n * gg, n * q, n), :], cut.at[rows(n * gg, 0, n), :], s.k_sem.at[gg]
            )

        def cut_contract():
            pull_con.wait()
            turned[:FF] = raw_con[...].T
            loop(G, lambda gg: con_block(gg).start())
            loop(G, lambda gg: con_block(gg).wait())
            piece_con[...] = cut[:D].T
            put = pltpu.make_async_copy(piece_con, w_ffn.at[1, rows(n * g, 0, n), :], local.at[3])
            put.start()
            put.wait()

        def project():
            def block(b):
                at = pl.ds(pl.multiple_of(b * B, 16), B)
                projT[at, :] = low(dot_nn(w_io[at, :], xo[1]))

            def add_bias(first, j):
                def each(b):
                    at = pl.ds(pl.multiple_of(b * B, 16), B)
                    to = pl.ds(pl.multiple_of(first + b * B, 16), B)
                    projT[to, :] = low(dot_nn(w_io[to, :], xo[1]) + column(j, at))

                loop(D // B, each)

            add_bias(0, 2)
            loop(D // B, lambda b: block(b + D // B))
            add_bias(2 * D, 3)

        def head_forward(h):
            at = pl.multiple_of(h * HD, HD)
            query = projT[pl.ds(at, HD), :]
            key = projT[pl.ds(pl.multiple_of(D + at, HD), HD), :]
            value = projT[pl.ds(pl.multiple_of(2 * D + at, HD), HD), :]
            scores = dot_nn(low(wide(key).T), query) * scale + maskb[...]
            peak = jnp.max(scores, axis=0, keepdims=True)
            logsum = peak + jnp.log(jnp.sum(jnp.exp(scores - peak), axis=0, keepdims=True))
            lse[h] = logsum
            weights = low(jnp.exp(scores - logsum))
            xo[0, pl.ds(at, HD), :] = low(dot_nn(value, weights))

        steps = [(start_own, k) for k in range(3)] + [(small_rounds, 0), (layout,)]
        steps += [(gather_wave, 0, 0), (start_own, 3), (gather_wave, 1, 0), (small_rounds, 1), (cut_contract,)]
        steps += [(gather_wave, 2, 0), (start_ffn, 0)] + [(small_rounds, b) for b in range(2, grp_bits)]
        steps += [(first_norm,)] + [(gather_wave, i, 0) for i in range(3, Z)] + [(gather_wave, 0, 1), (gather_wave, 1, 1)]
        steps += [(start_ffn_y, 0), (gather_wave, Z, 0), (upstream,), (gather_wave, 2, 1)]
        steps += [(partner_arrivals, k) for k in range(3)] + [(ffn_wave, 0, 1), (gather_wave, 3, 1)]
        steps += [(project,), (ffn_edges, 0, 0), (gather_wave, 4, 1), (share_start,)]
        served = {
            2: [(ffn_wave, 0, 2)],
            6: [(ffn_edges, 0, 1), (start_ffn, 1)],
            11: [(ffn_wave, 0, 3), (start_ffn_y, 1)],
            14: [(ffn_edges, 0, 2)],
            16: [(pass_start,)],
        }
        steps += ranges(head_forward, served)
        schedule(steps)

    pl.run_scoped(
        opening,
        pltpu.VMEM((n, FF), BF16),
        pltpu.VMEM((FF + PAD, n), BF16),
        pltpu.VMEM((D + PAD, n), BF16),
        pltpu.VMEM((n, D), BF16),
        pltpu.VMEM((D, T), F32),
        pltpu.VMEM((128, n), F32),
        pltpu.VMEM((n, 128), BF16),
    )
    swap_copy(0).start()
    partner_arrivals(3)

    def attention_out(b):
        at = pl.ds(pl.multiple_of(b * B, 16), B)
        to = pl.ds(pl.multiple_of(3 * D + b * B, 16), B)
        resT[at, :] = ioT[at, :] + dot_nn(w_io[to, :], xo[0]) + column(4, at)

    loop(D // B, attention_out)
    pull_io(cot_ref, 5).start()
    normed, _ = statistics(resT[...])
    h24[q] = low(normed * column(5) + column(6))
    share_copy(1, h24, 0).start()
    share_copy(1, h24, 1).start()

    def dy_rows(k, zz, core):
        gg = shard(zz, core)
        row = jnp.where(k == 0, 3 * D + n * gg, 3 * n * gg + n * (k - 1))
        return rows(row, 0, n)

    def dy_swap(k, zz):
        return remote(
            projT.at[dy_rows(k, zz, 1 - c), :],
            dyp.at[k, zz],
            s.dy_send.at[k, zz],
            s.dy_recv.at[k, zz],
            here.partner,
        )

    def middle(gp4, act4, bb4):
        def expand(t):
            def block(b):
                at = pl.ds(pl.multiple_of(b * B, 16), B)
                part = wide(small_all[at, :])
                bias = part[:, 8:9]
                for j in range(1, Q):
                    bias = jnp.where(q == j, part[:, 8 + j : 9 + j], bias)
                u = dot_nn(w_ffn[0, at, :], h24[t]) + bias
                th = jnp.tanh(GELU_A * (u + GELU_B * (u * u * u)))
                act4[t, at, :] = low(0.5 * u * (1.0 + th))
                gp4[t, at, :] = 0.5 * (1.0 + th) + (0.5 * GELU_A) * u * (1.0 - th * th) * (
                    1.0 + (3.0 * GELU_B) * (u * u)
                )

            loop(D // B, block)

        def expand_step(i):
            @pl.when(i == 1)
            def _():
                share_arrival(1, h24, 0).wait_recv()

            @pl.when(i == 2)
            def _():
                share_arrival(1, h24, 1).wait_recv()
                share_copy(1, h24, 2).start()

            @pl.when(i == 3)
            def _():
                share_arrival(1, h24, 2).wait_recv()

            expand(member(i))

        def gradients():
            share_arrival(0, st4, 0).wait_recv()
            share_arrival(0, st4, 2).wait_recv()
            ffn_grads(1, st4, act4)

        def member(i):
            first = jnp.where(i == 1, here.q_partner, q)
            return jnp.where(i == 2, here.q_x, jnp.where(i == 3, here.q_far, first))

        def back_step(i):
            t = member(Q - 1 - i)

            def block(b):
                at = pl.ds(pl.multiple_of(b * B, 16), B)
                value = accP[at, :] * gp4[t, at, :]
                bb4[t, at, :] = low(value)
                vecT[at, 12:13] = vecT[at, 12:13] + total_of(value)

            accP[...] = dot_tn(w_ffn[1, :D], st4[t])
            loop(D // B, block)
            accP[...] = dot_tn(w_ffn[0, :D], bb4[t])

            @pl.when(i == 0)
            def _():
                ps[1] = low(accP[...])
                part_to_partner(0, 1).start()

            @pl.when(i == 1)
            def _():
                part_to_partner(0, 1).wait_recv()
                pS[...] = low(accP[...] + wide(prb[0, 1]))
                part_to_x(0).start()

            @pl.when(i == 2)
            def _():
                ps[0] = low(accP[...])
                part_to_partner(0, 0).start()

        def expand_gradients():
            ffn_grads(0, bb4, h24)
            for j in range(2):
                part_to_partner(0, j).wait_send()

        def out_step(i):
            t = member(Q - 1 - i)
            brT[...] = dot_nn(w_ffn[1, :D], act4[t])

            @pl.when(i == 0)
            def _():
                ps[1] = low(brT[...])
                part_to_partner(1, 1).start()

            @pl.when(i == 1)
            def _():
                gp4[1] = brT[...]

            @pl.when(i == 2)
            def _():
                ps[0] = low(brT[...])
                part_to_partner(1, 0).start()

            @pl.when(i == 3)
            def _():
                gp4[0] = brT[...]

        steps = [(ffn_edges, 0, 3), (ffn_wave, 1, 1), (ffn_y_arrivals, 0), (expand_step, 0), (ffn_wave, 1, 2), (expand_step, 1)]
        steps += [(ffn_edges, 1, 0), (ffn_wave, 1, 3), (expand_step, 2), (ffn_edges, 1, 1), (expand_step, 3)]
        steps += [(ffn_edges, 1, 2), (gradients,), (ffn_edges, 1, 3), (ffn_y_arrivals, 1)]
        steps += [(back_step, 0), (back_step, 1), (ffn_reduce_y, 1, 0), (back_step, 2), (ffn_reduce_y, 1, 1)]
        steps += [(back_step, 3), (expand_gradients,), (ffn_reduce_y, 1, 2)] + [(out_step, i) for i in range(Q)]
        steps += [(ffn_reduce_y, 1, 3)]
        schedule(steps)
        part_to_partner(0, 0).wait_recv()
        part_to_x(0).wait_recv()
        back_hidden = accP[...] + wide(prb[0, 0]) + wide(xrb[0])
        normed, inverse = statistics(resT[...])
        vecT[:, 5:6] = total_of(back_hidden * normed)
        vecT[:, 6:7] = total_of(back_hidden)
        pull_io(cot_ref, 5).wait()
        start = jnp.where(live[...] > 0.5, ioT[...], 0.0)
        brT[...] = start + norm_back(back_hidden, normed, inverse, column(5))
        projT[pl.ds(3 * D, D), :] = low(brT[...])
        loop(Z, lambda zz: dy_swap(0, zz).start())
        pull_io(tok_ref, 5).start()
        part_to_x(0).wait_send()
        part_to_partner(1, 1).wait_recv()
        pS[...] = low(gp4[1] + wide(prb[1, 1]))
        resT[...] = resT[...] + gp4[0] + column(7)
        vecT[:, 4:5] = total_of(brT[...])

    pl.run_scoped(
        middle, pltpu.VMEM((Q, D, T), F32), pltpu.VMEM((Q, D, T), BF16), pltpu.VMEM((Q, D, T), BF16)
    )
    batt = xrb.at[0]
    batt[...] = low(dot_tn(w_io[pl.ds(3 * D, D), :], projT[pl.ds(3 * D, D), :]))

    def head_backward(h):
        at = pl.multiple_of(h * HD, HD)
        at_q = pl.ds(at, HD)
        at_k = pl.ds(pl.multiple_of(D + at, HD), HD)
        at_v = pl.ds(pl.multiple_of(2 * D + at, HD), HD)
        query, key, value, up = projT[at_q, :], projT[at_k, :], projT[at_v, :], batt[at_q, :]
        scores = dot_nn(low(wide(key).T), query) * scale + maskb[...]
        probability = jnp.exp(scores - lse[h])
        weights = low(probability)
        delta = jnp.sum(wide(up) * wide(xo[0, at_q, :]), axis=0, keepdims=True)
        flow = dot_nn(low(wide(value).T), up)
        slope = low(probability * (flow - delta) * scale)
        back_query = dot_nn(key, slope)
        back_value = dot_nt(up, weights)
        vecT[at_q, 2:3] = total_of(back_query)
        vecT[at_q, 3:4] = total_of(back_value)
        projT[at_k, :] = low(dot_nt(query, slope))
        projT[at_q, :] = low(back_query)
        projT[at_v, :] = low(back_value)

    wide_out = n - give_out

    def closing(plane, xs, stage, fin, con_in, con_turn, con_tall, con_flat, vec_own):
        def x_copy(k, zz):
            return remote(xs.at[k, zz], xb.at[k, zz], s.gx_send.at[k, zz], s.gx_recv.at[k, zz], here.xnbr)

        def y_copy(k, zz):
            return remote(plane.at[k, zz], yb_a.at[k, zz], s.gy_send.at[k, zz], s.gy_recv.at[k, zz], here.ynbr)

        def z_copy(k, zz):
            slot = line_slot(zz)
            return remote(
                plane.at[k, zz], zb_a.at[k, slot], s.gz_send.at[k, zz], s.gz_recv.at[k, slot], line_target(zz)
            )

        def z_arrival(k, slot):
            return remote(
                plane.at[k, slot], zb_a.at[k, slot], s.gz_send.at[k, slot], s.gz_recv.at[k, slot], line_target(mate)
            )

        def f_copy(k):
            return remote(plane.at[k, z], fx.at[k], s.gf_send.at[k], s.gf_recv.at[k], here.xnbr)

        def o_keep(k, dst):
            return pltpu.make_async_copy(fin.at[k % 2], dst, s.go_keep.at[k])

        def o_give(k, dst):
            return remote(fin.at[k % 2], dst, s.go_send.at[k], s.go_recv.at[k], here.partner)

        any_out = in_out.at[0]

        def bring(src, slot):
            copy = pltpu.make_async_copy(src, stage.at[slot], s.st_sem.at[slot])
            copy.start()
            return copy

        def multiply(k):
            j = jnp.where(k == 0, 0, 1)

            @pl.when(k == 0)
            def _():
                swap_copy(0).wait_recv()
                swap_copy(1).wait_recv()


            def each(i):
                zz = farthest(i)
                dy_swap(k, zz).wait_recv()
                term = dot_nt(projT[dy_rows(k, zz, c), :], xo[j]) + dot_nt(dyp[k, zz], xp[j])

                @pl.when(xi == 0)
                def _():
                    plane[k, zz] = low(term[:wide_out])
                    xs[k, zz] = low(term[wide_out:])

                @pl.when(xi == 1)
                def _():
                    plane[k, zz] = low(term[give_out:])
                    xs[k, zz] = low(term[:give_out])

                x_copy(k, zz).start()

            loop(Z, each)

        def after_x(k):
            def each(i):
                zz = farthest(i)
                x_copy(k, zz).wait_recv()
                got = wide(xb[k, zz])

                @pl.when(xi == 0)
                def _():
                    plane[k, zz, :give_out] = low(wide(plane[k, zz, :give_out]) + got)

                @pl.when(xi == 1)
                def _():
                    edge = wide_out - give_out
                    plane[k, zz, edge:] = low(wide(plane[k, zz, edge:]) + got)

                @pl.when(y != c)
                def _():
                    y_copy(k, zz).start()

            loop(Z, each)

        def after_y(k):
            @pl.when(source)
            def _():
                def fetch(i):
                    zz = farthest(i)
                    y_copy(k, zz).wait_recv()
                    bring(yb_a.at[k, zz], i)

                def add(i):
                    zz = farthest(i)
                    pltpu.make_async_copy(yb_a.at[k, zz], stage.at[i], s.st_sem.at[i]).wait()
                    plane[k, zz] = low(wide(plane[k, zz]) + wide(stage[i]))

                    @pl.when((zz == mate) | (at_end & (zz != z)))
                    def _():
                        z_copy(k, zz).start()

                def step(i):
                    @pl.when(i < Z)
                    def _():
                        fetch(i)

                    @pl.when(i > 0)
                    def _():
                        add(i - 1)

                loop(Z + 1, step)

        def relay(k):
            def each(i):
                zz = farthest(i)

                @pl.when(source & is_far(zz) & jnp.logical_not(at_end))
                def _():
                    z_arrival(k, zz).wait_recv()
                    bring(zb_a.at[k, zz], i).wait()
                    plane[k, zz] = low(wide(plane[k, zz]) + wide(stage[i]))
                    z_copy(k, zz).start()

            loop(Z, each)

        def after_z(k):
            @pl.when(source)
            def _():
                z_arrival(k, mate).wait_recv()
                near = bring(zb_a.at[k, mate], 0)
                z_arrival(k, z).wait_recv()
                far = bring(zb_a.at[k, z], 1)
                near.wait()
                far.wait()
                plane[k, z] = low(wide(plane[k, z]) + wide(stage[0]) + wide(stage[1]))
                f_copy(k).start()

        def finish(k):
            @pl.when(source)
            def _():
                f_copy(k).wait_recv()

                @pl.when(k >= 2)
                def _():
                    o_keep(k - 2, any_out).wait()
                    o_give(k - 2, any_out).wait_send()

                slot = k % 2

                def assemble(first, second):
                    fin[slot, :give_out] = first[:give_out]
                    fin[slot, give_out:wide_out] = low(
                        wide(first[give_out:]) + wide(second[: wide_out - give_out])
                    )
                    fin[slot, wide_out:] = second[wide_out - give_out :]

                @pl.when(xi == 0)
                def _():
                    assemble(plane[k, z], fx[k])

                @pl.when(xi == 1)
                def _():
                    assemble(fx[k], plane[k, z])

                deepen(fin.at[slot], k)
                @pl.when(k == 0)
                def _():
                    o_keep(k, out_out).start()
                    o_give(k, out_out).start()

                @pl.when(k > 0)
                def _():
                    o_keep(k, in_out.at[k - 1]).start()
                    o_give(k, in_out.at[k - 1]).start()


        def vec_copy(i):
            target_r, target_g = here.flip_rep(0)
            for b in range(1, rep_bits):
                other = here.flip_rep(b)
                target_r = jnp.where(i == b, other[0], target_r)
                target_g = jnp.where(i == b, other[1], target_g)
            for b in range(grp_bits):
                other = here.flip_grp(b)
                target_r = jnp.where(i == rep_bits + b, other[0], target_r)
                target_g = jnp.where(i == rep_bits + b, other[1], target_g)
            return remote(
                vec_buf.at[i], vec_got.at[i], s.v_send.at[i], s.v_recv.at[i], (target_r, target_g)
            )

        def swap_all():
            for k in range(1, N):
                loop(Z, lambda zz, k=k: dy_swap(k, zz).start())

        def last_norm():
            back_hidden = dot_tn(w_io[pl.ds(0, 3 * D), :], projT[: 3 * D])
            pull_io(tok_ref, 5).wait()
            normed, inverse = statistics(ioT[...])
            vecT[:, 0:1] = total_of(back_hidden * normed)
            vecT[:, 1:2] = total_of(back_hidden)
            accP[...] = brT[...] + norm_back(back_hidden, normed, inverse, column(0))
            tg_copy.start()
            spread = vecT[:, 12:13]
            for j in range(Q):
                vecT[:, 8 + j : 9 + j] = jnp.where(q == j, spread, 0.0)
            vec_buf[0] = vecT[...].T[:16]
            vec_copy(0).start()

        tg_copy = pltpu.make_async_copy(accP, tg_out, local.at[1])
        bo_copy = pltpu.make_async_copy(resT, bo_out, local.at[0])
        push_vec = pltpu.make_async_copy(vec_own, vec_out, local.at[2])

        def send_out():
            part_to_x(1).start()

        def block_done():
            part_to_partner(1, 0).wait_recv()
            part_to_x(1).wait_recv()
            output = resT[...] + wide(prb[1, 0]) + wide(xrb[1])
            resT[...] = jnp.where(live[...] > 0.5, output, 0.0)
            bo_copy.start()

        def vec_round(t):
            vec_copy(t).wait_recv()
            vec_buf[t + 1] = vec_buf[t] + vec_got[t]

            @pl.when(t + 1 < rounds)
            def _():
                vec_copy(t + 1).start()

            @pl.when(t + 1 == rounds)
            def _():
                vecT[:, :16] = vec_buf[rounds].T
                vec_own[...] = vecT[pl.ds(pl.multiple_of(n * g, 8), n), :].T[:16]
                push_vec.start()

        def bring_piece(j):
            return pltpu.make_async_copy(con_raw.at[j], con_in.at[j % 2], s.k_sem.at[2 * G + j % 2])

        def put_block(j, gg):
            return pltpu.make_async_copy(
                con_turn.at[j % 2, rows(n * gg, 0, n), :],
                con_cut.at[rows(Q * n * gg, n * j, n), :],
                s.k_sem.at[G * (j % 2) + gg],
            )

        def con_finals():
            final_keep(1).wait()
            final_arrival(1, 0).wait_recv()
            final_arrival(1, 2).wait_recv()
            bring_piece(0).start()
            bring_piece(1).start()

        def con_piece(j):
            bring_piece(j).wait()

            @pl.when(j >= 2)
            def _():
                loop(G, lambda gg: put_block(j - 2, gg).wait())

            con_turn[j % 2, :D] = con_in[j % 2].T

            @pl.when(j + 2 < Q)
            def _():
                bring_piece(j + 2).start()

            loop(G, lambda gg: put_block(j, gg).start())

        half_size = FF // 2

        def bring_side(half):
            return pltpu.make_async_copy(
                con_cut.at[rows(half_size * half, 0, half_size), :], con_tall, s.k_sem.at[2 * G + 2]
            )

        def put_side(half):
            to = pl.ds(pl.multiple_of(half_size * half, 128), half_size)
            return pltpu.make_async_copy(con_flat, con_out.at[:, to], s.k_sem.at[2 * G + 3])

        def con_side(i):
            @pl.when(i == 0)
            def _():
                loop(G, lambda gg: put_block(Q - 2, gg).wait())
                loop(G, lambda gg: put_block(Q - 1, gg).wait())
                bring_side(0).start()

            @pl.when(i > 0)
            def _():
                half = i - 1
                bring_side(half).wait()

                @pl.when(half == 1)
                def _():
                    put_side(0).wait()

                con_flat[...] = con_tall[...].T
                put_side(half).start()

                @pl.when(half == 0)
                def _():
                    bring_side(1).start()

        served = {7: [(edge_over, 1), (ffn_relay, 1)], 13: [(edge_over, 0), (ffn_reduce_y, 0, 0)]}
        steps = [(multiply, 0)] + ranges(head_backward, served)
        steps += [(swap_all,), (last_norm,), (multiply, 1), (ffn_reduce_y, 0, 1), (vec_round, 0), (after_x, 0)]
        steps += [(multiply, 2), (multiply, 3), (ffn_reduce_y, 0, 2), (ffn_reduce_y, 0, 3), (after_x, 1), (vec_round, 1)]
        steps += [(send_out,)]
        steps += [(ffn_reduce_own, 1), (after_x, 2), (after_y, 0), (ffn_relay, 0), (after_x, 3)]
        steps += [(relay, 0), (after_y, 1), (vec_round, 2), (relay, 1), (after_y, 2), (after_z, 0)]
        steps += [(relay, 2), (after_y, 3), (after_z, 1), (vec_round, 3), (relay, 3)]
        steps += [(ffn_reduce_far, 1), (finish, 0), (ffn_reduce_own, 0), (after_z, 2), (con_finals,), (finish, 1), (con_piece, 0)]
        steps += [(con_piece, 1), (con_piece, 2), (con_piece, 3), (block_done,), (after_z, 3), (con_side, 0), (vec_round, 4)]
        steps += [(finish, 2), (con_side, 1), (con_side, 2), (ffn_reduce_far, 0), (finish, 3)]
        steps += [(vec_round, t) for t in range(5, rounds)]
        schedule(steps)

        def settle(k):
            @pl.when(source)
            def _():
                @pl.when(z < Z - 1)
                def _():
                    own_copy(k, 0).wait_send()

                @pl.when(z > 0)
                def _():
                    own_copy(k, 1).wait_send()

                own_copy(k, 2).wait_send()

            def each(zz):
                @pl.when((y != c) | (zz != z))
                def _():
                    over_x(k, zz).wait_send()
                    plane_to_partner(k, zz, c).wait_send()
                    rest_to_partner(k, zz, c).wait_send()

                @pl.when(source & (zz != z))
                def _():
                    over_y(k, zz, y).wait_send()

                    @pl.when(goes_on(zz))
                    def _():
                        passing(k, zz).wait_send()

                x_copy(k, zz).wait_send()
                dy_swap(k, zz).wait_send()

                @pl.when(y != c)
                def _():
                    y_copy(k, zz).wait_send()

                @pl.when(source & (zz != z))
                def _():
                    z_copy(k, zz).wait_send()

            loop(Z, each)

            @pl.when(source)
            def _():
                f_copy(k).wait_send()

                @pl.when(k >= N - 2)
                def _():
                    o_keep(k, any_out).wait()
                    o_give(k, any_out).wait_send()

            @pl.when(y != c)
            def _():
                o_give(k, any_out).wait_recv()

        loop(N, settle)

        def settle_ffn(mt):
            @pl.when(z < Z - 1)
            def _():
                ffn_own(mt, 0).wait_send()
                edge_own(mt, 0).wait_send()

            @pl.when(z > 0)
            def _():
                ffn_own(mt, 1).wait_send()
                edge_own(mt, 1).wait_send()


            ffn_own_y(mt).wait_send()

            edge_y(mt).wait_send()

            def each(zz):
                fy_copy(mt, zz).wait_send()

                @pl.when(zz != z)
                def _():
                    ffn_over_y(mt, zz, y).wait_send()

                    @pl.when(goes_on(zz))
                    def _():
                        ffn_pass(mt, zz).wait_send()
                        edge_pass(mt, zz).wait_send()

                @pl.when(zz != z)
                def _():
                    fz_copy(mt, zz).wait_send()
                    edge_copy(mt, zz).wait_send()

            loop(Z, each)

        for mt in range(2):
            settle_ffn(mt)
            for kind in range(3):
                final_copy(mt, kind).wait_send()
        final_keep(0).wait()
        put_side(1).wait()
        final_arrival(0, 0).wait_recv()
        final_arrival(0, 2).wait_recv()
        for e, buf in ((0, st4), (1, h24)):
            for kind in range(3):
                share_copy(e, buf, kind).wait_send()
        for i in range(2):
            swap_copy(i).wait_send()
        for j in range(2):
            part_to_partner(1, j).wait_send()
        part_to_x(1).wait_send()
        for bit in range(grp_bits):
            small_copy(bit, True).wait_send()
        loop(rounds, lambda i: vec_copy(i).wait_send())
        bo_copy.wait()
        tg_copy.wait()
        push_vec.wait()

    pl.run_scoped(
        closing,
        pltpu.VMEM((N, Z, wide_out, D), BF16),
        pltpu.VMEM((N, Z, give_out, D), BF16),
        pltpu.VMEM((Z, wide_out, D), BF16),
        pltpu.VMEM((2, n, D), BF16),
        pltpu.VMEM((2, n, D), BF16),
        pltpu.VMEM((2, D + PAD, n), BF16),
        pltpu.VMEM((FF // 2, n), BF16),
        pltpu.VMEM((n, FF // 2), BF16),
        pltpu.VMEM((16, n), F32),
    )


def run_layer(lengths, tokens, cotangent, a_in, a_out, w_exp, w_con, vectors, R, G):
    D, T = tokens.shape
    FF = w_con.shape[1]
    n = D // G
    H = D // HD
    Z = G // YSIZE
    Q = TEAM
    N = 4
    give_in = (6 * n // 17) // 8 * 8
    give_out = (6 * n // 17) // 8 * 8
    wide_out = n - give_out
    rounds = bits_of(R) + bits_of(G)
    deep = bits_of(R) - 2
    dma = pltpu.SemaphoreType.DMA
    v = pltpu.VMEM
    scratch = dict(
        w_io=v((4 * D + PAD, D), BF16),
        w_ffn=v((2, D + PAD, D), BF16),
        small_all=v((D + PAD, 128), BF16),
        ioT=v((D, T), F32),
        xo=v((2, D, T), BF16),
        xp=v((2, D, T), BF16),
        projT=v((4 * D + PAD, T), BF16),
        resT=v((D, T), F32),
        h24=v((Q, D, T), BF16),
        st4=v((Q, D, T), BF16),
        brT=v((D, T), F32),
        dyp=v((N, Z, n, T), BF16),
        ps=v((2, D, T), BF16),
        pS=v((D, T), BF16),
        prb=v((2, 2, D, T), BF16),
        xrb=v((2, D, T), BF16),
        accP=v((D, T), F32),
        lse=v((H, 1, T), F32),
        maskb=v((T, T), F32),
        live=v((1, T), F32),
        vecT=v((D, 128), F32),
        vec_buf=v((rounds + 1, 16, D), F32),
        vec_got=v((rounds, 16, D), F32),
        gk=v((2, Z, n, D), BF16),
        gs=v((2, Z, n, D), BF16),
        yb_f=v((2, Z, n, D), BF16),
        zb_f=v((2, Z, n, D), BF16),
        zb_e=v((2, Z, (3 * n // 17) // 8 * 8, D), BF16),
        xb=v((N, Z, give_out, D), BF16),
        fx=v((N, wide_out, D), BF16),
        d_tmp=v((n, D) if deep > 0 else (8, 128), BF16),
        l_sem=dma((6,)),
        k_sem=dma((2 * G + 4,)),
        a_own=dma((N, 3)),
        w_own=dma((2, 3)),
        e_send=dma((2, 3)),
        e_recv=dma((2, 3)),
        p_send=dma((2,)),
        p_recv=dma((2,)),
        r_send=dma((2, 3)),
        r_recv=dma((2, 3)),
        s_send=dma((bits_of(G),)),
        s_recv=dma((bits_of(G),)),
        v_send=dma((rounds,)),
        v_recv=dma((rounds,)),
        fo_send=dma((2, 3)),
        fo_recv=dma((2, 3)),
        fo_keep=dma((2,)),
        fz_recv=dma((2, Z)),
        gz_recv=dma((N, Z)),
        gf_send=dma((N,)),
        gf_recv=dma((N,)),
        go_keep=dma((N,)),
        go_send=dma((N,)),
        go_recv=dma((N,)),
        st_sem=dma((Z,)),
        d_send=dma,
        d_local=dma,
        d_recv=dma((N + 2 * Q, max(deep, 1))),
        u_own=dma((2, 2)),
        ue_send=dma((2,)),
        ue_recv=dma((2,)),
        uz_send=dma((2, Z)),
        uz_recv=dma((2, Z)),
        u_rz=dma((2, Z)),
        u_fwd=dma((2, Z)),
        w_rz=dma((2, Z)),
        w_ry=dma((2, Z)),
        w_fwd=dma((2, Z)),
        w_y=dma((2, Z)),
        fy_send=dma((2, Z)),
        fy_recv=dma((2, Z)),
        fz_send=dma((2, Z)),
        a_rp=dma((N, Z)),
        a_rx=dma((N, Z)),
        a_rcp=dma((N, Z)),
        a_rcx=dma((N, Z)),
        a_fwd=dma((N, Z)),
        a_y=dma((N, Z)),
        a_x=dma((N, Z)),
        a_cp=dma((N, Z)),
        a_cx=dma((N, Z)),
        gx_send=dma((N, Z)),
        gx_recv=dma((N, Z)),
        gy_send=dma((N, Z)),
        gy_recv=dma((N, Z)),
        gz_send=dma((N, Z)),
        dy_send=dma((N, Z)),
        dy_recv=dma((N, Z)),
    )
    hbm = pl.BlockSpec(memory_space=pl.ANY)
    outs = pl.pallas_call(
        functools.partial(layer_kernel, R, G, give_in, give_out, tuple(scratch)),
        out_shape=(
            jax.ShapeDtypeStruct((D, T), F32),
            jax.ShapeDtypeStruct((D, T), F32),
            jax.ShapeDtypeStruct((3, n, D), BF16),
            jax.ShapeDtypeStruct((n, D), BF16),
            jax.ShapeDtypeStruct((Q, n, D), BF16),
            jax.ShapeDtypeStruct((n, FF), BF16),
            jax.ShapeDtypeStruct((16, n), F32),
            jax.ShapeDtypeStruct((Q, n, D), BF16),
            jax.ShapeDtypeStruct((FF, n), BF16),
            jax.ShapeDtypeStruct((N, Z, wide_out, D), BF16),
            jax.ShapeDtypeStruct((N, Z, wide_out, D), BF16),
            jax.ShapeDtypeStruct((N + 2 * Q, deep, n, D) if deep > 0 else (1, 1, 8, 128), BF16),
        ),
        in_specs=[pl.BlockSpec(memory_space=pltpu.SMEM)] + [hbm] * 6 + [pl.BlockSpec(memory_space=pltpu.VMEM)] * 9,
        out_specs=(hbm,) * 12,
        scratch_shapes=list(scratch.values()),
        compiler_params=pltpu.CompilerParams(collective_id=0, has_side_effects=True, vmem_limit_bytes=VMEM_LIMIT),
        name="layer",
    )(lengths, tokens, cotangent, a_in, a_out, w_exp, w_con, *vectors)
    return outs[:7]


def per_device(
    tokens,
    document_lengths,
    cotangent,
    first_gain,
    first_shift,
    attention_in,
    query_bias,
    value_bias,
    attention_out,
    output_bias,
    second_gain,
    second_shift,
    expand_weight,
    expand_bias,
    contract_weight,
    contract_bias,
):
    R, G = lax.axis_size("rep"), lax.axis_size("grp")
    T, D = tokens.shape
    n = D // G
    Q = TEAM
    vectors = [
        first_gain,
        first_shift,
        query_bias,
        value_bias,
        output_bias,
        second_gain,
        second_shift,
        contract_bias,
        expand_bias,
    ]
    block_t, tokens_t, in_grad, out_grad, exp_grad, con_grad, share = run_layer(
        document_lengths,
        tokens.T,
        cotangent.T,
        attention_in.T,
        attention_out.T,
        expand_weight.T,
        contract_weight.T,
        vectors,
        R,
        G,
    )
    out_grad = out_grad.T.astype(F32)
    in_grad = in_grad.reshape(3 * n, D).T.astype(F32)
    exp_grad = exp_grad.reshape(Q * n, D).T.astype(F32)
    con_grad = con_grad.T.astype(F32)
    return (
        block_t.T,
        tokens_t.T,
        share[0],
        share[1],
        in_grad,
        share[2],
        share[3],
        out_grad,
        share[4],
        share[5],
        share[6],
        exp_grad,
        share[8 : 8 + Q].reshape(Q * n),
        con_grad,
        share[7],
    )


def solution(mesh):
    rows = P(("rep", "grp"), None)
    split, columns = P("grp"), P(None, "grp")
    return jax.shard_map(
        per_device,
        mesh=mesh,
        in_specs=(
            rows,
            rows,
            rows,
            split,
            split,
            columns,
            split,
            split,
            columns,
            split,
            split,
            split,
            columns,
            split,
            columns,
            split,
        ),
        out_specs=(
            rows,
            rows,
            split,
            split,
            columns,
            split,
            split,
            columns,
            split,
            split,
            split,
            columns,
            split,
            columns,
            split,
        ),
        check_vma=False,
    )
```

```python
import functools
import types

import jax
import jax.numpy as jnp
from jax import lax
from jax.experimental import pallas as pl
from jax.experimental.pallas import tpu as pltpu
from jax.sharding import PartitionSpec as P

HD = 64
EPSILON = 1e-05
MASKED = -1e30
PAD = 8
YSIZE = 2
TEAM = 4
GELU_A = 0.7978845608028654
GELU_B = 0.044715
MESH_ID = pl.DeviceIdType.MESH
VMEM_LIMIT = 67043328
BF16, F32 = jnp.bfloat16, jnp.float32


def bits_of(count):
    return count.bit_length() - 1


def dot_nn(left, right):
    return lax.dot_general(left, right, (((1,), (0,)), ((), ())), preferred_element_type=F32)


def dot_nt(left, right):
    return lax.dot_general(left, right, (((1,), (1,)), ((), ())), preferred_element_type=F32)


def dot_tn(left, right):
    return lax.dot_general(left, right, (((0,), (0,)), ((), ())), preferred_element_type=F32)


def remote(src, dst, send, recv, target):
    return pltpu.make_async_remote_copy(
        src_ref=src, dst_ref=dst, send_sem=send, recv_sem=recv, device_id=target, device_id_type=MESH_ID
    )


def wide(value):
    return value.astype(F32)


def low(value):
    return value.astype(BF16)


class Place:
    def __init__(self, rep_count, grp_count):
        self.R, self.G = rep_count, grp_count
        self.Z = grp_count // YSIZE
        self.r = lax.axis_index("rep")
        self.g = lax.axis_index("grp")
        self.c = self.r % 2
        self.xi = (self.r // 2) % 2
        self.q = self.r % TEAM
        self.z = self.g // YSIZE
        self.y = self.g % YSIZE
        self.partner = (self.r + 1 - 2 * self.c, self.g)
        self.xnbr = (self.r + 2 - 4 * self.xi, self.g)
        self.ynbr = (self.r, self.g + 1 - 2 * self.y)
        self.up = (self.r, self.g + YSIZE)
        self.down = (self.r, self.g - YSIZE)
        self.q_partner = self.q + 1 - 2 * self.c
        self.q_x = self.q + 2 - 4 * self.xi
        self.q_far = self.q_x + 1 - 2 * self.c

    def on_line(self, zz):
        return (self.r, zz * YSIZE + self.y)

    def flip_rep(self, bit):
        on = (self.r // (1 << bit)) % 2
        return (self.r + (1 << bit) - (2 << bit) * on, self.g)

    def flip_grp(self, bit):
        on = (self.g // (1 << bit)) % 2
        return (self.r, self.g + (1 << bit) - (2 << bit) * on)


def greet(here, others):
    barrier = pltpu.get_barrier_semaphore()

    def hello(target):
        pl.semaphore_signal(barrier, inc=1, device_id=target, device_id_type=MESH_ID)

    for target in [here.partner, here.xnbr, here.ynbr] + others:
        hello(target)
    for zz in range(here.Z):

        @pl.when(here.z != zz)
        def _(zz=zz):
            hello(here.on_line(zz))

    pl.semaphore_wait(barrier, 2 + here.Z + len(others))


def loop(count, body):
    def step(i, carry):
        body(i)
        return carry

    lax.fori_loop(0, count, step, 0)


def layer_kernel(R, G, give_in, give_out, names, *refs):
    len_ref, tok_ref, cot_ref, ain_ref, aout_ref, exp_ref, con_ref = refs[:7]
    vector_refs = refs[7:16]
    bo_out, tg_out, in_out, out_out, exp_out, con_out, vec_out, con_raw, con_cut, yb_a, zb_a, deep_buf = refs[16:28]
    s = types.SimpleNamespace(**dict(zip(names, refs[28:])))
    ffn_out = (exp_out, con_raw)
    here = Place(R, G)
    Z, z, y, c, xi, q, g = here.Z, here.z, here.y, here.c, here.xi, here.q, here.g
    D, T = tok_ref.shape
    n = D // G
    H = D // HD
    Q = TEAM
    FF = con_ref.shape[1]
    n4 = Q * n
    B = 2 * n
    scale = HD ** (-0.5)
    rep_bits, grp_bits = bits_of(R), bits_of(G)
    rounds = rep_bits + grp_bits
    w_io, w_ffn = s.w_io, s.w_ffn
    ioT, xo, xp, projT, resT = s.ioT, s.xo, s.xp, s.projT, s.resT
    h24, st4, brT = s.h24, s.st4, s.brT
    dyp, ps, pS, prb, xrb, accP = s.dyp, s.ps, s.pS, s.prb, s.xrb, s.accP
    lse, maskb, live, vecT = s.lse, s.maskb, s.live, s.vecT
    vec_buf, vec_got = s.vec_buf, s.vec_got
    gk, gs, yb_f, zb_f = s.gk, s.gs, s.yb_f, s.zb_f
    xb, fx, small_all = s.xb, s.fx, s.small_all

    N = 4
    wide_in = n - give_in
    start_in = xi * give_in
    giving = xi * wide_in
    taking = (1 - xi) * wide_in

    def io_row(k, gg):
        return jnp.where(k < 3, 3 * n * gg + n * k, 3 * D + n * gg)

    first_y = (3 * n // 17) // 8 * 8

    def rows(base, offset, size):
        return pl.ds(pl.multiple_of(base + offset, 8), size)

    def plane_w(k, gg):
        return w_io.at[rows(io_row(k, gg), start_in, wide_in), :]

    def gift_w(k, gg):
        return w_io.at[rows(io_row(k, gg), giving, give_in), :]

    def due_w(k, gg):
        return w_io.at[rows(io_row(k, gg), taking, give_in), :]

    def shard(zz, yy):
        return zz * YSIZE + yy

    def farthest(i):
        table = [sorted(range(Z), key=lambda p: -abs(p - at)) for at in range(Z)]
        pick = jnp.int32(0)
        for at in range(Z):
            for j in range(Z):
                pick = jnp.where((z == at) & (i == j), table[at][j], pick)
        return pick

    assert Z == 4
    at_end = (z == 0) | (z == Z - 1)
    mate = z + 1 - 2 * (z % 2)

    def is_far(zz):
        return (zz != z) & (zz != mate)

    def line_target(zz):
        return here.on_line(jnp.where((zz == mate) | at_end, mate, zz))

    def line_slot(zz):
        return jnp.where(zz == mate, z, zz)

    def goes_on(zz):
        return ((zz < z) & (z < Z - 1)) | ((zz > z) & (z > 0))

    source = y == c
    onward_of = lambda zz: (here.r, g + jnp.where(zz < z, YSIZE, -YSIZE))

    def own_copy(k, way):
        ref = plane_w(k, g)
        return remote(ref, ref, s.a_own.at[k, way], s.a_rp.at[k, z], (here.up, here.down, here.ynbr)[way])

    def passing(k, zz):
        ref = plane_w(k, shard(zz, y))
        return remote(ref, ref, s.a_fwd.at[k, zz], s.a_rp.at[k, zz], onward_of(zz))

    def over_y(k, zz, yy):
        ref = plane_w(k, shard(zz, yy))
        return remote(ref, ref, s.a_y.at[k, zz], s.a_rp.at[k, zz], here.ynbr)

    def over_x(k, zz):
        ref = gift_w(k, shard(zz, c))
        return remote(ref, ref, s.a_x.at[k, zz], s.a_rx.at[k, zz], here.xnbr)

    def x_arrival(k, zz):
        ref = due_w(k, shard(zz, c))
        return remote(ref, ref, s.a_x.at[k, zz], s.a_rx.at[k, zz], here.xnbr)

    def plane_to_partner(k, zz, core):
        ref = plane_w(k, shard(zz, core))
        return remote(ref, ref, s.a_cp.at[k, zz], s.a_rcp.at[k, zz], here.partner)

    def rest_to_partner(k, zz, core):
        ref = due_w(k, shard(zz, core))
        return remote(ref, ref, s.a_cx.at[k, zz], s.a_rcx.at[k, zz], here.partner)

    def ffn_w(mt, gg):
        return w_ffn.at[mt, rows(n * gg, 0, n), :]

    def ffn_own(mt, way):
        ref = ffn_w(mt, g)
        return remote(ref, ref, s.w_own.at[mt, way], s.w_rz.at[mt, z], (here.up, here.down, here.ynbr)[way])

    def ffn_own_y(mt):
        ref = ffn_w(mt, g)
        return remote(ref, ref, s.w_own.at[mt, 2], s.w_ry.at[mt, z], here.ynbr)

    def ffn_pass(mt, zz):
        ref = ffn_w(mt, shard(zz, y))
        return remote(ref, ref, s.w_fwd.at[mt, zz], s.w_rz.at[mt, zz], onward_of(zz))

    def ffn_over_y(mt, zz, yy):
        ref = w_ffn.at[mt, rows(n * shard(zz, yy), 0, n - first_y), :]
        return remote(ref, ref, s.w_y.at[mt, zz], s.w_ry.at[mt, zz], here.ynbr)

    def ffn_own_y_arrival(mt):
        ref = ffn_w(mt, shard(z, 1 - y))
        return remote(ref, ref, s.w_own.at[mt, 2], s.w_ry.at[mt, z], here.ynbr)

    def ffn_edge(mt, zz):
        return w_ffn.at[mt, rows(n * shard(zz, 1 - y), n - first_y, first_y), :]

    def edge_own(mt, way):
        ref = ffn_edge(mt, z)
        return remote(ref, ref, s.u_own.at[mt, way], s.u_rz.at[mt, z], (here.up, here.down)[way])

    def edge_pass(mt, zz):
        ref = ffn_edge(mt, zz)
        return remote(ref, ref, s.u_fwd.at[mt, zz], s.u_rz.at[mt, zz], onward_of(zz))

    def start_own(k):
        @pl.when(source)
        def _():
            @pl.when(z < Z - 1)
            def _():
                own_copy(k, 0).start()

            @pl.when(z > 0)
            def _():
                own_copy(k, 1).start()

            own_copy(k, 2).start()

    def start_ffn(mt):
        @pl.when(z < Z - 1)
        def _():
            ffn_own(mt, 0).start()

        @pl.when(z > 0)
        def _():
            ffn_own(mt, 1).start()

    def start_ffn_y(mt):
        ffn_own_y(mt).start()

    def both_sides(distance, act):
        def side(i):
            zz = z + jnp.where(i == 0, -distance, distance)

            @pl.when((zz >= 0) & (zz < Z) & ((i == 0) | (distance > 0)))
            def _():
                act(zz)

        loop(2, side)

    def gather_wave(d, part):
        def plane_step(j):
            k = 3 * part + j

            @pl.when((k < N) & source & (d > 0))
            def _():
                def arrived(zz):
                    passing(k, zz).wait_recv()

                    @pl.when(goes_on(zz))
                    def _():
                        passing(k, zz).start()

                    over_y(k, zz, y).start()
                    over_x(k, zz).start()
                    plane_to_partner(k, zz, c).start()

                both_sides(d, arrived)

            @pl.when((k < N) & (y != c))
            def _():
                def arrived(zz):
                    over_y(k, zz, c).wait_recv()
                    over_x(k, zz).start()
                    plane_to_partner(k, zz, c).start()

                both_sides(d, arrived)

        def x_step(j):
            k = 3 * part + j

            @pl.when((k < N) & ((d > 1) | ((d > 0) & (y != c))))
            def _():
                def arrived(zz):
                    x_arrival(k, zz).wait_recv()
                    rest_to_partner(k, zz, c).start()

                both_sides(d - 1, arrived)

        loop(3, plane_step)
        loop(3, x_step)

    def partner_arrivals(k):
        def each(zz):
            @pl.when((y == c) | (zz != z))
            def _():
                plane_to_partner(k, zz, 1 - c).wait_recv()
                rest_to_partner(k, zz, 1 - c).wait_recv()

        loop(Z, each)

    def ffn_wave(mt, d):
        def arrived(zz):
            ffn_pass(mt, zz).wait_recv()

            @pl.when(goes_on(zz))
            def _():
                ffn_pass(mt, zz).start()

            ffn_over_y(mt, zz, y).start()

        both_sides(d, arrived)

    def ffn_edges(mt, d):
        @pl.when(d == 0)
        def _():
            ffn_own_y_arrival(mt).wait_recv()

            @pl.when(z < Z - 1)
            def _():
                edge_own(mt, 0).start()

            @pl.when(z > 0)
            def _():
                edge_own(mt, 1).start()

        @pl.when(d > 0)
        def _():
            def arrived(zz):
                edge_pass(mt, zz).wait_recv()

                @pl.when(goes_on(zz))
                def _():
                    edge_pass(mt, zz).start()

            both_sides(d, arrived)

    def ffn_y_arrivals(mt):
        def each(zz):
            @pl.when(zz != z)
            def _():
                ffn_over_y(mt, zz, 1 - y).wait_recv()

        loop(Z, each)

    def share_copy(e, buf, kind):
        slot = (q, q, here.q_x)[kind]
        target = (here.partner, here.xnbr, here.partner)[kind]
        ref = buf.at[slot]
        return remote(ref, ref, s.e_send.at[e, kind], s.e_recv.at[e, kind], target)

    def share_arrival(e, buf, kind):
        slot = (here.q_partner, here.q_x, here.q_far)[kind]
        target = (here.partner, here.xnbr, here.partner)[kind]
        ref = buf.at[slot]
        return remote(ref, ref, s.e_send.at[e, kind], s.e_recv.at[e, kind], target)

    def swap_copy(i):
        return remote(xo.at[i], xp.at[i], s.p_send.at[i], s.p_recv.at[i], here.partner)

    def part_to_partner(e, j):
        return remote(ps.at[j], prb.at[e, j], s.r_send.at[e, j], s.r_recv.at[e, j], here.partner)

    def part_to_x(e):
        return remote(pS, xrb.at[e], s.r_send.at[e, 2], s.r_recv.at[e, 2], here.xnbr)

    def small_copy(bit, mine):
        size = 1 << bit
        base = (g // size) * size
        if not mine:
            base = base + size - 2 * size * ((g // size) % 2)
        ref = small_all.at[rows(n * base, 0, n * size), :]
        return remote(ref, ref, s.s_send.at[bit], s.s_recv.at[bit], here.flip_grp(bit))

    main = n - first_y
    main_rows, edge_rows = pl.ds(0, main), pl.ds(main, first_y)

    def fy_copy(mt, zz):
        return remote(
            gs.at[mt, zz, main_rows],
            yb_f.at[mt, zz, main_rows],
            s.fy_send.at[mt, zz],
            s.fy_recv.at[mt, zz],
            here.ynbr,
        )

    def edge_y(mt):
        return remote(
            gs.at[mt, z, edge_rows], yb_f.at[mt, z, edge_rows], s.ue_send.at[mt], s.ue_recv.at[mt], here.ynbr
        )

    def edge_copy(mt, zz):
        return remote(
            gs.at[mt, zz, edge_rows], s.zb_e.at[mt, z], s.uz_send.at[mt, zz], s.uz_recv.at[mt, z], here.on_line(zz)
        )

    def edge_arrival(mt, zz):
        return remote(
            gs.at[mt, zz, edge_rows], s.zb_e.at[mt, zz], s.uz_send.at[mt, zz], s.uz_recv.at[mt, zz], here.on_line(zz)
        )

    def edge_over(mt):
        total = wide(gs[mt, z, main:])
        for i in range(Z - 1):
            zz = farthest(i)
            edge_arrival(mt, zz).wait_recv()
            total = total + wide(s.zb_e[mt, zz])
        gs[mt, z, main:] = low(total)
        edge_y(mt).start()

    def fz_copy(mt, zz):
        slot = line_slot(zz)
        return remote(gk.at[mt, zz], zb_f.at[mt, slot], s.fz_send.at[mt, zz], s.fz_recv.at[mt, slot], line_target(zz))

    def fz_arrival(mt, slot):
        return remote(gk.at[mt, slot], zb_f.at[mt, slot], s.fz_send.at[mt, slot], s.fz_recv.at[mt, slot], line_target(mate))

    def piece(mt, which):
        return N + Q * mt + which

    def final_copy(mt, kind):
        target = (here.partner, here.xnbr, here.partner)[kind]
        slot = (q, q, here.q_x)[kind]
        src = ffn_out[mt].at[slot] if kind == 2 else gk.at[mt, z]
        dst = ffn_out[mt].at[slot]
        return remote(src, dst, s.fo_send.at[mt, kind], s.fo_recv.at[mt, kind], target)

    def final_arrival(mt, kind):
        target = (here.partner, here.xnbr, here.partner)[kind]
        slot = (here.q_partner, here.q_x, here.q_far)[kind]
        ref = ffn_out[mt].at[slot]
        return remote(ref, ref, s.fo_send.at[mt, kind], s.fo_recv.at[mt, kind], target)

    def final_keep(mt):
        return pltpu.make_async_copy(gk.at[mt, z], ffn_out[mt].at[q], s.fo_keep.at[mt])

    def deepen(ref, k):
        for bit in range(2, rep_bits):
            j = bit - 2
            give = remote(ref, deep_buf.at[k, j], s.d_send, s.d_recv.at[k, j], here.flip_rep(bit))
            give.start()
            give.wait()
            bring = pltpu.make_async_copy(deep_buf.at[k, j], s.d_tmp, s.d_local)
            bring.start()
            bring.wait()
            ref[...] = low(wide(ref[...]) + wide(s.d_tmp[...]))

    def ffn_grads(mt, left, right):
        def block(b):
            at = pl.ds(pl.multiple_of(b * B, 16), B)
            total = dot_nt(left[0, at, :], right[0])
            for t in range(1, Q):
                total = total + dot_nt(left[t, at, :], right[t])

            @pl.when(y == 0)
            def _():
                gk[mt, b] = low(total[:n])
                gs[mt, b] = low(total[n:])

            @pl.when(y == 1)
            def _():
                gk[mt, b] = low(total[n:])
                gs[mt, b] = low(total[:n])

            fy_copy(mt, b).start()

            @pl.when(b != z)
            def _():
                edge_copy(mt, b).start()

        loop(Z, lambda i: block(farthest(i)))

    def ffn_reduce_y(mt, i):
        zz = farthest(i)
        fy_copy(mt, zz).wait_recv()
        gk[mt, zz, :main] = low(wide(gk[mt, zz, :main]) + wide(yb_f[mt, zz, :main]))

        @pl.when((zz == mate) | (at_end & (zz != z)))
        def _():
            fz_copy(mt, zz).start()

    def ffn_relay(mt):
        def each(i):
            zz = farthest(i)

            @pl.when(is_far(zz) & jnp.logical_not(at_end))
            def _():
                fz_arrival(mt, zz).wait_recv()
                gk[mt, zz] = low(wide(gk[mt, zz]) + wide(zb_f[mt, zz]))
                fz_copy(mt, zz).start()

        loop(Z, each)

    def ffn_reduce_own(mt):
        fz_arrival(mt, mate).wait_recv()
        fz_arrival(mt, z).wait_recv()
        total = wide(gk[mt, z]) + wide(zb_f[mt, mate]) + wide(zb_f[mt, z])
        edge_y(mt).wait_recv()
        gk[mt, z, :main] = low(total[:main])
        gk[mt, z, main:] = low(total[main:] + wide(yb_f[mt, z, main:]))
        deepen(gk.at[mt, z], piece(mt, 0))
        for m in range(2):

            @pl.when(mt == m)
            def _(m=m):
                final_keep(m).start()
                final_copy(m, 0).start()
                final_copy(m, 1).start()

    def ffn_reduce_far(mt):
        for m in range(2):

            @pl.when(mt == m)
            def _(m=m):
                final_arrival(m, 1).wait_recv()
                final_copy(m, 2).start()

    def column(j, at=None):
        block = small_all[: D] if at is None else small_all[at, :]
        return wide(block)[:, j : j + 1]

    def statistics(values):
        center = values - jnp.mean(values, axis=0, keepdims=True)
        inverse = lax.rsqrt(jnp.mean(center * center, axis=0, keepdims=True) + EPSILON)
        return center * inverse, inverse

    def norm_back(upstream, normed, inverse, gain):
        scaled = upstream * gain
        return inverse * (
            scaled
            - jnp.mean(scaled, axis=0, keepdims=True)
            - normed * jnp.mean(scaled * normed, axis=0, keepdims=True)
        )

    def total_of(values):
        return jnp.sum(values, axis=1, keepdims=True)

    extra = [here.flip_rep(b) for b in range(2, rep_bits)]

    def schedule(steps):
        def body(at):
            for act in dict.fromkeys(step[0] for step in steps):
                slots = [(i, step[1:]) for i, step in enumerate(steps) if step[0] is act]
                hit = at == slots[0][0]
                for i, _ in slots[1:]:
                    hit = hit | (at == i)

                @pl.when(hit)
                def _(act=act, slots=slots):
                    picked = []
                    for j in range(len(slots[0][1])):
                        values = [args[j] for _, args in slots]
                        pick = jnp.int32(values[0])
                        if len(set(values)) > 1:
                            for (i, _), value in zip(slots[1:], values[1:]):
                                pick = jnp.where(at == i, value, pick)
                        picked.append(pick)
                    act(*picked)

        loop(len(steps), body)

    def ranges(head, served):
        def run(first, last):
            def each(h, carry):
                head(h)
                return carry

            lax.fori_loop(first, last, each, 0)

        steps, first = [], 0
        for h in sorted(served):
            steps += [(run, first, h + 1)] + served[h]
            first = h + 1
        if first < H:
            steps += [(run, first, H)]
        return steps

    local = s.l_sem

    def pull_io(ref, i):
        return pltpu.make_async_copy(ref, ioT, local.at[i])

    def opening(raw_con, turned, cut, piece_con, raw_cot, small_rows, small_own):
        put_in = pltpu.make_async_copy(ain_ref, w_io.at[rows(3 * n * g, 0, 3 * n), :], local.at[0])
        put_out = pltpu.make_async_copy(aout_ref, w_io.at[rows(3 * D + n * g, 0, n), :], local.at[1])
        put_exp = pltpu.make_async_copy(
            exp_ref.at[rows(n * q, 0, n), :], w_ffn.at[0, rows(n * g, 0, n), :], local.at[2]
        )
        pull_con = pltpu.make_async_copy(con_ref, raw_con, local.at[3])
        pull_cot = pltpu.make_async_copy(cot_ref, raw_cot, local.at[4])
        pull_tok = pull_io(tok_ref, 5)
        put_in.start()
        put_out.start()
        pull_tok.start()
        put_exp.start()
        pull_cot.start()
        pull_con.start()
        small_rows[...] = jnp.zeros_like(small_rows)
        for j, ref in enumerate(vector_refs[:8]):
            small_rows[j : j + 1, :] = wide(ref[...]).reshape(1, n)
        expand_bias = wide(vector_refs[8][...]).reshape(1, Q * n)
        for j in range(Q):
            small_rows[8 + j : 9 + j, :] = expand_bias[:, j * n : (j + 1) * n]
        small_own[...] = low(small_rows[...].T)
        put_small = pltpu.make_async_copy(small_own, small_all.at[rows(n * g, 0, n), :], s.k_sem.at[0])
        put_small.start()
        greet(here, extra)
        put_in.wait()
        put_small.wait()
        small_copy(0, True).start()
        put_out.wait()
        put_exp.wait()
        ends = []
        end = 0
        for i in range(len_ref.shape[1]):
            end = end + len_ref[0, i]
            ends.append(end)

        def labels(position):
            number = jnp.zeros(position.shape, jnp.int32)
            for end in ends:
                number = number + jnp.where(position >= end, 1, 0)
            return jnp.where(position < ends[-1], number, len(ends) + position)

        def small_rounds(bit):
            for b in range(grp_bits):

                @pl.when(bit == b)
                def _(b=b):
                    small_copy(b, False).wait_recv()
                    if b + 1 < grp_bits:
                        small_copy(b + 1, True).start()

        def layout():
            query_slot = lax.broadcasted_iota(jnp.int32, (1, T), 1)
            key_slot = lax.broadcasted_iota(jnp.int32, (T, 1), 0)
            query_label, key_label = labels(query_slot), labels(key_slot)
            allowed = (key_slot <= query_slot) & (key_label == query_label)
            maskb[...] = jnp.where(allowed, 0.0, MASKED)
            live[...] = jnp.where(query_slot < ends[-1], 1.0, 0.0)

        def first_norm():
            pull_tok.wait()
            normed, _ = statistics(ioT[...])
            xo[1] = low(normed * column(0) + column(1))
            swap_copy(1).start()

        def upstream():
            pull_cot.wait()
            start = jnp.where(live[...] > 0.5, raw_cot[...], 0.0)
            st4[q] = low(start)
            vecT[...] = jnp.zeros_like(vecT)
            vecT[:, 7:8] = total_of(start)

        def share_start():
            share_copy(0, st4, 0).start()
            share_copy(0, st4, 1).start()

        def pass_start():
            share_arrival(0, st4, 1).wait_recv()
            share_copy(0, st4, 2).start()

        def con_block(gg):
            return pltpu.make_async_copy(
                turned.at[rows(Q * n * gg, n * q, n), :], cut.at[rows(n * gg, 0, n), :], s.k_sem.at[gg]
            )

        def cut_contract():
            pull_con.wait()
            turned[:FF] = raw_con[...].T
            loop(G, lambda gg: con_block(gg).start())
            loop(G, lambda gg: con_block(gg).wait())
            piece_con[...] = cut[:D].T
            put = pltpu.make_async_copy(piece_con, w_ffn.at[1, rows(n * g, 0, n), :], local.at[3])
            put.start()
            put.wait()

        def project():
            def block(b):
                at = pl.ds(pl.multiple_of(b * B, 16), B)
                projT[at, :] = low(dot_nn(w_io[at, :], xo[1]))

            def add_bias(first, j):
                def each(b):
                    at = pl.ds(pl.multiple_of(b * B, 16), B)
                    to = pl.ds(pl.multiple_of(first + b * B, 16), B)
                    projT[to, :] = low(dot_nn(w_io[to, :], xo[1]) + column(j, at))

                loop(D // B, each)

            add_bias(0, 2)
            loop(D // B, lambda b: block(b + D // B))
            add_bias(2 * D, 3)

        def head_forward(h):
            at = pl.multiple_of(h * HD, HD)
            query = projT[pl.ds(at, HD), :]
            key = projT[pl.ds(pl.multiple_of(D + at, HD), HD), :]
            value = projT[pl.ds(pl.multiple_of(2 * D + at, HD), HD), :]
            scores = dot_nn(low(wide(key).T), query) * scale + maskb[...]
            peak = jnp.max(scores, axis=0, keepdims=True)
            logsum = peak + jnp.log(jnp.sum(jnp.exp(scores - peak), axis=0, keepdims=True))
            lse[h] = logsum
            weights = low(jnp.exp(scores - logsum))
            xo[0, pl.ds(at, HD), :] = low(dot_nn(value, weights))

        steps = [(start_own, k) for k in range(3)] + [(small_rounds, 0), (layout,)]
        steps += [(gather_wave, 0, 0), (start_own, 3), (gather_wave, 1, 0), (small_rounds, 1), (cut_contract,)]
        steps += [(gather_wave, 2, 0), (start_ffn, 0)] + [(small_rounds, b) for b in range(2, grp_bits)]
        steps += [(first_norm,)] + [(gather_wave, i, 0) for i in range(3, Z)] + [(gather_wave, 0, 1), (gather_wave, 1, 1)]
        steps += [(start_ffn_y, 0), (gather_wave, Z, 0), (upstream,), (gather_wave, 2, 1)]
        steps += [(partner_arrivals, k) for k in range(3)] + [(ffn_wave, 0, 1), (gather_wave, 3, 1)]
        steps += [(project,), (ffn_edges, 0, 0), (gather_wave, 4, 1), (share_start,)]
        served = {
            2: [(ffn_wave, 0, 2)],
            6: [(ffn_edges, 0, 1), (start_ffn, 1)],
            11: [(ffn_wave, 0, 3), (start_ffn_y, 1)],
            14: [(ffn_edges, 0, 2)],
            16: [(pass_start,)],
        }
        steps += ranges(head_forward, served)
        schedule(steps)

    pl.run_scoped(
        opening,
        pltpu.VMEM((n, FF), BF16),
        pltpu.VMEM((FF + PAD, n), BF16),
        pltpu.VMEM((D + PAD, n), BF16),
        pltpu.VMEM((n, D), BF16),
        pltpu.VMEM((D, T), F32),
        pltpu.VMEM((128, n), F32),
        pltpu.VMEM((n, 128), BF16),
    )
    swap_copy(0).start()
    partner_arrivals(3)

    def attention_out(b):
        at = pl.ds(pl.multiple_of(b * B, 16), B)
        to = pl.ds(pl.multiple_of(3 * D + b * B, 16), B)
        resT[at, :] = ioT[at, :] + dot_nn(w_io[to, :], xo[0]) + column(4, at)

    loop(D // B, attention_out)
    pull_io(cot_ref, 5).start()
    normed, _ = statistics(resT[...])
    h24[q] = low(normed * column(5) + column(6))
    share_copy(1, h24, 0).start()
    share_copy(1, h24, 1).start()

    def dy_rows(k, zz, core):
        gg = shard(zz, core)
        row = jnp.where(k == 0, 3 * D + n * gg, 3 * n * gg + n * (k - 1))
        return rows(row, 0, n)

    def dy_swap(k, zz):
        return remote(
            projT.at[dy_rows(k, zz, 1 - c), :],
            dyp.at[k, zz],
            s.dy_send.at[k, zz],
            s.dy_recv.at[k, zz],
            here.partner,
        )

    def middle(gp4, act4, bb4):
        def expand(t):
            def block(b):
                at = pl.ds(pl.multiple_of(b * B, 16), B)
                part = wide(small_all[at, :])
                bias = part[:, 8:9]
                for j in range(1, Q):
                    bias = jnp.where(q == j, part[:, 8 + j : 9 + j], bias)
                u = dot_nn(w_ffn[0, at, :], h24[t]) + bias
                th = jnp.tanh(GELU_A * (u + GELU_B * (u * u * u)))
                act4[t, at, :] = low(0.5 * u * (1.0 + th))
                gp4[t, at, :] = 0.5 * (1.0 + th) + (0.5 * GELU_A) * u * (1.0 - th * th) * (
                    1.0 + (3.0 * GELU_B) * (u * u)
                )

            loop(D // B, block)

        def expand_step(i):
            @pl.when(i == 1)
            def _():
                share_arrival(1, h24, 0).wait_recv()

            @pl.when(i == 2)
            def _():
                share_arrival(1, h24, 1).wait_recv()
                share_copy(1, h24, 2).start()

            @pl.when(i == 3)
            def _():
                share_arrival(1, h24, 2).wait_recv()

            expand(member(i))

        def gradients():
            share_arrival(0, st4, 0).wait_recv()
            share_arrival(0, st4, 2).wait_recv()
            ffn_grads(1, st4, act4)

        def member(i):
            first = jnp.where(i == 1, here.q_partner, q)
            return jnp.where(i == 2, here.q_x, jnp.where(i == 3, here.q_far, first))

        def back_step(i):
            t = member(Q - 1 - i)

            def block(b):
                at = pl.ds(pl.multiple_of(b * B, 16), B)
                value = accP[at, :] * gp4[t, at, :]
                bb4[t, at, :] = low(value)
                vecT[at, 12:13] = vecT[at, 12:13] + total_of(value)

            accP[...] = dot_tn(w_ffn[1, :D], st4[t])
            loop(D // B, block)
            accP[...] = dot_tn(w_ffn[0, :D], bb4[t])

            @pl.when(i == 0)
            def _():
                ps[1] = low(accP[...])
                part_to_partner(0, 1).start()

            @pl.when(i == 1)
            def _():
                part_to_partner(0, 1).wait_recv()
                pS[...] = low(accP[...] + wide(prb[0, 1]))
                part_to_x(0).start()

            @pl.when(i == 2)
            def _():
                ps[0] = low(accP[...])
                part_to_partner(0, 0).start()

        def expand_gradients():
            ffn_grads(0, bb4, h24)
            for j in range(2):
                part_to_partner(0, j).wait_send()

        def out_step(i):
            t = member(Q - 1 - i)
            brT[...] = dot_nn(w_ffn[1, :D], act4[t])

            @pl.when(i == 0)
            def _():
                ps[1] = low(brT[...])
                part_to_partner(1, 1).start()

            @pl.when(i == 1)
            def _():
                gp4[1] = brT[...]

            @pl.when(i == 2)
            def _():
                ps[0] = low(brT[...])
                part_to_partner(1, 0).start()

            @pl.when(i == 3)
            def _():
                gp4[0] = brT[...]

        steps = [(ffn_edges, 0, 3), (ffn_wave, 1, 1), (ffn_y_arrivals, 0), (expand_step, 0), (ffn_wave, 1, 2), (expand_step, 1)]
        steps += [(ffn_edges, 1, 0), (ffn_wave, 1, 3), (expand_step, 2), (ffn_edges, 1, 1), (expand_step, 3)]
        steps += [(ffn_edges, 1, 2), (gradients,), (ffn_edges, 1, 3), (ffn_y_arrivals, 1)]
        steps += [(back_step, 0), (back_step, 1), (ffn_reduce_y, 1, 0), (back_step, 2), (ffn_reduce_y, 1, 1)]
        steps += [(back_step, 3), (expand_gradients,), (ffn_reduce_y, 1, 2)] + [(out_step, i) for i in range(Q)]
        steps += [(ffn_reduce_y, 1, 3)]
        schedule(steps)
        part_to_partner(0, 0).wait_recv()
        part_to_x(0).wait_recv()
        back_hidden = accP[...] + wide(prb[0, 0]) + wide(xrb[0])
        normed, inverse = statistics(resT[...])
        vecT[:, 5:6] = total_of(back_hidden * normed)
        vecT[:, 6:7] = total_of(back_hidden)
        pull_io(cot_ref, 5).wait()
        start = jnp.where(live[...] > 0.5, ioT[...], 0.0)
        brT[...] = start + norm_back(back_hidden, normed, inverse, column(5))
        projT[pl.ds(3 * D, D), :] = low(brT[...])
        loop(Z, lambda zz: dy_swap(0, zz).start())
        pull_io(tok_ref, 5).start()
        part_to_x(0).wait_send()
        part_to_partner(1, 1).wait_recv()
        pS[...] = low(gp4[1] + wide(prb[1, 1]))
        resT[...] = resT[...] + gp4[0] + column(7)
        vecT[:, 4:5] = total_of(brT[...])

    pl.run_scoped(
        middle, pltpu.VMEM((Q, D, T), F32), pltpu.VMEM((Q, D, T), BF16), pltpu.VMEM((Q, D, T), BF16)
    )
    batt = xrb.at[0]
    batt[...] = low(dot_tn(w_io[pl.ds(3 * D, D), :], projT[pl.ds(3 * D, D), :]))

    def head_backward(h):
        at = pl.multiple_of(h * HD, HD)
        at_q = pl.ds(at, HD)
        at_k = pl.ds(pl.multiple_of(D + at, HD), HD)
        at_v = pl.ds(pl.multiple_of(2 * D + at, HD), HD)
        query, key, value, up = projT[at_q, :], projT[at_k, :], projT[at_v, :], batt[at_q, :]
        scores = dot_nn(low(wide(key).T), query) * scale + maskb[...]
        probability = jnp.exp(scores - lse[h])
        weights = low(probability)
        delta = jnp.sum(wide(up) * wide(xo[0, at_q, :]), axis=0, keepdims=True)
        flow = dot_nn(low(wide(value).T), up)
        slope = low(probability * (flow - delta) * scale)
        back_query = dot_nn(key, slope)
        back_value = dot_nt(up, weights)
        vecT[at_q, 2:3] = total_of(back_query)
        vecT[at_q, 3:4] = total_of(back_value)
        projT[at_k, :] = low(dot_nt(query, slope))
        projT[at_q, :] = low(back_query)
        projT[at_v, :] = low(back_value)

    wide_out = n - give_out

    def closing(plane, xs, stage, fin, con_in, con_turn, con_tall, con_flat, vec_own):
        def x_copy(k, zz):
            return remote(xs.at[k, zz], xb.at[k, zz], s.gx_send.at[k, zz], s.gx_recv.at[k, zz], here.xnbr)

        def y_copy(k, zz):
            return remote(plane.at[k, zz], yb_a.at[k, zz], s.gy_send.at[k, zz], s.gy_recv.at[k, zz], here.ynbr)

        def z_copy(k, zz):
            slot = line_slot(zz)
            return remote(
                plane.at[k, zz], zb_a.at[k, slot], s.gz_send.at[k, zz], s.gz_recv.at[k, slot], line_target(zz)
            )

        def z_arrival(k, slot):
            return remote(
                plane.at[k, slot], zb_a.at[k, slot], s.gz_send.at[k, slot], s.gz_recv.at[k, slot], line_target(mate)
            )

        def f_copy(k):
            return remote(plane.at[k, z], fx.at[k], s.gf_send.at[k], s.gf_recv.at[k], here.xnbr)

        def o_keep(k, dst):
            return pltpu.make_async_copy(fin.at[k % 2], dst, s.go_keep.at[k])

        def o_give(k, dst):
            return remote(fin.at[k % 2], dst, s.go_send.at[k], s.go_recv.at[k], here.partner)

        any_out = in_out.at[0]

        def bring(src, slot):
            copy = pltpu.make_async_copy(src, stage.at[slot], s.st_sem.at[slot])
            copy.start()
            return copy

        def multiply(k):
            j = jnp.where(k == 0, 0, 1)

            @pl.when(k == 0)
            def _():
                swap_copy(0).wait_recv()
                swap_copy(1).wait_recv()


            def each(i):
                zz = farthest(i)
                dy_swap(k, zz).wait_recv()
                term = dot_nt(projT[dy_rows(k, zz, c), :], xo[j]) + dot_nt(dyp[k, zz], xp[j])

                @pl.when(xi == 0)
                def _():
                    plane[k, zz] = low(term[:wide_out])
                    xs[k, zz] = low(term[wide_out:])

                @pl.when(xi == 1)
                def _():
                    plane[k, zz] = low(term[give_out:])
                    xs[k, zz] = low(term[:give_out])

                x_copy(k, zz).start()

            loop(Z, each)

        def after_x(k):
            def each(i):
                zz = farthest(i)
                x_copy(k, zz).wait_recv()
                got = wide(xb[k, zz])

                @pl.when(xi == 0)
                def _():
                    plane[k, zz, :give_out] = low(wide(plane[k, zz, :give_out]) + got)

                @pl.when(xi == 1)
                def _():
                    edge = wide_out - give_out
                    plane[k, zz, edge:] = low(wide(plane[k, zz, edge:]) + got)

                @pl.when(y != c)
                def _():
                    y_copy(k, zz).start()

            loop(Z, each)

        def after_y(k):
            @pl.when(source)
            def _():
                def fetch(i):
                    zz = farthest(i)
                    y_copy(k, zz).wait_recv()
                    bring(yb_a.at[k, zz], i)

                def add(i):
                    zz = farthest(i)
                    pltpu.make_async_copy(yb_a.at[k, zz], stage.at[i], s.st_sem.at[i]).wait()
                    plane[k, zz] = low(wide(plane[k, zz]) + wide(stage[i]))

                    @pl.when((zz == mate) | (at_end & (zz != z)))
                    def _():
                        z_copy(k, zz).start()

                def step(i):
                    @pl.when(i < Z)
                    def _():
                        fetch(i)

                    @pl.when(i > 0)
                    def _():
                        add(i - 1)

                loop(Z + 1, step)

        def relay(k):
            def each(i):
                zz = farthest(i)

                @pl.when(source & is_far(zz) & jnp.logical_not(at_end))
                def _():
                    z_arrival(k, zz).wait_recv()
                    bring(zb_a.at[k, zz], i).wait()
                    plane[k, zz] = low(wide(plane[k, zz]) + wide(stage[i]))
                    z_copy(k, zz).start()

            loop(Z, each)

        def after_z(k):
            @pl.when(source)
            def _():
                z_arrival(k, mate).wait_recv()
                near = bring(zb_a.at[k, mate], 0)
                z_arrival(k, z).wait_recv()
                far = bring(zb_a.at[k, z], 1)
                near.wait()
                far.wait()
                plane[k, z] = low(wide(plane[k, z]) + wide(stage[0]) + wide(stage[1]))
                f_copy(k).start()

        def finish(k):
            @pl.when(source)
            def _():
                f_copy(k).wait_recv()

                @pl.when(k >= 2)
                def _():
                    o_keep(k - 2, any_out).wait()
                    o_give(k - 2, any_out).wait_send()

                slot = k % 2

                def assemble(first, second):
                    fin[slot, :give_out] = first[:give_out]
                    fin[slot, give_out:wide_out] = low(
                        wide(first[give_out:]) + wide(second[: wide_out - give_out])
                    )
                    fin[slot, wide_out:] = second[wide_out - give_out :]

                @pl.when(xi == 0)
                def _():
                    assemble(plane[k, z], fx[k])

                @pl.when(xi == 1)
                def _():
                    assemble(fx[k], plane[k, z])

                deepen(fin.at[slot], k)
                @pl.when(k == 0)
                def _():
                    o_keep(k, out_out).start()
                    o_give(k, out_out).start()

                @pl.when(k > 0)
                def _():
                    o_keep(k, in_out.at[k - 1]).start()
                    o_give(k, in_out.at[k - 1]).start()


        def vec_copy(i):
            target_r, target_g = here.flip_rep(0)
            for b in range(1, rep_bits):
                other = here.flip_rep(b)
                target_r = jnp.where(i == b, other[0], target_r)
                target_g = jnp.where(i == b, other[1], target_g)
            for b in range(grp_bits):
                other = here.flip_grp(b)
                target_r = jnp.where(i == rep_bits + b, other[0], target_r)
                target_g = jnp.where(i == rep_bits + b, other[1], target_g)
            return remote(
                vec_buf.at[i], vec_got.at[i], s.v_send.at[i], s.v_recv.at[i], (target_r, target_g)
            )

        def swap_all():
            for k in range(1, N):
                loop(Z, lambda zz, k=k: dy_swap(k, zz).start())

        def last_norm():
            back_hidden = dot_tn(w_io[pl.ds(0, 3 * D), :], projT[: 3 * D])
            pull_io(tok_ref, 5).wait()
            normed, inverse = statistics(ioT[...])
            vecT[:, 0:1] = total_of(back_hidden * normed)
            vecT[:, 1:2] = total_of(back_hidden)
            accP[...] = brT[...] + norm_back(back_hidden, normed, inverse, column(0))
            tg_copy.start()
            spread = vecT[:, 12:13]
            for j in range(Q):
                vecT[:, 8 + j : 9 + j] = jnp.where(q == j, spread, 0.0)
            vec_buf[0] = vecT[...].T[:16]
            vec_copy(0).start()

        tg_copy = pltpu.make_async_copy(accP, tg_out, local.at[1])
        bo_copy = pltpu.make_async_copy(resT, bo_out, local.at[0])
        push_vec = pltpu.make_async_copy(vec_own, vec_out, local.at[2])

        def send_out():
            part_to_x(1).start()

        def block_done():
            part_to_partner(1, 0).wait_recv()
            part_to_x(1).wait_recv()
            output = resT[...] + wide(prb[1, 0]) + wide(xrb[1])
            resT[...] = jnp.where(live[...] > 0.5, output, 0.0)
            bo_copy.start()

        def vec_round(t):
            vec_copy(t).wait_recv()
            vec_buf[t + 1] = vec_buf[t] + vec_got[t]

            @pl.when(t + 1 < rounds)
            def _():
                vec_copy(t + 1).start()

            @pl.when(t + 1 == rounds)
            def _():
                vecT[:, :16] = vec_buf[rounds].T
                vec_own[...] = vecT[pl.ds(pl.multiple_of(n * g, 8), n), :].T[:16]
                push_vec.start()

        def bring_piece(j):
            return pltpu.make_async_copy(con_raw.at[j], con_in.at[j % 2], s.k_sem.at[2 * G + j % 2])

        def put_block(j, gg):
            return pltpu.make_async_copy(
                con_turn.at[j % 2, rows(n * gg, 0, n), :],
                con_cut.at[rows(Q * n * gg, n * j, n), :],
                s.k_sem.at[G * (j % 2) + gg],
            )

        def con_finals():
            final_keep(1).wait()
            final_arrival(1, 0).wait_recv()
            final_arrival(1, 2).wait_recv()
            bring_piece(0).start()
            bring_piece(1).start()

        def con_piece(j):
            bring_piece(j).wait()

            @pl.when(j >= 2)
            def _():
                loop(G, lambda gg: put_block(j - 2, gg).wait())

            con_turn[j % 2, :D] = con_in[j % 2].T

            @pl.when(j + 2 < Q)
            def _():
                bring_piece(j + 2).start()

            loop(G, lambda gg: put_block(j, gg).start())

        half_size = FF // 2

        def bring_side(half):
            return pltpu.make_async_copy(
                con_cut.at[rows(half_size * half, 0, half_size), :], con_tall, s.k_sem.at[2 * G + 2]
            )

        def put_side(half):
            to = pl.ds(pl.multiple_of(half_size * half, 128), half_size)
            return pltpu.make_async_copy(con_flat, con_out.at[:, to], s.k_sem.at[2 * G + 3])

        def con_side(i):
            @pl.when(i == 0)
            def _():
                loop(G, lambda gg: put_block(Q - 2, gg).wait())
                loop(G, lambda gg: put_block(Q - 1, gg).wait())
                bring_side(0).start()

            @pl.when(i > 0)
            def _():
                half = i - 1
                bring_side(half).wait()

                @pl.when(half == 1)
                def _():
                    put_side(0).wait()

                con_flat[...] = con_tall[...].T
                put_side(half).start()

                @pl.when(half == 0)
                def _():
                    bring_side(1).start()

        served = {7: [(edge_over, 1), (ffn_relay, 1)], 13: [(edge_over, 0), (ffn_reduce_y, 0, 0)]}
        steps = [(multiply, 0)] + ranges(head_backward, served)
        steps += [(swap_all,), (last_norm,), (multiply, 1), (ffn_reduce_y, 0, 1), (vec_round, 0), (after_x, 0)]
        steps += [(multiply, 2), (multiply, 3), (ffn_reduce_y, 0, 2), (ffn_reduce_y, 0, 3), (after_x, 1), (vec_round, 1)]
        steps += [(send_out,)]
        steps += [(ffn_reduce_own, 1), (after_x, 2), (after_y, 0), (ffn_relay, 0), (after_x, 3)]
        steps += [(relay, 0), (after_y, 1), (vec_round, 2), (relay, 1), (after_y, 2), (after_z, 0)]
        steps += [(relay, 2), (after_y, 3), (after_z, 1), (vec_round, 3), (relay, 3)]
        steps += [(ffn_reduce_far, 1), (finish, 0), (ffn_reduce_own, 0), (after_z, 2), (con_finals,), (finish, 1), (con_piece, 0)]
        steps += [(con_piece, 1), (con_piece, 2), (con_piece, 3), (block_done,), (after_z, 3), (con_side, 0), (vec_round, 4)]
        steps += [(finish, 2), (con_side, 1), (con_side, 2), (ffn_reduce_far, 0), (finish, 3)]
        steps += [(vec_round, t) for t in range(5, rounds)]
        schedule(steps)

        def settle(k):
            @pl.when(source)
            def _():
                @pl.when(z < Z - 1)
                def _():
                    own_copy(k, 0).wait_send()

                @pl.when(z > 0)
                def _():
                    own_copy(k, 1).wait_send()

                own_copy(k, 2).wait_send()

            def each(zz):
                @pl.when((y != c) | (zz != z))
                def _():
                    over_x(k, zz).wait_send()
                    plane_to_partner(k, zz, c).wait_send()
                    rest_to_partner(k, zz, c).wait_send()

                @pl.when(source & (zz != z))
                def _():
                    over_y(k, zz, y).wait_send()

                    @pl.when(goes_on(zz))
                    def _():
                        passing(k, zz).wait_send()

                x_copy(k, zz).wait_send()
                dy_swap(k, zz).wait_send()

                @pl.when(y != c)
                def _():
                    y_copy(k, zz).wait_send()

                @pl.when(source & (zz != z))
                def _():
                    z_copy(k, zz).wait_send()

            loop(Z, each)

            @pl.when(source)
            def _():
                f_copy(k).wait_send()

                @pl.when(k >= N - 2)
                def _():
                    o_keep(k, any_out).wait()
                    o_give(k, any_out).wait_send()

            @pl.when(y != c)
            def _():
                o_give(k, any_out).wait_recv()

        loop(N, settle)

        def settle_ffn(mt):
            @pl.when(z < Z - 1)
            def _():
                ffn_own(mt, 0).wait_send()
                edge_own(mt, 0).wait_send()

            @pl.when(z > 0)
            def _():
                ffn_own(mt, 1).wait_send()
                edge_own(mt, 1).wait_send()


            ffn_own_y(mt).wait_send()

            edge_y(mt).wait_send()

            def each(zz):
                fy_copy(mt, zz).wait_send()

                @pl.when(zz != z)
                def _():
                    ffn_over_y(mt, zz, y).wait_send()

                    @pl.when(goes_on(zz))
                    def _():
                        ffn_pass(mt, zz).wait_send()
                        edge_pass(mt, zz).wait_send()

                @pl.when(zz != z)
                def _():
                    fz_copy(mt, zz).wait_send()
                    edge_copy(mt, zz).wait_send()

            loop(Z, each)

        for mt in range(2):
            settle_ffn(mt)
            for kind in range(3):
                final_copy(mt, kind).wait_send()
        final_keep(0).wait()
        put_side(1).wait()
        final_arrival(0, 0).wait_recv()
        final_arrival(0, 2).wait_recv()
        for e, buf in ((0, st4), (1, h24)):
            for kind in range(3):
                share_copy(e, buf, kind).wait_send()
        for i in range(2):
            swap_copy(i).wait_send()
        for j in range(2):
            part_to_partner(1, j).wait_send()
        part_to_x(1).wait_send()
        for bit in range(grp_bits):
            small_copy(bit, True).wait_send()
        loop(rounds, lambda i: vec_copy(i).wait_send())
        bo_copy.wait()
        tg_copy.wait()
        push_vec.wait()

    pl.run_scoped(
        closing,
        pltpu.VMEM((N, Z, wide_out, D), BF16),
        pltpu.VMEM((N, Z, give_out, D), BF16),
        pltpu.VMEM((Z, wide_out, D), BF16),
        pltpu.VMEM((2, n, D), BF16),
        pltpu.VMEM((2, n, D), BF16),
        pltpu.VMEM((2, D + PAD, n), BF16),
        pltpu.VMEM((FF // 2, n), BF16),
        pltpu.VMEM((n, FF // 2), BF16),
        pltpu.VMEM((16, n), F32),
    )


def run_layer(lengths, tokens, cotangent, a_in, a_out, w_exp, w_con, vectors, R, G):
    D, T = tokens.shape
    FF = w_con.shape[1]
    n = D // G
    H = D // HD
    Z = G // YSIZE
    Q = TEAM
    N = 4
    give_in = (6 * n // 17) // 8 * 8
    give_out = (5 * n // 17) // 8 * 8
    wide_out = n - give_out
    rounds = bits_of(R) + bits_of(G)
    deep = bits_of(R) - 2
    dma = pltpu.SemaphoreType.DMA
    v = pltpu.VMEM
    scratch = dict(
        w_io=v((4 * D + PAD, D), BF16),
        w_ffn=v((2, D + PAD, D), BF16),
        small_all=v((D + PAD, 128), BF16),
        ioT=v((D, T), F32),
        xo=v((2, D, T), BF16),
        xp=v((2, D, T), BF16),
        projT=v((4 * D + PAD, T), BF16),
        resT=v((D, T), F32),
        h24=v((Q, D, T), BF16),
        st4=v((Q, D, T), BF16),
        brT=v((D, T), F32),
        dyp=v((N, Z, n, T), BF16),
        ps=v((2, D, T), BF16),
        pS=v((D, T), BF16),
        prb=v((2, 2, D, T), BF16),
        xrb=v((2, D, T), BF16),
        accP=v((D, T), F32),
        lse=v((H, 1, T), F32),
        maskb=v((T, T), F32),
        live=v((1, T), F32),
        vecT=v((D, 128), F32),
        vec_buf=v((rounds + 1, 16, D), F32),
        vec_got=v((rounds, 16, D), F32),
        gk=v((2, Z, n, D), BF16),
        gs=v((2, Z, n, D), BF16),
        yb_f=v((2, Z, n, D), BF16),
        zb_f=v((2, Z, n, D), BF16),
        zb_e=v((2, Z, (3 * n // 17) // 8 * 8, D), BF16),
        xb=v((N, Z, give_out, D), BF16),
        fx=v((N, wide_out, D), BF16),
        d_tmp=v((n, D) if deep > 0 else (8, 128), BF16),
        l_sem=dma((6,)),
        k_sem=dma((2 * G + 4,)),
        a_own=dma((N, 3)),
        w_own=dma((2, 3)),
        e_send=dma((2, 3)),
        e_recv=dma((2, 3)),
        p_send=dma((2,)),
        p_recv=dma((2,)),
        r_send=dma((2, 3)),
        r_recv=dma((2, 3)),
        s_send=dma((bits_of(G),)),
        s_recv=dma((bits_of(G),)),
        v_send=dma((rounds,)),
        v_recv=dma((rounds,)),
        fo_send=dma((2, 3)),
        fo_recv=dma((2, 3)),
        fo_keep=dma((2,)),
        fz_recv=dma((2, Z)),
        gz_recv=dma((N, Z)),
        gf_send=dma((N,)),
        gf_recv=dma((N,)),
        go_keep=dma((N,)),
        go_send=dma((N,)),
        go_recv=dma((N,)),
        st_sem=dma((Z,)),
        d_send=dma,
        d_local=dma,
        d_recv=dma((N + 2 * Q, max(deep, 1))),
        u_own=dma((2, 2)),
        ue_send=dma((2,)),
        ue_recv=dma((2,)),
        uz_send=dma((2, Z)),
        uz_recv=dma((2, Z)),
        u_rz=dma((2, Z)),
        u_fwd=dma((2, Z)),
        w_rz=dma((2, Z)),
        w_ry=dma((2, Z)),
        w_fwd=dma((2, Z)),
        w_y=dma((2, Z)),
        fy_send=dma((2, Z)),
        fy_recv=dma((2, Z)),
        fz_send=dma((2, Z)),
        a_rp=dma((N, Z)),
        a_rx=dma((N, Z)),
        a_rcp=dma((N, Z)),
        a_rcx=dma((N, Z)),
        a_fwd=dma((N, Z)),
        a_y=dma((N, Z)),
        a_x=dma((N, Z)),
        a_cp=dma((N, Z)),
        a_cx=dma((N, Z)),
        gx_send=dma((N, Z)),
        gx_recv=dma((N, Z)),
        gy_send=dma((N, Z)),
        gy_recv=dma((N, Z)),
        gz_send=dma((N, Z)),
        dy_send=dma((N, Z)),
        dy_recv=dma((N, Z)),
    )
    hbm = pl.BlockSpec(memory_space=pl.ANY)
    outs = pl.pallas_call(
        functools.partial(layer_kernel, R, G, give_in, give_out, tuple(scratch)),
        out_shape=(
            jax.ShapeDtypeStruct((D, T), F32),
            jax.ShapeDtypeStruct((D, T), F32),
            jax.ShapeDtypeStruct((3, n, D), BF16),
            jax.ShapeDtypeStruct((n, D), BF16),
            jax.ShapeDtypeStruct((Q, n, D), BF16),
            jax.ShapeDtypeStruct((n, FF), BF16),
            jax.ShapeDtypeStruct((16, n), F32),
            jax.ShapeDtypeStruct((Q, n, D), BF16),
            jax.ShapeDtypeStruct((FF, n), BF16),
            jax.ShapeDtypeStruct((N, Z, wide_out, D), BF16),
            jax.ShapeDtypeStruct((N, Z, wide_out, D), BF16),
            jax.ShapeDtypeStruct((N + 2 * Q, deep, n, D) if deep > 0 else (1, 1, 8, 128), BF16),
        ),
        in_specs=[pl.BlockSpec(memory_space=pltpu.SMEM)] + [hbm] * 6 + [pl.BlockSpec(memory_space=pltpu.VMEM)] * 9,
        out_specs=(hbm,) * 12,
        scratch_shapes=list(scratch.values()),
        compiler_params=pltpu.CompilerParams(collective_id=0, has_side_effects=True, vmem_limit_bytes=VMEM_LIMIT),
        name="layer",
    )(lengths, tokens, cotangent, a_in, a_out, w_exp, w_con, *vectors)
    return outs[:7]


def per_device(
    tokens,
    document_lengths,
    cotangent,
    first_gain,
    first_shift,
    attention_in,
    query_bias,
    value_bias,
    attention_out,
    output_bias,
    second_gain,
    second_shift,
    expand_weight,
    expand_bias,
    contract_weight,
    contract_bias,
):
    R, G = lax.axis_size("rep"), lax.axis_size("grp")
    T, D = tokens.shape
    n = D // G
    Q = TEAM
    vectors = [
        first_gain,
        first_shift,
        query_bias,
        value_bias,
        output_bias,
        second_gain,
        second_shift,
        contract_bias,
        expand_bias,
    ]
    block_t, tokens_t, in_grad, out_grad, exp_grad, con_grad, share = run_layer(
        document_lengths,
        tokens.T,
        cotangent.T,
        attention_in.T,
        attention_out.T,
        expand_weight.T,
        contract_weight.T,
        vectors,
        R,
        G,
    )
    out_grad = out_grad.T.astype(F32)
    in_grad = in_grad.reshape(3 * n, D).T.astype(F32)
    exp_grad = exp_grad.reshape(Q * n, D).T.astype(F32)
    con_grad = con_grad.T.astype(F32)
    return (
        block_t.T,
        tokens_t.T,
        share[0],
        share[1],
        in_grad,
        share[2],
        share[3],
        out_grad,
        share[4],
        share[5],
        share[6],
        exp_grad,
        share[8 : 8 + Q].reshape(Q * n),
        con_grad,
        share[7],
    )


def solution(mesh):
    rows = P(("rep", "grp"), None)
    split, columns = P("grp"), P(None, "grp")
    return jax.shard_map(
        per_device,
        mesh=mesh,
        in_specs=(
            rows,
            rows,
            rows,
            split,
            split,
            columns,
            split,
            split,
            columns,
            split,
            split,
            split,
            columns,
            split,
            columns,
            split,
        ),
        out_specs=(
            rows,
            rows,
            split,
            split,
            columns,
            split,
            split,
            columns,
            split,
            split,
            split,
            columns,
            split,
            columns,
            split,
        ),
        check_vma=False,
    )
```
